32 devices in a mesh: gx: 8 (over y, x, core), gy: 4 (over z).
Axes of the slice: x: 2, y: 2, z: 4, core: 2. Of those that a mesh axis runs over, the one named last changes fastest.
Arguments:
- ocean_heat_field: float32 [8, 192, 128, 128], P('gy', 'gx'), may hold values from -6 to 6
- patch_zone: int32 [192], replicated, may hold values from 0 to 31, as said below
- patch_position: int32 [192], replicated, may hold values from 0 to 11, as said below
- quarter_spins: int32 [192], replicated, may hold values from 0 to 3
- zone_patch_tally: int32 [32], P(('gx', 'gy')), may hold values from 0 to 12, as said below
Outputs:
- regional: float32 [8, 32, 12, 128, 128], P(None, ('gx', 'gy'))
The draws below stay inside these ranges and needn't reach their ends.
Inputs may be any that keep to these rules, and one draw needn't show every extreme that they name: In each aligned group of 24 blocks no more than 6 go to regions of one column patch_zone // 4, and each group has a column with exactly 6. A region receives at most 12 blocks and some region receives exactly 12. `patch_position`: the blocks of one region have distinct slots 0 to zone_patch_tally of that region minus 1, in increasing block order. zone_patch_tally[r] is the number of blocks j with patch_zone[j] = r.
All inputs are finite; a program needn't handle non-finite values.
Results may differ from the reference program's by a relative error of at most 0.00002.
Values sent between devices are 32-bit elements; how exact they have to be, the bound alone decides.
A program may use at most 128 MiB of HBM per device.

```python
import jax
import jax.numpy as jnp

PATCH_SIDE = 128
BLK_DEV = 24
INPUT_PATCHES = 192
EPOCH_TOTAL = 8
REGIONS = 32
MOST = 6
CAP = 12


def rank_within(labels, label_count):
    onehot = (labels[:, None] == jnp.arange(label_count, dtype=jnp.int32)[None, :]).astype(jnp.int32)
    running = jnp.cumsum(onehot, axis=0) - onehot
    return jnp.sum(running * onehot, axis=1).astype(jnp.int32)


def routing(key):
    column_count = INPUT_PATCHES // BLK_DEV
    row_count = REGIONS // column_count
    column_slots = column_count * MOST
    group_key = jax.random.fold_in(key, 101)
    order_key = jax.random.fold_in(key, 202)

    def group_columns(subkey):
        pick_key, score_key, shuffle_key = jax.random.split(subkey, 3)
        chosen = jax.random.randint(pick_key, (), 0, column_count, dtype=jnp.int32)
        slot_ids = jnp.arange(column_slots, dtype=jnp.int32)
        scores = jax.random.permutation(score_key, column_slots).astype(jnp.int32)
        scores = jnp.where(slot_ids // MOST == chosen, slot_ids % MOST - MOST, scores)
        ranked = jnp.argsort(scores, stable=True).astype(jnp.int32)
        return jax.random.permutation(shuffle_key, ranked[:BLK_DEV] // MOST)
    columns = jax.vmap(group_columns)(jax.random.split(group_key, column_count)).reshape(-1)

    def column_order(subkey):
        pick_key, score_key = jax.random.split(subkey)
        chosen = jax.random.randint(pick_key, (), 0, row_count, dtype=jnp.int32)
        slot_ids = jnp.arange(column_slots, dtype=jnp.int32)
        scores = jax.random.permutation(score_key, column_slots).astype(jnp.int32)
        scores = jnp.where(slot_ids // CAP == chosen, slot_ids % CAP - CAP, scores)
        return jnp.argsort(scores, stable=True).astype(jnp.int32)
    orders = jax.vmap(column_order)(jax.random.split(order_key, column_count))
    within = rank_within(columns, column_count)
    rows = orders[columns, within] // CAP
    regions = (columns * row_count + rows).astype(jnp.int32)
    slots = rank_within(regions, REGIONS)
    counts = jnp.sum((regions[:, None] == jnp.arange(REGIONS, dtype=jnp.int32)[None, :]).astype(jnp.int32), axis=0)
    return (regions, slots, counts.astype(jnp.int32))


def draw_patch_zone(key, part):
    return routing(key)[0]


def draw_patch_position(key, part):
    return routing(key)[1]


def draw_zone_patch_tally(key, part):
    return routing(key)[2]


def plant(array, key, smallest, largest):
    shape = array.shape
    index_at = [jax.random.randint(jax.random.fold_in(key, axis), (), 0, shape[axis]) for axis in range(len(shape))]
    array = array.at[tuple(index_at)].set(smallest)
    longest = shape.index(max(shape))
    index_at[longest] = (index_at[longest] + 1) % shape[longest]
    return array.at[tuple(index_at)].set(largest)


def level_of(rng, extent, pieces, low, high):
    def one(axis_at, blocks):
        heights = jax.random.uniform(jax.random.fold_in(jax.random.fold_in(rng, 6), axis_at), (blocks,), jnp.float32, low / len(pieces), high / len(pieces))
        return jnp.repeat(jnp.exp(heights), extent[axis_at] // blocks).reshape((-1,) + (1,) * (len(extent) - axis_at - 1))

    loudness = one(*pieces[0])
    for cut in pieces[1:]:
        loudness = loudness * one(*cut)
    return loudness


def noise(rng, dims, deviation, limit, cuts=(), kind=jnp.bfloat16):
    result = jax.random.normal(rng, dims, jnp.float32) * deviation
    if len(cuts) > 0:
        result = level_of(rng, dims, cuts, -0.22, 0.18) * result
    return jnp.clip(result, min=-limit, max=limit).astype(kind)


def setup_inputs(seed: int = 0) -> dict:
    streams_of = jax.random.split(jax.random.key(seed), 6)
    return {
        "ocean_heat_field": noise(streams_of[0], (EPOCH_TOTAL, INPUT_PATCHES, PATCH_SIDE, PATCH_SIDE), 1.0, 6.0, ((0, 4), (1, 8)), jnp.float32),
        "patch_zone": draw_patch_zone(jax.random.fold_in(streams_of[5], 71), 0),
        "patch_position": draw_patch_position(jax.random.fold_in(streams_of[5], 71), 0),
        "quarter_spins": plant(jax.random.randint(streams_of[3], (INPUT_PATCHES,), 0, 4), jax.random.fold_in(streams_of[3], 1), 0, 3).astype(jnp.int32),
        "zone_patch_tally": draw_zone_patch_tally(jax.random.fold_in(streams_of[5], 71), 0),
    }


def spin_patches(incoming_patches, turn_codes):
    first_turn = jnp.rot90(incoming_patches, 1, axes=(2, 3))
    half_turn = jnp.rot90(incoming_patches, 2, axes=(2, 3))
    last_turn = jnp.rot90(incoming_patches, 3, axes=(2, 3))
    shaped = turn_codes[None, :, None, None]
    return jnp.where(shaped == 0, incoming_patches, jnp.where(shaped == 1, first_turn, jnp.where(shaped == 2, half_turn, last_turn)))


def reference(ocean_heat_field, patch_zone, patch_position, quarter_spins, zone_patch_tally):
    spun_patches = spin_patches(ocean_heat_field, quarter_spins)
    centered = spun_patches - jnp.mean(spun_patches, axis=0, keepdims=True)
    arranged = jnp.zeros((EPOCH_TOTAL, REGIONS, CAP, PATCH_SIDE, PATCH_SIDE), jnp.float32)
    arranged = arranged.at[:, patch_zone, patch_position].set(centered)
    in_use = jnp.arange(CAP, dtype=jnp.int32)[None, :] < zone_patch_tally[:, None]
    return jnp.where(in_use[None, :, :, None, None], arranged, jnp.float32(0.0))
```

```python
import functools

import jax
import jax.numpy as jnp
from jax import lax
from jax.experimental import pallas as pl
from jax.experimental.pallas import tpu as pltpu
from jax.sharding import PartitionSpec as P

MESH = pl.DeviceIdType.MESH
PART = 8
STEP_BLOCKS = 4


def chunk_units(times, side):
    units = [(r, t) for r in range(side // (2 * PART)) for t in range(times)]
    small = 2 * (times // 2 + times % 2)
    cuts = list(range(0, small + 1, max(times // 2, 1)))
    cuts += list(range(small + times, len(units) - small + 1, times))
    cuts += list(range(len(units) - small + max(times // 2, 1), len(units) + 1, max(times // 2, 1)))
    return [units[a:b] for a, b in zip(cuts[:-1], cuts[1:])]


def mirror_lanes(block):
    side = block.shape[1]
    lane = side - 1 - lax.broadcasted_iota(jnp.int32, block.shape, 1)
    return jnp.take_along_axis(block, lane, axis=1)


def turn_blocks(first, chunks, spins, field, turned):
    times, blocks, side, _ = field.shape
    for b in range(blocks):
        code = spins[first + b]
        for kind in range(4):
            @pl.when(code == kind)
            def _(kind=kind, b=b):
                for t in range(times):
                    block = field[t, b]
                    if kind == 1:
                        block = mirror_lanes(block).T
                    elif kind == 2:
                        block = mirror_lanes(mirror_lanes(block).T).T
                    elif kind == 3:
                        block = mirror_lanes(block.T)
                    for c, chunk in enumerate(chunks):
                        for i, (r, at) in enumerate(chunk):
                            if at == t:
                                for h in range(2):
                                    top = h * (side // 2) + r * PART
                                    turned[c][h, b, i] = block[top:top + PART]


def prepare(dims, zone, slot, spins, field, *refs):
    pairs, rows, per_group, per_pair, cap, chunks, sizes = dims
    turned = refs[:len(chunks)]
    send_table, pick_table, tallies, choice, counts, fills = refs[len(chunks):]
    gx = lax.axis_index("gx")
    pair = gx // 2
    group = 2 * per_group
    local = 2 * rows
    step = pl.program_id(0)

    @pl.when(step == 0)
    def _():
        def clear(ref, size):
            def body(i, c):
                ref[i] = 0
                return c
            lax.fori_loop(0, size, body, 0, unroll=8)
        clear(send_table, pairs * per_pair + 1)
        clear(pick_table, local * cap + 1)
        clear(counts, pairs * local)
        clear(fills, pairs * pairs)

        for source in range(pairs):
            behind = lax.rem(pair - source + pairs, pairs) * per_pair

            def place(j, c, source=source, behind=behind):
                region = zone[source * group + j]
                counts[region] = counts[region] + 1
                target = region // local
                cell = source * pairs + target
                rank = fills[cell]
                fills[cell] = rank + 1
                ahead = lax.rem(target - source + pairs, pairs) * per_pair
                send_table[jnp.where(source == pair, ahead + rank, pairs * per_pair)] = j
                at = (region - target * local) * cap + slot[source * group + j]
                pick_table[jnp.where(target == pair, at, local * cap)] = behind + rank
                return c
            lax.fori_loop(0, group, place, 0, unroll=4)
        most_pair = jnp.int32(0)
        most_row = jnp.int32(0)
        for q in range(pairs):
            for r in range(pairs):
                if q != r:
                    most_pair = jnp.maximum(most_pair, fills[q * pairs + r])
            pooled = [counts[q * local + r] + counts[q * local + rows + r] for r in range(rows)]
            for value in pooled:
                most_row = jnp.maximum(most_row, value)
        for r in range(local):
            tallies[r] = counts[pair * local + r]
        chosen = jnp.int32(len(sizes) - 1)
        for at in range(len(sizes) - 2, -1, -1):
            wide, tall = sizes[at]
            fits = jnp.logical_and(most_pair <= wide, most_row <= tall)
            chosen = jnp.where(fits, at, chosen)
        choice[0] = chosen

    turn_blocks(gx * per_group + step * field.shape[1], chunks, spins, field, turned)


def origin_of(z, rows, k, relay):
    if not relay:
        return lax.rem(z - k + rows, rows)
    low = z < 2
    return [z, z + 1 - 2 * lax.rem(z, 2), jnp.where(low, 2, 1), jnp.where(low, 3, 0)][k]


def exchange(dims, send_table, pick_table, tallies, *refs):
    pairs, rows, per_group, per_pair, wide, tall, cap, chunks = dims
    turned, final, scratch = refs[:chunks], refs[chunks:2 * chunks], refs[2 * chunks:]
    kinds = 7
    groups = [scratch[i * chunks:(i + 1) * chunks] for i in range(kinds)]
    held, packed, landed, lifted, risen, given, kept = groups
    sems = list(scratch[kinds * chunks:])
    row_list = sems.pop(0)
    own_sem, swap_send, swap_recv, pair_send, pair_recv, row_send, row_recv, give_send, give_recv, keep_sem = sems
    gx = lax.axis_index("gx")
    z = lax.axis_index("gy")
    pair = gx // 2
    half = lax.rem(gx, 2)
    mate = (2 * pair + 1 - half, z)

    def across(o):
        return (2 * lax.rem(pair + o, pairs) + half, z)

    def along(o):
        return (gx, lax.rem(z + o, rows))

    barrier = pltpu.get_barrier_semaphore()
    friends = [mate] + [across(o) for o in range(1, pairs)] + [along(o) for o in range(1, rows)]
    for friend in friends:
        pl.semaphore_signal(barrier, inc=1, device_id=friend, device_id_type=MESH)
    own_copies = []
    for c in range(chunks):
        own = pltpu.make_async_copy(turned[c].at[half], held[c].at[pl.ds(half * per_group, per_group)], own_sem.at[c])
        own.start()
        own_copies.append(own)
    pl.semaphore_wait(barrier, len(friends))

    swaps = []
    for c in range(chunks):
        swap = pltpu.make_async_remote_copy(
            src_ref=turned[c].at[1 - half], dst_ref=held[c].at[pl.ds(half * per_group, per_group)],
            send_sem=swap_send.at[c], recv_sem=swap_recv.at[c], device_id=mate, device_id_type=MESH)
        swap.start()
        swaps.append(swap)

    unsent = []
    pair_copies = []
    for c in range(chunks):
        own_copies[c].wait()
        swaps[c].wait_recv()
        unsent.append(swaps[c])
        sent = []
        for o in range(1, pairs):
            def pack(k, carry, o=o, c=c):
                packed[c][o - 1, k] = held[c][send_table[o * per_pair + k]]
                return carry
            lax.fori_loop(0, wide, pack, 0, unroll=4)
            copy = pltpu.make_async_remote_copy(
                src_ref=packed[c].at[o - 1], dst_ref=landed[c].at[pl.ds(o * per_pair, wide)],
                send_sem=pair_send.at[c, o - 1], recv_sem=pair_recv.at[c, o - 1],
                device_id=across(o), device_id_type=MESH)
            copy.start()
            sent.append(copy)
        unsent.extend(sent)

        def stay(k, carry, c=c):
            landed[c][k] = held[c][send_table[k]]
            return carry
        lax.fori_loop(0, per_pair, stay, 0, unroll=4)
        pair_copies.append(sent)

    for r in range(rows):
        first = tallies[r]

        def compact(k, carry, r=r, first=first):
            at = jnp.minimum(jnp.where(k < first, r * cap + k, (rows + r) * cap + k - first), 2 * rows * cap - 1)
            row_list[r * tall + k] = pick_table[at]
            return carry
        lax.fori_loop(0, tall, compact, 0, unroll=4)

    gives = []

    def settle_all(c):
        first = tallies[z]

        def settle(s, carry, c=c):
            mine = jnp.minimum(s + half * first, tall - 1)
            other = jnp.minimum(s + (1 - half) * first, tall - 1)
            for o in range(rows):
                given[c][s, o] = risen[c][o, other]
                kept[c][s, o] = risen[c][o, mine]
            return carry
        lax.fori_loop(0, cap, settle, 0)
        give = pltpu.make_async_remote_copy(
            src_ref=given[c], dst_ref=final[c].at[half],
            send_sem=give_send.at[c], recv_sem=give_recv.at[c], device_id=mate, device_id_type=MESH)
        give.start()
        keep = pltpu.make_async_copy(kept[c], final[c].at[half], keep_sem.at[c])
        keep.start()
        gives.append((give, keep))

    row_copies = []
    for c in range(chunks):
        for copy in pair_copies[c]:
            copy.wait_recv()
        sent = []
        for o in list(range(rows - 1, 0, -1)) + [0]:
            row = lax.rem(z + o, rows)

            def lift(k, carry, o=o, c=c, row=row):
                tile = landed[c][row_list[row * tall + k]]
                if o > 0:
                    lifted[c][o - 1, k] = tile
                else:
                    risen[c][0, k] = tile
                return carry
            lax.fori_loop(0, tall, lift, 0, unroll=4)
            if o > 0:
                copy = pltpu.make_async_remote_copy(
                    src_ref=lifted[c].at[o - 1], dst_ref=risen[c].at[o],
                    send_sem=row_send.at[c, o - 1], recv_sem=row_recv.at[c, o - 1],
                    device_id=along(o), device_id_type=MESH)
                copy.start()
                sent.append(copy)
        row_copies.append(sent)
        unsent.extend(sent)
    for c in range(chunks):
        for copy in row_copies[c]:
            copy.wait_recv()
        settle_all(c)
    for copy in unsent:
        copy.wait_send()
    for give, keep in gives:
        give.wait()
        keep.wait()


def finish(rows, chunks, relay, tally, *refs):
    final, regional = refs[:-1], refs[-1]
    z = lax.axis_index("gy")
    slot = pl.program_id(0)
    side = regional.shape[3]
    times = regional.shape[0] // rows
    place = {unit: (c, i) for c, chunk in enumerate(chunks) for i, unit in enumerate(chunk)}

    @pl.when(slot < tally[0])
    def _():
        for h in range(2):
            for r in range(side // (2 * PART)):
                span = pl.ds(h * (side // 2) + r * PART, PART)
                tiles = {}
                for t in range(times):
                    c, i = place[(r, t)]
                    for o in range(rows):
                        tiles[o, t] = final[c][h, 0, o, i]
                mean = sum(tiles.values()) * jnp.float32(1.0 / (rows * times))
                for o in range(rows):
                    start = origin_of(z, rows, o, relay) * times
                    for t in range(times):
                        regional[start + t, 0, 0, span, :] = tiles[o, t] - mean

    @pl.when(slot >= tally[0])
    def _():
        regional[...] = jnp.zeros_like(regional)


def levels(most, steps):
    return sorted({-(-most * s // 48) for s in steps})


def balanced_sizes(per_pair, tall):
    steps = ((36, 36, 54), (40, 38, 58), (40, 42, 62), (44, 44, 68), (48, 48, 96))
    return [(-(-per_pair * w // 48), -(-tall * e // 48), -(-tall * f // 48)) for w, e, f in steps]

def beside(x, step):
    return jnp.concatenate([x[step:], x[:step]], axis=0)


def plan_tables(dims, sizes, pair, zone, slot, allow):
    pairs, rows, per_group, per_pair, cap, extra = dims
    group, local, tall = 2 * per_group, 2 * rows, 2 * cap
    bins = pairs * rows
    width = zone.shape[1]
    i32, f32, bf16 = jnp.int32, jnp.float32, jnp.bfloat16
    lane = lax.broadcasted_iota(i32, (1, width), 1)
    valid = zone >= 0
    source = sum((lane >= group * k).astype(i32) for k in range(1, pairs))
    home = sum((zone >= local * k).astype(i32) for k in range(1, pairs))
    inside = zone - home * local
    side = (inside >= rows).astype(i32)
    row = inside - side * rows
    bin_at = lax.broadcasted_iota(i32, (bins, width), 0)
    before = (lax.broadcasted_iota(i32, (width, width), 0) < lax.broadcasted_iota(i32, (width, width), 1)).astype(bf16)

    def marks(key):
        return jnp.where(bin_at == jnp.where(valid, key, -1), 1.0, 0.0).astype(f32)

    def tally(mark):
        return jnp.sum(mark, axis=1, keepdims=True)

    def look(mark, table):
        return jnp.sum(mark * table, axis=0, keepdims=True)

    def ranks(mark):
        return jnp.dot(mark.astype(bf16), before, preferred_element_type=f32)

    at = lax.broadcasted_iota(i32, (bins, 128), 0)
    at_row = at & (rows - 1)
    at_home = at >> (rows.bit_length() - 1)
    edge = jnp.logical_or(at_row == 0, at_row == rows - 1)

    def flip(x, bit):
        step = 1 << bit
        if 2 * step == bins:
            return beside(x, step)
        return jnp.where((at & step) == 0, beside(x, step), beside(x, bins - step))

    across_x = lambda x: flip(x, 2)
    across_y = lambda x: flip(x, 3)
    mark = marks(home * rows + row)
    order = look(mark, ranks(mark))
    native = jnp.broadcast_to(tally(mark), (bins, 128)).astype(i32)

    def whole(x):
        x = x + across_x(x)
        return x + across_y(x)

    load = native
    half_sum = whole(native + flip(native, 0))
    goal = (jnp.maximum(half_sum, flip(half_sum, 1)) + pairs - 1) >> (pairs.bit_length() - 1)
    row_sum = (whole(native) + pairs - 1) >> (pairs.bit_length() - 1)
    end_goal = jnp.maximum(jnp.maximum(row_sum, flip(flip(row_sum, 0), 1)), (2 * goal * 171) >> 9)
    used = [jnp.zeros_like(native), jnp.zeros_like(native)]
    for _ in range(2):
        for d, partner in enumerate((across_x, across_y)):
            for stage in range(2):
                if stage == 0:
                    now, want, here = load, end_goal, edge
                else:
                    now, want, here = load + flip(load, 0), goal, jnp.logical_not(edge)
                move = jnp.minimum((now - partner(now)) >> 1, now - want)
                move = jnp.minimum(move, jnp.minimum(extra - used[d], native - used[0] - used[1]))
                move = jnp.where(here, jnp.maximum(move, 0), 0)
                used[d] = used[d] + move
                load = load + partner(move) - move
    first = look(mark, (used[0] * allow)[:, :1].astype(f32))
    second = look(mark, (used[1] * allow)[:, :1].astype(f32))
    leaves_x = order < first
    leaves_y = jnp.logical_and(order >= first, order < first + second)
    way = leaves_y.astype(i32)
    guest = order - jnp.where(leaves_y, first, 0.0)
    home_x = home & 1
    home_y = home >> 1
    via = jnp.where(leaves_x, home_y * 2 + 1 - home_x, jnp.where(leaves_y, (1 - home_y) * 2 + home_x, home))

    flow = marks(source * pairs + via)
    line = marks(via * rows + row)
    both = ranks(jnp.concatenate([flow, line], axis=0))
    rank = look(flow, both[:bins])
    place = look(line, both[bins:])
    flows = jnp.broadcast_to(tally(flow), (bins, 128))
    lines = jnp.broadcast_to(tally(line), (bins, 128))
    halves = lines + flip(lines, 0)
    stays = at_home == at_row
    chosen = jnp.zeros((1, 128), f32)
    for wide, end, far in sizes:
        over = jnp.where(flows > jnp.where(stays, per_pair, wide).astype(f32), 1.0, 0.0)
        over = jnp.maximum(over, jnp.where(lines > jnp.where(edge, end, tall).astype(f32), 1.0, 0.0))
        over = jnp.maximum(over, jnp.where(halves > jnp.float32(far), 1.0, 0.0))
        chosen = chosen + jnp.max(over, axis=0, keepdims=True)

    my_x, my_y = pair % 2, pair // 2

    def offset(other):
        other_y = other >> 1
        other_x = other - 2 * other_y
        return jnp.where(other_x == my_x, 0, 1) + jnp.where(other_y == my_y, 0, 2)

    def invert(here, key, value):
        key = jnp.where(jnp.logical_and(valid, here), key, -1)
        hit = jnp.where(lax.broadcasted_iota(i32, (128, width), 0) == key, 1.0, 0.0).astype(bf16)
        value = jnp.broadcast_to(value.astype(bf16), (16, width))
        return lax.dot_general(value, hit, (((1,), (1,)), ((), ())), preferred_element_type=f32)[:1]

    rank = rank.astype(i32)
    place = place.astype(i32)
    guest = guest.astype(i32)
    landing = offset(source) * per_pair + rank
    mine = via == pair
    ours = home == pair
    return chosen, [
        invert(source == pair, offset(via) * per_pair + rank, (lane - group * pair).astype(f32)),
        invert(mine, row * tall + place, landing.astype(f32)),
        invert(jnp.logical_and(mine, home != pair), (way * rows + row) * extra + guest, place.astype(f32)),
        invert(ours, (side * rows + row) * cap + slot, jnp.where(mine, place, tall + way * extra + guest).astype(f32)),
        invert(mine, row, jnp.ones((1, width), f32)),
    ]


def prepare_balanced(dims, sizes, chunks, zone, slot, spins, field, *refs):
    per_group = dims[2]
    turned = refs[:len(chunks)]
    table, choice, padded = refs[len(chunks):]
    gx = lax.axis_index("gx")
    step = pl.program_id(0)

    @pl.when(step == 0)
    def _():
        padded[...] = jnp.full_like(padded, -1)
        padded[0:1, 0:zone.shape[1]] = zone[...]
        padded[1:2, 0:zone.shape[1]] = slot[...]

        def fill(sizes, allow):
            chosen, rows_of = plan_tables(dims, sizes, gx // 2, padded[0:1], padded[1:2], allow)
            for k, line in enumerate(rows_of):
                table[k:k + 1] = line.astype(jnp.int32)
            return jnp.max(chosen).astype(jnp.int32)

        chosen = fill(sizes, 1)
        choice[0] = jnp.minimum(chosen, len(sizes) - 1)

        @pl.when(chosen == len(sizes))
        def _():
            fill(sizes[:0], 0)

    turn_blocks(gx * per_group + step * field.shape[1], chunks, spins, field, turned)


def exchange_balanced(dims, table, *refs):
    pairs, rows, per_group, per_pair, cap, extra, wide, end, far, starts = dims
    tall = 2 * cap
    chunks = len(starts)
    turned, final, scratch = refs[:chunks], refs[chunks:2 * chunks], refs[2 * chunks:]
    kinds = 12
    groups = [scratch[i * chunks:(i + 1) * chunks] for i in range(kinds)]
    held, packed, landed, lifted, risen, given, kept, pooled, crossed, passed, leaving, visiting = groups
    sems = list(scratch[kinds * chunks:])
    far_list = sems.pop(0)
    own_sem, swap_send, swap_recv, pair_send, pair_recv, near_send, near_recv = sems[:7]
    give_send, give_recv, keep_sem, far_send, far_recv, pass_send, pass_recv, side_send, side_recv = sems[7:]
    gx = lax.axis_index("gx")
    z = lax.axis_index("gy")
    pair = gx // 2
    half = lax.rem(gx, 2)
    mate = (2 * pair + 1 - half, z)
    pair_x = lax.rem(pair, 2)
    pair_y = pair // 2
    near, far_in, far_out = (origin_of(z, rows, k, True) for k in (1, 2, 3))
    inner = jnp.logical_or(z == 1, z == 2)
    outer = jnp.logical_not(inner)
    role = jnp.where(inner, 0, 1)

    def across(o):
        x = 1 - pair_x if o % 2 else pair_x
        y = 1 - pair_y if o // 2 else pair_y
        return (2 * (2 * y + x) + half, z)

    barrier = pltpu.get_barrier_semaphore()
    friends = [mate] + [across(o) for o in range(1, pairs)] + [(gx, lax.rem(z + o, rows)) for o in range(1, rows)]
    for friend in friends:
        pl.semaphore_signal(barrier, inc=1, device_id=friend, device_id_type=MESH)
    own_copies = []
    for c in range(chunks):
        own = pltpu.make_async_copy(turned[c].at[half], held[c].at[pl.ds(half * per_group, per_group)], own_sem.at[c])
        own.start()
        own_copies.append(own)
    pl.semaphore_wait(barrier, len(friends))

    swaps = []
    for c in range(chunks):
        swap = pltpu.make_async_remote_copy(
            src_ref=turned[c].at[1 - half], dst_ref=held[c].at[pl.ds(half * per_group, per_group)],
            send_sem=swap_send.at[c], recv_sem=swap_recv.at[c], device_id=mate, device_id_type=MESH)
        swap.start()
        swaps.append(swap)

    unsent = []
    pair_copies = {}

    def send_pairs(c):
        own_copies[c].wait()
        swaps[c].wait_recv()
        unsent.append(swaps[c])
        sent = []
        for o in range(1, pairs):
            def pack(k, carry, o=o):
                packed[c][o - 1, k] = held[c][table[0, o * per_pair + k]]
                return carry
            lax.fori_loop(0, wide, pack, 0, unroll=4)
            copy = pltpu.make_async_remote_copy(
                src_ref=packed[c].at[o - 1], dst_ref=landed[c].at[pl.ds(o * per_pair, wide)],
                send_sem=pair_send.at[c, o - 1], recv_sem=pair_recv.at[c, o - 1],
                device_id=across(o), device_id_type=MESH)
            copy.start()
            sent.append(copy)
        unsent.extend(sent)
        pair_copies[c] = sent

        def stay(k, carry):
            landed[c][k] = held[c][table[0, k]]
            return carry
        lax.fori_loop(0, per_pair, stay, 0, unroll=4)

        if c == 0:
            lead = table[4, far_in]

            def gather_far(k, carry):
                at = jnp.where(k < lead, far_in * tall + k, far_out * tall + k - lead)
                far_list[k] = table[1, jnp.minimum(at, rows * tall - 1)]
                return carry
            lax.fori_loop(0, far, gather_far, 0, unroll=4)

    skip = table[4, z]

    def near_copy(c, size):
        return pltpu.make_async_remote_copy(
            src_ref=lifted[c].at[pl.ds(0, size)], dst_ref=risen[c].at[1, pl.ds(0, size)],
            send_sem=near_send.at[c], recv_sem=near_recv.at[c],
            device_id=(gx, near), device_id_type=MESH)

    def far_copy(c, place):
        return pltpu.make_async_remote_copy(
            src_ref=pooled[c], dst_ref=crossed[c].at[place],
            send_sem=far_send.at[c], recv_sem=far_recv.at[c, place],
            device_id=(gx, far_in), device_id_type=MESH)

    def pass_copy(c, place):
        return pltpu.make_async_remote_copy(
            src_ref=passed[c].at[place], dst_ref=risen[c].at[2 + place, pl.ds(0, end)],
            send_sem=pass_send.at[c, place], recv_sem=pass_recv.at[c, place],
            device_id=(gx, near), device_id_type=MESH)

    def side_copy(c, d):
        return pltpu.make_async_remote_copy(
            src_ref=leaving[c].at[d], dst_ref=visiting[c].at[d],
            send_sem=side_send.at[c, d], recv_sem=side_recv.at[c, d],
            device_id=across(1 + d), device_id_type=MESH)

    def send_rows(c):
        for copy in pair_copies[c]:
            copy.wait_recv()

        def pool(k, carry):
            pooled[c][k] = landed[c][far_list[k]]
            return carry
        lax.fori_loop(0, far, pool, 0, unroll=4)
        far_copy(c, role).start()
        unsent.append(far_copy(c, role))

        def lift(k, carry):
            lifted[c][k] = landed[c][table[1, near * tall + k]]
            return carry
        lax.fori_loop(0, tall, lift, 0, unroll=4)

        @pl.when(inner)
        def _():
            near_copy(c, end).start()

        @pl.when(outer)
        def _():
            near_copy(c, tall).start()

        def own(k, carry):
            risen[c][0, k] = landed[c][table[1, z * tall + k]]
            return carry
        lax.fori_loop(0, tall, own, 0, unroll=4)

    def hand_on(c):
        @pl.when(inner)
        def _():
            for place in range(2):
                far_copy(c, place).wait_recv()
            for place in range(2):
                def onward(k, carry, place=place):
                    passed[c][place, k] = crossed[c][place, jnp.minimum(skip + k, far - 1)]
                    return carry
                lax.fori_loop(0, end, onward, 0, unroll=4)
                pass_copy(c, place).start()

                def land(k, carry, place=place):
                    risen[c][2 + place, k] = crossed[c][place, k]
                    return carry
                lax.fori_loop(0, tall, land, 0, unroll=4)

    def send_sides(c):
        @pl.when(inner)
        def _():
            near_copy(c, tall).wait_recv()

        @pl.when(outer)
        def _():
            near_copy(c, end).wait_recv()
            for place in range(2):
                pass_copy(c, place).wait_recv()

        for d in range(2):
            def leave(k, carry, d=d):
                at = table[2, (d * rows + z) * extra + k]
                for o in range(rows):
                    leaving[c][d, o, k] = risen[c][o, at]
                return carry
            lax.fori_loop(0, extra, leave, 0)
            side_copy(c, d).start()
            unsent.append(side_copy(c, d))

    gives = []

    def settle(c):
        for d in range(2):
            side_copy(c, d).wait_recv()

        def place(s, carry):
            for side, out in ((1 - half, given), (half, kept)):
                at = table[3, (side * rows + z) * cap + s]
                guest = jnp.maximum(at - tall, 0)
                way = guest // extra
                for o in range(rows):
                    home = risen[c][o, jnp.minimum(at, tall - 1)]
                    visitor = visiting[c][way, o, guest - way * extra]
                    out[c][s, o] = jnp.where(at < tall, home, visitor)
            return carry
        lax.fori_loop(0, cap, place, 0)
        give = pltpu.make_async_remote_copy(
            src_ref=given[c], dst_ref=final[c].at[half],
            send_sem=give_send.at[c], recv_sem=give_recv.at[c], device_id=mate, device_id_type=MESH)
        give.start()
        keep = pltpu.make_async_copy(kept[c], final[c].at[half], keep_sem.at[c])
        keep.start()
        gives.append((give, keep))

    for _, _, c, act in timetable(starts, wide, end, far, extra, (send_pairs, send_rows, hand_on, send_sides, settle)):
        act(c)

    @pl.when(inner)
    def _():
        for c in range(chunks):
            near_copy(c, end).wait_send()
            for place in range(2):
                pass_copy(c, place).wait_send()

    @pl.when(outer)
    def _():
        for c in range(chunks):
            near_copy(c, tall).wait_send()

    for copy in unsent:
        copy.wait_send()
    for give, keep in gives:
        give.wait()
        keep.wait()


def timetable(starts, wide, end, far, extra, acts):
    sent = crossed = passed = 0.0
    last = (starts[-1][1] * 4 * wide) + 60
    events = []
    for c, (begin, close) in enumerate(starts):
        size = close - begin
        sent = sent + 4 * wide * size
        landed = sent + 60
        crossed = max(crossed, landed) + 4 * far * size
        passed = max(passed, crossed + 40) + 4 * end * size
        sides = passed + 40
        done = max(sides + 8 * extra * size + 40, last + 1)
        for k, at in enumerate((0.0, landed, crossed + 40, sides, done)):
            events.append((at, k, c, acts[k]))
    return sorted(events, key=lambda e: e[:3])


def on_device(field, zone, slot, spins, tally):
    times, per_group, side, _ = field.shape
    columns = lax.axis_size("gx")
    rows = lax.axis_size("gy")
    pairs = columns // 2
    cap = 2 * per_group // rows
    per_pair = 4 * (2 * per_group // columns)
    chunks = chunk_units(times, side)
    tiles = [(len(chunk), PART, side) for chunk in chunks]
    balanced = rows == 4 and pairs == 4 and columns * per_group < 256 and 2 * rows * cap <= 128 and pairs * per_pair <= 128
    send = balanced_exchange if balanced else plain_exchange
    final = send(field, zone, slot, spins, chunks, tiles, cap, per_pair)
    return pl.pallas_call(
        functools.partial(finish, rows, chunks, balanced),
        grid_spec=pltpu.PrefetchScalarGridSpec(
            num_scalar_prefetch=1,
            grid=(cap,),
            in_specs=[pl.BlockSpec(
                (2, 1, rows) + tile,
                lambda s, count: (0, jnp.maximum(jnp.minimum(s, count[0] - 1), 0), 0, 0, 0, 0)) for tile in tiles],
            out_specs=pl.BlockSpec((rows * times, 1, 1, side, side), lambda s, count: (0, 0, s, 0, 0)),
        ),
        out_shape=jax.ShapeDtypeStruct((rows * times, 1, cap, side, side), jnp.float32),
        name="finish",
    )(tally, *final)


def scratch_of(tiles, *shapes):
    return [pltpu.VMEM(lead + tile, jnp.float32) for lead in shapes for tile in tiles]


def balanced_exchange(field, zone, slot, spins, chunks, tiles, cap, per_pair):
    times, per_group, side, _ = field.shape
    columns = lax.axis_size("gx")
    rows = lax.axis_size("gy")
    pairs = columns // 2
    tall = 2 * cap
    extra = cap // 3
    smem = pl.BlockSpec(memory_space=pltpu.SMEM)
    anywhere = pl.BlockSpec(memory_space=pl.ANY)
    whole = pl.BlockSpec((1, columns * per_group), lambda i: (0, 0))
    sizes = balanced_sizes(per_pair, tall)
    lanes = -(-columns * per_group // 128) * 128
    *turned, table, choice = pl.pallas_call(
        functools.partial(prepare_balanced, (pairs, rows, per_group, per_pair, cap, extra), sizes, chunks),
        grid=(per_group // STEP_BLOCKS,),
        in_specs=[whole, whole, smem, pl.BlockSpec((times, STEP_BLOCKS, side, side), lambda i: (0, i, 0, 0))],
        out_specs=[
            *[pl.BlockSpec((2, STEP_BLOCKS) + tile, lambda i: (0, i, 0, 0, 0)) for tile in tiles],
            pl.BlockSpec((8, 128), lambda i: (0, 0)), smem,
        ],
        out_shape=[
            *[jax.ShapeDtypeStruct((2, per_group) + tile, jnp.float32) for tile in tiles],
            jax.ShapeDtypeStruct((8, 128), jnp.int32),
            jax.ShapeDtypeStruct((1,), jnp.int32),
        ],
        scratch_shapes=[pltpu.VMEM((8, lanes), jnp.int32)],
        name="prepare",
    )(zone.reshape(1, -1), slot.reshape(1, -1), spins, field)

    starts = []
    for chunk in chunks:
        begin = starts[-1][1] if starts else 0
        starts.append((begin, begin + len(chunk)))
    count = len(chunks)

    def moved(wide, end, far, tag):
        dma = pltpu.SemaphoreType.DMA
        buffers = [
            *scratch_of(
                tiles, (2 * per_group,), (pairs - 1, wide), (pairs * per_pair,), (tall,), (rows, tall), (cap, rows),
                (cap, rows), (far,), (2, far), (2, end), (2, rows, extra), (2, rows, extra)),
            pltpu.SMEM((far,), jnp.int32),
            dma((count,)), dma((count,)), dma((count,)),
            dma((count, pairs - 1)), dma((count, pairs - 1)),
            dma((count,)), dma((count,)),
            dma((count,)), dma((count,)), dma((count,)),
            dma((count,)), dma((count, 2)),
            dma((count, 2)), dma((count, 2)), dma((count, 2)), dma((count, 2)),
        ]
        return lambda: pl.pallas_call(
            functools.partial(
                exchange_balanced, (pairs, rows, per_group, per_pair, cap, extra, wide, end, far, tuple(starts))),
            in_specs=[smem] + [anywhere] * count,
            out_specs=[anywhere] * count,
            out_shape=[jax.ShapeDtypeStruct((2, cap, rows) + tile, jnp.float32) for tile in tiles],
            scratch_shapes=buffers,
            compiler_params=pltpu.CompilerParams(collective_id=tag, has_side_effects=True, vmem_limit_bytes=62 * 2**20),
            name=f"exchange_{tag}",
        )(table, *turned)

    return lax.switch(choice[0], [moved(*size, tag) for tag, size in enumerate(sizes)])


def plain_exchange(field, zone, slot, spins, chunks, tiles, cap, per_pair):
    times, per_group, side, _ = field.shape
    columns = lax.axis_size("gx")
    rows = lax.axis_size("gy")
    pairs = columns // 2
    per_row = 2 * cap
    smem = pl.BlockSpec(memory_space=pltpu.SMEM)
    anywhere = pl.BlockSpec(memory_space=pl.ANY)
    i32 = jnp.int32
    narrow = levels(per_pair, (40,))[0]
    sizes = [(narrow, tall) for tall in levels(per_row, (36, 42))]
    sizes.append((per_pair, per_row))
    *turned, send_table, pick_table, tallies, choice = pl.pallas_call(
        functools.partial(prepare, (pairs, rows, per_group, per_pair, cap, chunks, sizes)),
        grid=(per_group // STEP_BLOCKS,),
        in_specs=[smem, smem, smem, pl.BlockSpec((times, STEP_BLOCKS, side, side), lambda i: (0, i, 0, 0))],
        out_specs=[
            *[pl.BlockSpec((2, STEP_BLOCKS) + tile, lambda i: (0, i, 0, 0, 0)) for tile in tiles],
            smem, smem, smem, smem,
        ],
        out_shape=[
            *[jax.ShapeDtypeStruct((2, per_group) + tile, jnp.float32) for tile in tiles],
            jax.ShapeDtypeStruct((pairs * per_pair + 1,), i32),
            jax.ShapeDtypeStruct((per_row * rows + 1,), i32),
            jax.ShapeDtypeStruct((2 * rows,), i32),
            jax.ShapeDtypeStruct((1,), i32),
        ],
        scratch_shapes=[pltpu.SMEM((columns * rows,), i32), pltpu.SMEM((pairs * pairs,), i32)],
        name="prepare",
    )(zone, slot, spins, field)
    count = len(chunks)

    def moved(wide, tall, tag):
        dma = pltpu.SemaphoreType.DMA
        buffers = [
            *scratch_of(
                tiles, (2 * per_group,), (pairs - 1, wide), (pairs * per_pair,), (rows - 1, tall), (rows, tall),
                (cap, rows), (cap, rows)),
            pltpu.SMEM((rows * tall,), i32),
            dma((count,)), dma((count,)), dma((count,)),
            dma((count, pairs - 1)), dma((count, pairs - 1)),
            dma((count, rows - 1)), dma((count, rows - 1)),
            dma((count,)), dma((count,)), dma((count,)),
        ]
        return lambda: pl.pallas_call(
            functools.partial(exchange, (pairs, rows, per_group, per_pair, wide, tall, cap, count)),
            in_specs=[smem, smem, smem] + [anywhere] * count,
            out_specs=[anywhere] * count,
            out_shape=[jax.ShapeDtypeStruct((2, cap, rows) + tile, jnp.float32) for tile in tiles],
            scratch_shapes=buffers,
            compiler_params=pltpu.CompilerParams(collective_id=tag, has_side_effects=True, vmem_limit_bytes=60 * 2**20),
            name=f"exchange_{tag}",
        )(send_table, pick_table, tallies, *turned)

    return lax.switch(choice[0], [moved(*size, tag) for tag, size in enumerate(sizes)])


def solution(mesh):
    placed = (P("gy", "gx", None, None), P(), P(), P(), P(("gx", "gy")))
    return jax.shard_map(
        on_device,
        mesh=mesh,
        in_specs=placed,
        out_specs=P(None, ("gx", "gy"), None, None, None),
        check_vma=False,
    )
```

```python
import functools

import jax
import jax.numpy as jnp
from jax import lax
from jax.experimental import pallas as pl
from jax.experimental.pallas import tpu as pltpu
from jax.sharding import PartitionSpec as P

MESH = pl.DeviceIdType.MESH
PART = 8
STEP_BLOCKS = 4


def chunk_units(times, side):
    units = [(r, t) for r in range(side // (2 * PART)) for t in range(times)]
    small = 2 * (times // 2 + times % 2)
    cuts = list(range(0, small + 1, max(times // 2, 1)))
    cuts += list(range(small + times, len(units) - small + 1, times))
    cuts += list(range(len(units) - small + max(times // 2, 1), len(units) + 1, max(times // 2, 1)))
    return [units[a:b] for a, b in zip(cuts[:-1], cuts[1:])]


def mirror_lanes(block):
    side = block.shape[1]
    lane = side - 1 - lax.broadcasted_iota(jnp.int32, block.shape, 1)
    return jnp.take_along_axis(block, lane, axis=1)


def turn_blocks(first, chunks, spins, field, turned):
    times, blocks, side, _ = field.shape
    for b in range(blocks):
        code = spins[first + b]
        for kind in range(4):
            @pl.when(code == kind)
            def _(kind=kind, b=b):
                for t in range(times):
                    block = field[t, b]
                    if kind == 1:
                        block = mirror_lanes(block).T
                    elif kind == 2:
                        block = mirror_lanes(mirror_lanes(block).T).T
                    elif kind == 3:
                        block = mirror_lanes(block.T)
                    for c, chunk in enumerate(chunks):
                        for i, (r, at) in enumerate(chunk):
                            if at == t:
                                for h in range(2):
                                    top = h * (side // 2) + r * PART
                                    turned[c][h, b, i] = block[top:top + PART]


def prepare(dims, zone, slot, spins, field, *refs):
    pairs, rows, per_group, per_pair, cap, chunks, sizes = dims
    turned = refs[:len(chunks)]
    send_table, pick_table, tallies, choice, counts, fills = refs[len(chunks):]
    gx = lax.axis_index("gx")
    pair = gx // 2
    group = 2 * per_group
    local = 2 * rows
    step = pl.program_id(0)

    @pl.when(step == 0)
    def _():
        def clear(ref, size):
            def body(i, c):
                ref[i] = 0
                return c
            lax.fori_loop(0, size, body, 0, unroll=8)
        clear(send_table, pairs * per_pair + 1)
        clear(pick_table, local * cap + 1)
        clear(counts, pairs * local)
        clear(fills, pairs * pairs)

        for source in range(pairs):
            behind = lax.rem(pair - source + pairs, pairs) * per_pair

            def place(j, c, source=source, behind=behind):
                region = zone[source * group + j]
                counts[region] = counts[region] + 1
                target = region // local
                cell = source * pairs + target
                rank = fills[cell]
                fills[cell] = rank + 1
                ahead = lax.rem(target - source + pairs, pairs) * per_pair
                send_table[jnp.where(source == pair, ahead + rank, pairs * per_pair)] = j
                at = (region - target * local) * cap + slot[source * group + j]
                pick_table[jnp.where(target == pair, at, local * cap)] = behind + rank
                return c
            lax.fori_loop(0, group, place, 0, unroll=4)
        most_pair = jnp.int32(0)
        most_row = jnp.int32(0)
        for q in range(pairs):
            for r in range(pairs):
                if q != r:
                    most_pair = jnp.maximum(most_pair, fills[q * pairs + r])
            pooled = [counts[q * local + r] + counts[q * local + rows + r] for r in range(rows)]
            for value in pooled:
                most_row = jnp.maximum(most_row, value)
        for r in range(local):
            tallies[r] = counts[pair * local + r]
        chosen = jnp.int32(len(sizes) - 1)
        for at in range(len(sizes) - 2, -1, -1):
            wide, tall = sizes[at]
            fits = jnp.logical_and(most_pair <= wide, most_row <= tall)
            chosen = jnp.where(fits, at, chosen)
        choice[0] = chosen

    turn_blocks(gx * per_group + step * field.shape[1], chunks, spins, field, turned)


def origin_of(z, rows, k, relay):
    if not relay:
        return lax.rem(z - k + rows, rows)
    low = z < 2
    return [z, z + 1 - 2 * lax.rem(z, 2), jnp.where(low, 2, 1), jnp.where(low, 3, 0)][k]


def exchange(dims, send_table, pick_table, tallies, *refs):
    pairs, rows, per_group, per_pair, wide, tall, cap, chunks = dims
    turned, final, scratch = refs[:chunks], refs[chunks:2 * chunks], refs[2 * chunks:]
    kinds = 7
    groups = [scratch[i * chunks:(i + 1) * chunks] for i in range(kinds)]
    held, packed, landed, lifted, risen, given, kept = groups
    sems = list(scratch[kinds * chunks:])
    row_list = sems.pop(0)
    own_sem, swap_send, swap_recv, pair_send, pair_recv, row_send, row_recv, give_send, give_recv, keep_sem = sems
    gx = lax.axis_index("gx")
    z = lax.axis_index("gy")
    pair = gx // 2
    half = lax.rem(gx, 2)
    mate = (2 * pair + 1 - half, z)

    def across(o):
        return (2 * lax.rem(pair + o, pairs) + half, z)

    def along(o):
        return (gx, lax.rem(z + o, rows))

    barrier = pltpu.get_barrier_semaphore()
    friends = [mate] + [across(o) for o in range(1, pairs)] + [along(o) for o in range(1, rows)]
    for friend in friends:
        pl.semaphore_signal(barrier, inc=1, device_id=friend, device_id_type=MESH)
    own_copies = []
    for c in range(chunks):
        own = pltpu.make_async_copy(turned[c].at[half], held[c].at[pl.ds(half * per_group, per_group)], own_sem.at[c])
        own.start()
        own_copies.append(own)
    pl.semaphore_wait(barrier, len(friends))

    swaps = []
    for c in range(chunks):
        swap = pltpu.make_async_remote_copy(
            src_ref=turned[c].at[1 - half], dst_ref=held[c].at[pl.ds(half * per_group, per_group)],
            send_sem=swap_send.at[c], recv_sem=swap_recv.at[c], device_id=mate, device_id_type=MESH)
        swap.start()
        swaps.append(swap)

    unsent = []
    pair_copies = []
    for c in range(chunks):
        own_copies[c].wait()
        swaps[c].wait_recv()
        unsent.append(swaps[c])
        sent = []
        for o in range(1, pairs):
            def pack(k, carry, o=o, c=c):
                packed[c][o - 1, k] = held[c][send_table[o * per_pair + k]]
                return carry
            lax.fori_loop(0, wide, pack, 0, unroll=4)
            copy = pltpu.make_async_remote_copy(
                src_ref=packed[c].at[o - 1], dst_ref=landed[c].at[pl.ds(o * per_pair, wide)],
                send_sem=pair_send.at[c, o - 1], recv_sem=pair_recv.at[c, o - 1],
                device_id=across(o), device_id_type=MESH)
            copy.start()
            sent.append(copy)
        unsent.extend(sent)

        def stay(k, carry, c=c):
            landed[c][k] = held[c][send_table[k]]
            return carry
        lax.fori_loop(0, per_pair, stay, 0, unroll=4)
        pair_copies.append(sent)

    for r in range(rows):
        first = tallies[r]

        def compact(k, carry, r=r, first=first):
            at = jnp.minimum(jnp.where(k < first, r * cap + k, (rows + r) * cap + k - first), 2 * rows * cap - 1)
            row_list[r * tall + k] = pick_table[at]
            return carry
        lax.fori_loop(0, tall, compact, 0, unroll=4)

    gives = []

    def settle_all(c):
        first = tallies[z]

        def settle(s, carry, c=c):
            mine = jnp.minimum(s + half * first, tall - 1)
            other = jnp.minimum(s + (1 - half) * first, tall - 1)
            for o in range(rows):
                given[c][s, o] = risen[c][o, other]
                kept[c][s, o] = risen[c][o, mine]
            return carry
        lax.fori_loop(0, cap, settle, 0)
        give = pltpu.make_async_remote_copy(
            src_ref=given[c], dst_ref=final[c].at[half],
            send_sem=give_send.at[c], recv_sem=give_recv.at[c], device_id=mate, device_id_type=MESH)
        give.start()
        keep = pltpu.make_async_copy(kept[c], final[c].at[half], keep_sem.at[c])
        keep.start()
        gives.append((give, keep))

    row_copies = []
    for c in range(chunks):
        for copy in pair_copies[c]:
            copy.wait_recv()
        sent = []
        for o in list(range(rows - 1, 0, -1)) + [0]:
            row = lax.rem(z + o, rows)

            def lift(k, carry, o=o, c=c, row=row):
                tile = landed[c][row_list[row * tall + k]]
                if o > 0:
                    lifted[c][o - 1, k] = tile
                else:
                    risen[c][0, k] = tile
                return carry
            lax.fori_loop(0, tall, lift, 0, unroll=4)
            if o > 0:
                copy = pltpu.make_async_remote_copy(
                    src_ref=lifted[c].at[o - 1], dst_ref=risen[c].at[o],
                    send_sem=row_send.at[c, o - 1], recv_sem=row_recv.at[c, o - 1],
                    device_id=along(o), device_id_type=MESH)
                copy.start()
                sent.append(copy)
        row_copies.append(sent)
        unsent.extend(sent)
    for c in range(chunks):
        for copy in row_copies[c]:
            copy.wait_recv()
        settle_all(c)
    for copy in unsent:
        copy.wait_send()
    for give, keep in gives:
        give.wait()
        keep.wait()


def finish(rows, chunks, relay, tally, *refs):
    final, regional = refs[:-1], refs[-1]
    z = lax.axis_index("gy")
    slot = pl.program_id(0)
    side = regional.shape[3]
    times = regional.shape[0] // rows
    place = {unit: (c, i) for c, chunk in enumerate(chunks) for i, unit in enumerate(chunk)}

    @pl.when(slot < tally[0])
    def _():
        for h in range(2):
            for r in range(side // (2 * PART)):
                span = pl.ds(h * (side // 2) + r * PART, PART)
                tiles = {}
                for t in range(times):
                    c, i = place[(r, t)]
                    for o in range(rows):
                        tiles[o, t] = final[c][h, 0, o, i]
                mean = sum(tiles.values()) * jnp.float32(1.0 / (rows * times))
                for o in range(rows):
                    start = origin_of(z, rows, o, relay) * times
                    for t in range(times):
                        regional[start + t, 0, 0, span, :] = tiles[o, t] - mean

    @pl.when(slot >= tally[0])
    def _():
        regional[...] = jnp.zeros_like(regional)


def levels(most, steps):
    return sorted({-(-most * s // 48) for s in steps})


def balanced_sizes(per_pair, tall):
    steps = ((36, 36, 54), (40, 38, 58), (40, 42, 62), (44, 44, 68), (48, 48, 96))
    return [(-(-per_pair * w // 48), -(-tall * e // 48), -(-tall * f // 48)) for w, e, f in steps]

def beside(x, step):
    return jnp.concatenate([x[step:], x[:step]], axis=0)


def plan_tables(dims, sizes, pair, zone, slot, allow):
    pairs, rows, per_group, per_pair, cap, extra = dims
    group, local, tall = 2 * per_group, 2 * rows, 2 * cap
    bins = pairs * rows
    width = zone.shape[1]
    i32, f32, bf16 = jnp.int32, jnp.float32, jnp.bfloat16
    lane = lax.broadcasted_iota(i32, (1, width), 1)
    valid = zone >= 0
    source = sum((lane >= group * k).astype(i32) for k in range(1, pairs))
    home = sum((zone >= local * k).astype(i32) for k in range(1, pairs))
    inside = zone - home * local
    side = (inside >= rows).astype(i32)
    row = inside - side * rows
    bin_at = lax.broadcasted_iota(i32, (bins, width), 0)
    before = (lax.broadcasted_iota(i32, (width, width), 0) < lax.broadcasted_iota(i32, (width, width), 1)).astype(bf16)

    def marks(key):
        return jnp.where(bin_at == jnp.where(valid, key, -1), 1.0, 0.0).astype(f32)

    def tally(mark):
        return jnp.sum(mark, axis=1, keepdims=True)

    def look(mark, table):
        return jnp.sum(mark * table, axis=0, keepdims=True)

    def ranks(mark):
        return jnp.dot(mark.astype(bf16), before, preferred_element_type=f32)

    at = lax.broadcasted_iota(i32, (bins, 128), 0)
    at_row = at & (rows - 1)
    at_home = at >> (rows.bit_length() - 1)
    edge = jnp.logical_or(at_row == 0, at_row == rows - 1)

    def flip(x, bit):
        step = 1 << bit
        if 2 * step == bins:
            return beside(x, step)
        return jnp.where((at & step) == 0, beside(x, step), beside(x, bins - step))

    across_x = lambda x: flip(x, 2)
    across_y = lambda x: flip(x, 3)
    mark = marks(home * rows + row)
    order = look(mark, ranks(mark))
    native = jnp.broadcast_to(tally(mark), (bins, 128)).astype(i32)

    def whole(x):
        x = x + across_x(x)
        return x + across_y(x)

    load = native
    half_sum = whole(native + flip(native, 0))
    goal = (jnp.maximum(half_sum, flip(half_sum, 1)) + pairs - 1) >> (pairs.bit_length() - 1)
    row_sum = (whole(native) + pairs - 1) >> (pairs.bit_length() - 1)
    end_goal = jnp.maximum(jnp.maximum(row_sum, flip(flip(row_sum, 0), 1)), (2 * goal * 171) >> 9)
    used = [jnp.zeros_like(native), jnp.zeros_like(native)]
    for _ in range(2):
        for d, partner in enumerate((across_x, across_y)):
            for stage in range(2):
                if stage == 0:
                    now, want, here = load, end_goal, edge
                else:
                    now, want, here = load + flip(load, 0), goal, jnp.logical_not(edge)
                move = jnp.minimum((now - partner(now)) >> 1, now - want)
                move = jnp.minimum(move, jnp.minimum(extra - used[d], native - used[0] - used[1]))
                move = jnp.where(here, jnp.maximum(move, 0), 0)
                used[d] = used[d] + move
                load = load + partner(move) - move
    first = look(mark, (used[0] * allow)[:, :1].astype(f32))
    second = look(mark, (used[1] * allow)[:, :1].astype(f32))
    leaves_x = order < first
    leaves_y = jnp.logical_and(order >= first, order < first + second)
    way = leaves_y.astype(i32)
    guest = order - jnp.where(leaves_y, first, 0.0)
    home_x = home & 1
    home_y = home >> 1
    via = jnp.where(leaves_x, home_y * 2 + 1 - home_x, jnp.where(leaves_y, (1 - home_y) * 2 + home_x, home))

    flow = marks(source * pairs + via)
    line = marks(via * rows + row)
    both = ranks(jnp.concatenate([flow, line], axis=0))
    rank = look(flow, both[:bins])
    place = look(line, both[bins:])
    flows = jnp.broadcast_to(tally(flow), (bins, 128))
    lines = jnp.broadcast_to(tally(line), (bins, 128))
    halves = lines + flip(lines, 0)
    stays = at_home == at_row
    chosen = jnp.zeros((1, 128), f32)
    for wide, end, far in sizes:
        over = jnp.where(flows > jnp.where(stays, per_pair, wide).astype(f32), 1.0, 0.0)
        over = jnp.maximum(over, jnp.where(lines > jnp.where(edge, end, tall).astype(f32), 1.0, 0.0))
        over = jnp.maximum(over, jnp.where(halves > jnp.float32(far), 1.0, 0.0))
        chosen = chosen + jnp.max(over, axis=0, keepdims=True)

    my_x, my_y = pair % 2, pair // 2

    def offset(other):
        other_y = other >> 1
        other_x = other - 2 * other_y
        return jnp.where(other_x == my_x, 0, 1) + jnp.where(other_y == my_y, 0, 2)

    def invert(here, key, value):
        key = jnp.where(jnp.logical_and(valid, here), key, -1)
        hit = jnp.where(lax.broadcasted_iota(i32, (128, width), 0) == key, 1.0, 0.0).astype(bf16)
        value = jnp.broadcast_to(value.astype(bf16), (16, width))
        return lax.dot_general(value, hit, (((1,), (1,)), ((), ())), preferred_element_type=f32)[:1]

    rank = rank.astype(i32)
    place = place.astype(i32)
    guest = guest.astype(i32)
    landing = offset(source) * per_pair + rank
    mine = via == pair
    ours = home == pair
    return chosen, [
        invert(source == pair, offset(via) * per_pair + rank, (lane - group * pair).astype(f32)),
        invert(mine, row * tall + place, landing.astype(f32)),
        invert(jnp.logical_and(mine, home != pair), (way * rows + row) * extra + guest, place.astype(f32)),
        invert(ours, (side * rows + row) * cap + slot, jnp.where(mine, place, tall + way * extra + guest).astype(f32)),
        invert(mine, row, jnp.ones((1, width), f32)),
    ]


def prepare_balanced(dims, sizes, chunks, zone, slot, spins, field, *refs):
    per_group = dims[2]
    turned = refs[:len(chunks)]
    table, choice, padded = refs[len(chunks):]
    gx = lax.axis_index("gx")
    step = pl.program_id(0)

    @pl.when(step == 0)
    def _():
        padded[...] = jnp.full_like(padded, -1)
        padded[0:1, 0:zone.shape[1]] = zone[...]
        padded[1:2, 0:zone.shape[1]] = slot[...]

        def fill(sizes, allow):
            chosen, rows_of = plan_tables(dims, sizes, gx // 2, padded[0:1], padded[1:2], allow)
            for k, line in enumerate(rows_of):
                table[k:k + 1] = line.astype(jnp.int32)
            return jnp.max(chosen).astype(jnp.int32)

        chosen = fill(sizes, 1)
        choice[0] = jnp.minimum(chosen, len(sizes) - 1)

        @pl.when(chosen == len(sizes))
        def _():
            fill(sizes[:0], 0)

    turn_blocks(gx * per_group + step * field.shape[1], chunks, spins, field, turned)


def exchange_balanced(dims, table, *refs):
    pairs, rows, per_group, per_pair, cap, extra, wide, end, far, starts = dims
    tall = 2 * cap
    chunks = len(starts)
    turned, final, scratch = refs[:chunks], refs[chunks:2 * chunks], refs[2 * chunks:]
    kinds = 12
    groups = [scratch[i * chunks:(i + 1) * chunks] for i in range(kinds)]
    held, packed, landed, lifted, risen, given, kept, pooled, crossed, passed, leaving, visiting = groups
    sems = list(scratch[kinds * chunks:])
    far_list = sems.pop(0)
    own_sem, swap_send, swap_recv, pair_send, pair_recv, near_send, near_recv = sems[:7]
    give_send, give_recv, keep_sem, far_send, far_recv, pass_send, pass_recv, side_send, side_recv = sems[7:]
    gx = lax.axis_index("gx")
    z = lax.axis_index("gy")
    pair = gx // 2
    half = lax.rem(gx, 2)
    mate = (2 * pair + 1 - half, z)
    pair_x = lax.rem(pair, 2)
    pair_y = pair // 2
    near, far_in, far_out = (origin_of(z, rows, k, True) for k in (1, 2, 3))
    inner = jnp.logical_or(z == 1, z == 2)
    outer = jnp.logical_not(inner)
    role = jnp.where(inner, 0, 1)

    def across(o):
        x = 1 - pair_x if o % 2 else pair_x
        y = 1 - pair_y if o // 2 else pair_y
        return (2 * (2 * y + x) + half, z)

    barrier = pltpu.get_barrier_semaphore()
    friends = [mate] + [across(o) for o in range(1, pairs)] + [(gx, lax.rem(z + o, rows)) for o in range(1, rows)]
    for friend in friends:
        pl.semaphore_signal(barrier, inc=1, device_id=friend, device_id_type=MESH)
    own_copies = []
    for c in range(chunks):
        own = pltpu.make_async_copy(turned[c].at[half], held[c].at[pl.ds(half * per_group, per_group)], own_sem.at[c])
        own.start()
        own_copies.append(own)
    pl.semaphore_wait(barrier, len(friends))

    swaps = []
    for c in range(chunks):
        swap = pltpu.make_async_remote_copy(
            src_ref=turned[c].at[1 - half], dst_ref=held[c].at[pl.ds(half * per_group, per_group)],
            send_sem=swap_send.at[c], recv_sem=swap_recv.at[c], device_id=mate, device_id_type=MESH)
        swap.start()
        swaps.append(swap)

    unsent = []
    pair_copies = {}

    def send_pairs(c):
        own_copies[c].wait()
        swaps[c].wait_recv()
        unsent.append(swaps[c])
        sent = []
        for o in range(1, pairs):
            def pack(k, carry, o=o):
                packed[c][o - 1, k] = held[c][table[0, o * per_pair + k]]
                return carry
            lax.fori_loop(0, wide, pack, 0, unroll=4)
            sent.append(pltpu.make_async_remote_copy(
                src_ref=packed[c].at[o - 1], dst_ref=landed[c].at[pl.ds(o * per_pair, wide)],
                send_sem=pair_send.at[c, o - 1], recv_sem=pair_recv.at[c, o - 1],
                device_id=across(o), device_id_type=MESH))
        unsent.extend(sent)
        pair_copies[c] = sent

        @pl.when(half == 0)
        def _():
            for copy in sent:
                copy.start()

        @pl.when(half == 1)
        def _():
            for copy in sent[::-1]:
                copy.start()

        def stay(k, carry):
            landed[c][k] = held[c][table[0, k]]
            return carry
        lax.fori_loop(0, per_pair, stay, 0, unroll=4)

        if c == 0:
            lead = table[4, far_in]

            def gather_far(k, carry):
                at = jnp.where(k < lead, far_in * tall + k, far_out * tall + k - lead)
                far_list[k] = table[1, jnp.minimum(at, rows * tall - 1)]
                return carry
            lax.fori_loop(0, far, gather_far, 0, unroll=4)

    skip = table[4, z]

    def near_copy(c, size):
        return pltpu.make_async_remote_copy(
            src_ref=lifted[c].at[pl.ds(0, size)], dst_ref=risen[c].at[1, pl.ds(0, size)],
            send_sem=near_send.at[c], recv_sem=near_recv.at[c],
            device_id=(gx, near), device_id_type=MESH)

    def far_copy(c, place):
        return pltpu.make_async_remote_copy(
            src_ref=pooled[c], dst_ref=crossed[c].at[place],
            send_sem=far_send.at[c], recv_sem=far_recv.at[c, place],
            device_id=(gx, far_in), device_id_type=MESH)

    def pass_copy(c, place):
        return pltpu.make_async_remote_copy(
            src_ref=passed[c].at[place], dst_ref=risen[c].at[2 + place, pl.ds(0, end)],
            send_sem=pass_send.at[c, place], recv_sem=pass_recv.at[c, place],
            device_id=(gx, near), device_id_type=MESH)

    def side_copy(c, d):
        return pltpu.make_async_remote_copy(
            src_ref=leaving[c].at[d], dst_ref=visiting[c].at[d],
            send_sem=side_send.at[c, d], recv_sem=side_recv.at[c, d],
            device_id=across(1 + d), device_id_type=MESH)

    def send_rows(c):
        for copy in pair_copies[c]:
            copy.wait_recv()

        def pool(k, carry):
            pooled[c][k] = landed[c][far_list[k]]
            return carry
        lax.fori_loop(0, far, pool, 0, unroll=4)

        def lift(k, carry):
            lifted[c][k] = landed[c][table[1, near * tall + k]]
            return carry
        lax.fori_loop(0, tall, lift, 0, unroll=4)
        unsent.append(far_copy(c, role))

        @pl.when(half == 0)
        def _():
            far_copy(c, role).start()

        @pl.when(inner)
        def _():
            near_copy(c, end).start()

        @pl.when(outer)
        def _():
            near_copy(c, tall).start()

        @pl.when(half == 1)
        def _():
            far_copy(c, role).start()

        def own(k, carry):
            risen[c][0, k] = landed[c][table[1, z * tall + k]]
            return carry
        lax.fori_loop(0, tall, own, 0, unroll=4)

    def hand_on(c):
        @pl.when(inner)
        def _():
            for place in range(2):
                far_copy(c, place).wait_recv()
            for place in range(2):
                def onward(k, carry, place=place):
                    passed[c][place, k] = crossed[c][place, jnp.minimum(skip + k, far - 1)]
                    return carry
                lax.fori_loop(0, end, onward, 0, unroll=4)
                pass_copy(c, place).start()

                def land(k, carry, place=place):
                    risen[c][2 + place, k] = crossed[c][place, k]
                    return carry
                lax.fori_loop(0, tall, land, 0, unroll=4)

    def send_sides(c):
        @pl.when(inner)
        def _():
            near_copy(c, tall).wait_recv()

        @pl.when(outer)
        def _():
            near_copy(c, end).wait_recv()
            for place in range(2):
                pass_copy(c, place).wait_recv()

        for d in range(2):
            def leave(k, carry, d=d):
                at = table[2, (d * rows + z) * extra + k]
                for o in range(rows):
                    leaving[c][d, o, k] = risen[c][o, at]
                return carry
            lax.fori_loop(0, extra, leave, 0)
            side_copy(c, d).start()
            unsent.append(side_copy(c, d))

    gives = []

    def settle(c):
        for d in range(2):
            side_copy(c, d).wait_recv()

        def place(s, carry):
            for side, out in ((1 - half, given), (half, kept)):
                at = table[3, (side * rows + z) * cap + s]
                guest = jnp.maximum(at - tall, 0)
                way = guest // extra
                for o in range(rows):
                    home = risen[c][o, jnp.minimum(at, tall - 1)]
                    visitor = visiting[c][way, o, guest - way * extra]
                    out[c][s, o] = jnp.where(at < tall, home, visitor)
            return carry
        lax.fori_loop(0, cap, place, 0)
        give = pltpu.make_async_remote_copy(
            src_ref=given[c], dst_ref=final[c].at[half],
            send_sem=give_send.at[c], recv_sem=give_recv.at[c], device_id=mate, device_id_type=MESH)
        give.start()
        keep = pltpu.make_async_copy(kept[c], final[c].at[half], keep_sem.at[c])
        keep.start()
        gives.append((give, keep))

    for _, _, c, act in timetable(starts, wide, end, far, extra, (send_pairs, send_rows, hand_on, send_sides, settle)):
        act(c)

    @pl.when(inner)
    def _():
        for c in range(chunks):
            near_copy(c, end).wait_send()
            for place in range(2):
                pass_copy(c, place).wait_send()

    @pl.when(outer)
    def _():
        for c in range(chunks):
            near_copy(c, tall).wait_send()

    for copy in unsent:
        copy.wait_send()
    for give, keep in gives:
        give.wait()
        keep.wait()


def timetable(starts, wide, end, far, extra, acts):
    sent = crossed = passed = 0.0
    last = (starts[-1][1] * 4 * wide) + 60
    events = []
    for c, (begin, close) in enumerate(starts):
        size = close - begin
        sent = sent + 4 * wide * size
        landed = sent + 60
        crossed = max(crossed, landed) + 4 * far * size
        passed = max(passed, crossed + 40) + 4 * end * size
        sides = passed + 40
        done = max(sides + 8 * extra * size + 40, last + 1)
        for k, at in enumerate((0.0, landed, crossed + 40, sides, done)):
            events.append((at, k, c, acts[k]))
    return sorted(events, key=lambda e: e[:3])


def on_device(field, zone, slot, spins, tally):
    times, per_group, side, _ = field.shape
    columns = lax.axis_size("gx")
    rows = lax.axis_size("gy")
    pairs = columns // 2
    cap = 2 * per_group // rows
    per_pair = 4 * (2 * per_group // columns)
    chunks = chunk_units(times, side)
    tiles = [(len(chunk), PART, side) for chunk in chunks]
    balanced = rows == 4 and pairs == 4 and columns * per_group < 256 and 2 * rows * cap <= 128 and pairs * per_pair <= 128
    send = balanced_exchange if balanced else plain_exchange
    final = send(field, zone, slot, spins, chunks, tiles, cap, per_pair)
    return pl.pallas_call(
        functools.partial(finish, rows, chunks, balanced),
        grid_spec=pltpu.PrefetchScalarGridSpec(
            num_scalar_prefetch=1,
            grid=(cap,),
            in_specs=[pl.BlockSpec(
                (2, 1, rows) + tile,
                lambda s, count: (0, jnp.maximum(jnp.minimum(s, count[0] - 1), 0), 0, 0, 0, 0)) for tile in tiles],
            out_specs=pl.BlockSpec((rows * times, 1, 1, side, side), lambda s, count: (0, 0, s, 0, 0)),
        ),
        out_shape=jax.ShapeDtypeStruct((rows * times, 1, cap, side, side), jnp.float32),
        name="finish",
    )(tally, *final)


def scratch_of(tiles, *shapes):
    return [pltpu.VMEM(lead + tile, jnp.float32) for lead in shapes for tile in tiles]


def balanced_exchange(field, zone, slot, spins, chunks, tiles, cap, per_pair):
    times, per_group, side, _ = field.shape
    columns = lax.axis_size("gx")
    rows = lax.axis_size("gy")
    pairs = columns // 2
    tall = 2 * cap
    extra = cap // 3
    smem = pl.BlockSpec(memory_space=pltpu.SMEM)
    anywhere = pl.BlockSpec(memory_space=pl.ANY)
    whole = pl.BlockSpec((1, columns * per_group), lambda i: (0, 0))
    sizes = balanced_sizes(per_pair, tall)
    lanes = -(-columns * per_group // 128) * 128
    *turned, table, choice = pl.pallas_call(
        functools.partial(prepare_balanced, (pairs, rows, per_group, per_pair, cap, extra), sizes, chunks),
        grid=(per_group // STEP_BLOCKS,),
        in_specs=[whole, whole, smem, pl.BlockSpec((times, STEP_BLOCKS, side, side), lambda i: (0, i, 0, 0))],
        out_specs=[
            *[pl.BlockSpec((2, STEP_BLOCKS) + tile, lambda i: (0, i, 0, 0, 0)) for tile in tiles],
            pl.BlockSpec((8, 128), lambda i: (0, 0)), smem,
        ],
        out_shape=[
            *[jax.ShapeDtypeStruct((2, per_group) + tile, jnp.float32) for tile in tiles],
            jax.ShapeDtypeStruct((8, 128), jnp.int32),
            jax.ShapeDtypeStruct((1,), jnp.int32),
        ],
        scratch_shapes=[pltpu.VMEM((8, lanes), jnp.int32)],
        name="prepare",
    )(zone.reshape(1, -1), slot.reshape(1, -1), spins, field)

    starts = []
    for chunk in chunks:
        begin = starts[-1][1] if starts else 0
        starts.append((begin, begin + len(chunk)))
    count = len(chunks)

    def moved(wide, end, far, tag):
        dma = pltpu.SemaphoreType.DMA
        buffers = [
            *scratch_of(
                tiles, (2 * per_group,), (pairs - 1, wide), (pairs * per_pair,), (tall,), (rows, tall), (cap, rows),
                (cap, rows), (far,), (2, far), (2, end), (2, rows, extra), (2, rows, extra)),
            pltpu.SMEM((far,), jnp.int32),
            dma((count,)), dma((count,)), dma((count,)),
            dma((count, pairs - 1)), dma((count, pairs - 1)),
            dma((count,)), dma((count,)),
            dma((count,)), dma((count,)), dma((count,)),
            dma((count,)), dma((count, 2)),
            dma((count, 2)), dma((count, 2)), dma((count, 2)), dma((count, 2)),
        ]
        return lambda: pl.pallas_call(
            functools.partial(
                exchange_balanced, (pairs, rows, per_group, per_pair, cap, extra, wide, end, far, tuple(starts))),
            in_specs=[smem] + [anywhere] * count,
            out_specs=[anywhere] * count,
            out_shape=[jax.ShapeDtypeStruct((2, cap, rows) + tile, jnp.float32) for tile in tiles],
            scratch_shapes=buffers,
            compiler_params=pltpu.CompilerParams(collective_id=tag, has_side_effects=True, vmem_limit_bytes=62 * 2**20),
            name=f"exchange_{tag}",
        )(table, *turned)

    return lax.switch(choice[0], [moved(*size, tag) for tag, size in enumerate(sizes)])


def plain_exchange(field, zone, slot, spins, chunks, tiles, cap, per_pair):
    times, per_group, side, _ = field.shape
    columns = lax.axis_size("gx")
    rows = lax.axis_size("gy")
    pairs = columns // 2
    per_row = 2 * cap
    smem = pl.BlockSpec(memory_space=pltpu.SMEM)
    anywhere = pl.BlockSpec(memory_space=pl.ANY)
    i32 = jnp.int32
    narrow = levels(per_pair, (40,))[0]
    sizes = [(narrow, tall) for tall in levels(per_row, (36, 42))]
    sizes.append((per_pair, per_row))
    *turned, send_table, pick_table, tallies, choice = pl.pallas_call(
        functools.partial(prepare, (pairs, rows, per_group, per_pair, cap, chunks, sizes)),
        grid=(per_group // STEP_BLOCKS,),
        in_specs=[smem, smem, smem, pl.BlockSpec((times, STEP_BLOCKS, side, side), lambda i: (0, i, 0, 0))],
        out_specs=[
            *[pl.BlockSpec((2, STEP_BLOCKS) + tile, lambda i: (0, i, 0, 0, 0)) for tile in tiles],
            smem, smem, smem, smem,
        ],
        out_shape=[
            *[jax.ShapeDtypeStruct((2, per_group) + tile, jnp.float32) for tile in tiles],
            jax.ShapeDtypeStruct((pairs * per_pair + 1,), i32),
            jax.ShapeDtypeStruct((per_row * rows + 1,), i32),
            jax.ShapeDtypeStruct((2 * rows,), i32),
            jax.ShapeDtypeStruct((1,), i32),
        ],
        scratch_shapes=[pltpu.SMEM((columns * rows,), i32), pltpu.SMEM((pairs * pairs,), i32)],
        name="prepare",
    )(zone, slot, spins, field)
    count = len(chunks)

    def moved(wide, tall, tag):
        dma = pltpu.SemaphoreType.DMA
        buffers = [
            *scratch_of(
                tiles, (2 * per_group,), (pairs - 1, wide), (pairs * per_pair,), (rows - 1, tall), (rows, tall),
                (cap, rows), (cap, rows)),
            pltpu.SMEM((rows * tall,), i32),
            dma((count,)), dma((count,)), dma((count,)),
            dma((count, pairs - 1)), dma((count, pairs - 1)),
            dma((count, rows - 1)), dma((count, rows - 1)),
            dma((count,)), dma((count,)), dma((count,)),
        ]
        return lambda: pl.pallas_call(
            functools.partial(exchange, (pairs, rows, per_group, per_pair, wide, tall, cap, count)),
            in_specs=[smem, smem, smem] + [anywhere] * count,
            out_specs=[anywhere] * count,
            out_shape=[jax.ShapeDtypeStruct((2, cap, rows) + tile, jnp.float32) for tile in tiles],
            scratch_shapes=buffers,
            compiler_params=pltpu.CompilerParams(collective_id=tag, has_side_effects=True, vmem_limit_bytes=60 * 2**20),
            name=f"exchange_{tag}",
        )(send_table, pick_table, tallies, *turned)

    return lax.switch(choice[0], [moved(*size, tag) for tag, size in enumerate(sizes)])


def solution(mesh):
    placed = (P("gy", "gx", None, None), P(), P(), P(), P(("gx", "gy")))
    return jax.shard_map(
        on_device,
        mesh=mesh,
        in_specs=placed,
        out_specs=P(None, ("gx", "gy"), None, None, None),
        check_vma=False,
    )
```

```python
import functools

import jax
import jax.numpy as jnp
from jax import lax
from jax.experimental import pallas as pl
from jax.experimental.pallas import tpu as pltpu
from jax.sharding import PartitionSpec as P

MESH = pl.DeviceIdType.MESH
PART = 8
STEP_BLOCKS = 4
LOADS = 2
VMEM_BYTES = 52 * 2**20


def chunk_units(times, side):
    units = [(r, t) for r in range(side // (2 * PART)) for t in range(times)]
    small = 2 * (times // 2 + times % 2)
    cuts = list(range(0, small + 1, max(times // 2, 1)))
    cuts += list(range(small + times, len(units) - small + 1, times))
    cuts += list(range(len(units) - small + max(times // 2, 1), len(units) + 1, max(times // 2, 1)))
    return [units[a:b] for a, b in zip(cuts[:-1], cuts[1:])]


def time_major(times, side):
    units = [(r, t) for t in range(times) for r in range(side // (2 * PART))]
    sizes = [1, 1] + [2] * ((len(units) - 4) // 2) + [1, 1]
    cuts = [sum(sizes[:c]) for c in range(len(sizes) + 1)]
    return [units[a:b] for a, b in zip(cuts[:-1], cuts[1:])]


def mirror_lanes(block):
    side = block.shape[1]
    lane = side - 1 - lax.broadcasted_iota(jnp.int32, block.shape, 1)
    return jnp.take_along_axis(block, lane, axis=1)


def turn_blocks(first, chunks, spins, field, turned):
    times, blocks, side, _ = field.shape
    for b in range(blocks):
        code = spins[first + b]
        for kind in range(4):
            @pl.when(code == kind)
            def _(kind=kind, b=b):
                for t in range(times):
                    block = field[t, b]
                    if kind == 1:
                        block = mirror_lanes(block).T
                    elif kind == 2:
                        block = mirror_lanes(mirror_lanes(block).T).T
                    elif kind == 3:
                        block = mirror_lanes(block.T)
                    for c, chunk in enumerate(chunks):
                        for i, (r, at) in enumerate(chunk):
                            if at == t:
                                for h in range(2):
                                    top = h * (side // 2) + r * PART
                                    turned[c][h, b, i] = block[top:top + PART]


def prepare(dims, zone, slot, spins, field, *refs):
    pairs, rows, per_group, per_pair, cap, chunks, sizes = dims
    turned = refs[:len(chunks)]
    send_table, pick_table, tallies, choice, counts, fills = refs[len(chunks):]
    gx = lax.axis_index("gx")
    pair = gx // 2
    group = 2 * per_group
    local = 2 * rows
    step = pl.program_id(0)

    @pl.when(step == 0)
    def _():
        def clear(ref, size):
            def body(i, c):
                ref[i] = 0
                return c
            lax.fori_loop(0, size, body, 0, unroll=8)
        clear(send_table, pairs * per_pair + 1)
        clear(pick_table, local * cap + 1)
        clear(counts, pairs * local)
        clear(fills, pairs * pairs)

        for source in range(pairs):
            behind = lax.rem(pair - source + pairs, pairs) * per_pair

            def place(j, c, source=source, behind=behind):
                region = zone[source * group + j]
                counts[region] = counts[region] + 1
                target = region // local
                cell = source * pairs + target
                rank = fills[cell]
                fills[cell] = rank + 1
                ahead = lax.rem(target - source + pairs, pairs) * per_pair
                send_table[jnp.where(source == pair, ahead + rank, pairs * per_pair)] = j
                at = (region - target * local) * cap + slot[source * group + j]
                pick_table[jnp.where(target == pair, at, local * cap)] = behind + rank
                return c
            lax.fori_loop(0, group, place, 0, unroll=4)
        most_pair = jnp.int32(0)
        most_row = jnp.int32(0)
        for q in range(pairs):
            for r in range(pairs):
                if q != r:
                    most_pair = jnp.maximum(most_pair, fills[q * pairs + r])
            pooled = [counts[q * local + r] + counts[q * local + rows + r] for r in range(rows)]
            for value in pooled:
                most_row = jnp.maximum(most_row, value)
        for r in range(local):
            tallies[r] = counts[pair * local + r]
        chosen = jnp.int32(len(sizes) - 1)
        for at in range(len(sizes) - 2, -1, -1):
            wide, tall = sizes[at]
            fits = jnp.logical_and(most_pair <= wide, most_row <= tall)
            chosen = jnp.where(fits, at, chosen)
        choice[0] = chosen

    turn_blocks(gx * per_group + step * field.shape[1], chunks, spins, field, turned)


def origin_of(z, rows, k, relay):
    if not relay:
        return lax.rem(z - k + rows, rows)
    low = z < 2
    return [z, z + 1 - 2 * lax.rem(z, 2), jnp.where(low, 2, 1), jnp.where(low, 3, 0)][k]


def exchange(dims, send_table, pick_table, tallies, *refs):
    pairs, rows, per_group, per_pair, wide, tall, cap, chunks = dims
    turned, final, scratch = refs[:chunks], refs[chunks:2 * chunks], refs[2 * chunks:]
    kinds = 7
    groups = [scratch[i * chunks:(i + 1) * chunks] for i in range(kinds)]
    held, packed, landed, lifted, risen, given, kept = groups
    sems = list(scratch[kinds * chunks:])
    row_list = sems.pop(0)
    own_sem, swap_send, swap_recv, pair_send, pair_recv, row_send, row_recv, give_send, give_recv, keep_sem = sems
    gx = lax.axis_index("gx")
    z = lax.axis_index("gy")
    pair = gx // 2
    half = lax.rem(gx, 2)
    mate = (2 * pair + 1 - half, z)

    def across(o):
        return (2 * lax.rem(pair + o, pairs) + half, z)

    def along(o):
        return (gx, lax.rem(z + o, rows))

    barrier = pltpu.get_barrier_semaphore()
    friends = [mate] + [across(o) for o in range(1, pairs)] + [along(o) for o in range(1, rows)]
    for friend in friends:
        pl.semaphore_signal(barrier, inc=1, device_id=friend, device_id_type=MESH)
    own_copies = []
    for c in range(chunks):
        own = pltpu.make_async_copy(turned[c].at[half], held[c].at[pl.ds(half * per_group, per_group)], own_sem.at[c])
        own.start()
        own_copies.append(own)
    pl.semaphore_wait(barrier, len(friends))

    swaps = []
    for c in range(chunks):
        swap = pltpu.make_async_remote_copy(
            src_ref=turned[c].at[1 - half], dst_ref=held[c].at[pl.ds(half * per_group, per_group)],
            send_sem=swap_send.at[c], recv_sem=swap_recv.at[c], device_id=mate, device_id_type=MESH)
        swap.start()
        swaps.append(swap)

    unsent = []
    pair_copies = []
    for c in range(chunks):
        own_copies[c].wait()
        swaps[c].wait_recv()
        unsent.append(swaps[c])
        sent = []
        for o in range(1, pairs):
            def pack(k, carry, o=o, c=c):
                packed[c][o - 1, k] = held[c][send_table[o * per_pair + k]]
                return carry
            lax.fori_loop(0, wide, pack, 0, unroll=4)
            copy = pltpu.make_async_remote_copy(
                src_ref=packed[c].at[o - 1], dst_ref=landed[c].at[pl.ds(o * per_pair, wide)],
                send_sem=pair_send.at[c, o - 1], recv_sem=pair_recv.at[c, o - 1],
                device_id=across(o), device_id_type=MESH)
            copy.start()
            sent.append(copy)
        unsent.extend(sent)

        def stay(k, carry, c=c):
            landed[c][k] = held[c][send_table[k]]
            return carry
        lax.fori_loop(0, per_pair, stay, 0, unroll=4)
        pair_copies.append(sent)

    for r in range(rows):
        first = tallies[r]

        def compact(k, carry, r=r, first=first):
            at = jnp.minimum(jnp.where(k < first, r * cap + k, (rows + r) * cap + k - first), 2 * rows * cap - 1)
            row_list[r * tall + k] = pick_table[at]
            return carry
        lax.fori_loop(0, tall, compact, 0, unroll=4)

    gives = []

    def settle_all(c):
        first = tallies[z]

        def settle(s, carry, c=c):
            mine = jnp.minimum(s + half * first, tall - 1)
            other = jnp.minimum(s + (1 - half) * first, tall - 1)
            for o in range(rows):
                given[c][s, o] = risen[c][o, other]
                kept[c][s, o] = risen[c][o, mine]
            return carry
        lax.fori_loop(0, cap, settle, 0)
        give = pltpu.make_async_remote_copy(
            src_ref=given[c], dst_ref=final[c].at[half],
            send_sem=give_send.at[c], recv_sem=give_recv.at[c], device_id=mate, device_id_type=MESH)
        give.start()
        keep = pltpu.make_async_copy(kept[c], final[c].at[half], keep_sem.at[c])
        keep.start()
        gives.append((give, keep))

    row_copies = []
    for c in range(chunks):
        for copy in pair_copies[c]:
            copy.wait_recv()
        sent = []
        for o in list(range(rows - 1, 0, -1)) + [0]:
            row = lax.rem(z + o, rows)

            def lift(k, carry, o=o, c=c, row=row):
                tile = landed[c][row_list[row * tall + k]]
                if o > 0:
                    lifted[c][o - 1, k] = tile
                else:
                    risen[c][0, k] = tile
                return carry
            lax.fori_loop(0, tall, lift, 0, unroll=4)
            if o > 0:
                copy = pltpu.make_async_remote_copy(
                    src_ref=lifted[c].at[o - 1], dst_ref=risen[c].at[o],
                    send_sem=row_send.at[c, o - 1], recv_sem=row_recv.at[c, o - 1],
                    device_id=along(o), device_id_type=MESH)
                copy.start()
                sent.append(copy)
        row_copies.append(sent)
        unsent.extend(sent)
    for c in range(chunks):
        for copy in row_copies[c]:
            copy.wait_recv()
        settle_all(c)
    for copy in unsent:
        copy.wait_send()
    for give, keep in gives:
        give.wait()
        keep.wait()


def finish(rows, chunks, tally, *refs):
    final, regional = refs[:-1], refs[-1]
    z = lax.axis_index("gy")
    slot = pl.program_id(0)
    side = regional.shape[3]
    times = regional.shape[0] // rows
    place = {unit: (c, i) for c, chunk in enumerate(chunks) for i, unit in enumerate(chunk)}

    @pl.when(slot < tally[0])
    def _():
        for h in range(2):
            for r in range(side // (2 * PART)):
                span = pl.ds(h * (side // 2) + r * PART, PART)
                tiles = {}
                for t in range(times):
                    c, i = place[(r, t)]
                    for o in range(rows):
                        tiles[o, t] = final[c][h, 0, o, i]
                mean = sum(tiles.values()) * jnp.float32(1.0 / (rows * times))
                for o in range(rows):
                    start = origin_of(z, rows, o, False) * times
                    for t in range(times):
                        regional[start + t, 0, 0, span, :] = tiles[o, t] - mean

    @pl.when(slot >= tally[0])
    def _():
        regional[...] = jnp.zeros_like(regional)


def levels(most, steps):
    return sorted({-(-most * s // 48) for s in steps})


def balanced_sizes(per_pair, tall):
    steps = ((36, 36, 54), (40, 38, 58), (40, 42, 62), (44, 44, 68), (48, 48, 96))
    return [(-(-per_pair * w // 48), -(-tall * e // 48), -(-tall * f // 48)) for w, e, f in steps]

def beside(x, step):
    return jnp.concatenate([x[step:], x[:step]], axis=0)


def plan_tables(dims, sizes, pair, zone, slot, allow):
    pairs, rows, per_group, per_pair, cap, extra = dims
    group, local, tall = 2 * per_group, 2 * rows, 2 * cap
    bins = pairs * rows
    width = zone.shape[1]
    i32, f32, bf16 = jnp.int32, jnp.float32, jnp.bfloat16
    lane = lax.broadcasted_iota(i32, (1, width), 1)
    valid = zone >= 0
    source = sum((lane >= group * k).astype(i32) for k in range(1, pairs))
    home = sum((zone >= local * k).astype(i32) for k in range(1, pairs))
    inside = zone - home * local
    side = (inside >= rows).astype(i32)
    row = inside - side * rows
    bin_at = lax.broadcasted_iota(i32, (bins, width), 0)
    before = (lax.broadcasted_iota(i32, (width, width), 0) < lax.broadcasted_iota(i32, (width, width), 1)).astype(bf16)

    def marks(key):
        return jnp.where(bin_at == jnp.where(valid, key, -1), 1.0, 0.0).astype(f32)

    def tally(mark):
        return jnp.sum(mark, axis=1, keepdims=True)

    def look(mark, table):
        return jnp.sum(mark * table, axis=0, keepdims=True)

    def ranks(mark):
        return jnp.dot(mark.astype(bf16), before, preferred_element_type=f32)

    at = lax.broadcasted_iota(i32, (bins, 128), 0)
    at_row = at & (rows - 1)
    at_home = at >> (rows.bit_length() - 1)
    edge = jnp.logical_or(at_row == 0, at_row == rows - 1)

    def flip(x, bit):
        step = 1 << bit
        if 2 * step == bins:
            return beside(x, step)
        return jnp.where((at & step) == 0, beside(x, step), beside(x, bins - step))

    across_x = lambda x: flip(x, 2)
    across_y = lambda x: flip(x, 3)
    mark = marks(home * rows + row)
    order = look(mark, ranks(mark))
    native = jnp.broadcast_to(tally(mark), (bins, 128)).astype(i32)

    def whole(x):
        x = x + across_x(x)
        return x + across_y(x)

    load = native
    half_sum = whole(native + flip(native, 0))
    goal = (jnp.maximum(half_sum, flip(half_sum, 1)) + pairs - 1) >> (pairs.bit_length() - 1)
    row_sum = (whole(native) + pairs - 1) >> (pairs.bit_length() - 1)
    end_goal = jnp.maximum(jnp.maximum(row_sum, flip(flip(row_sum, 0), 1)), (2 * goal * 171) >> 9)
    used = [jnp.zeros_like(native), jnp.zeros_like(native)]
    for _ in range(2):
        for d, partner in enumerate((across_x, across_y)):
            for stage in range(2):
                if stage == 0:
                    now, want, here = load, end_goal, edge
                else:
                    now, want, here = load + flip(load, 0), goal, jnp.logical_not(edge)
                move = jnp.minimum((now - partner(now)) >> 1, now - want)
                move = jnp.minimum(move, jnp.minimum(extra - used[d], native - used[0] - used[1]))
                move = jnp.where(here, jnp.maximum(move, 0), 0)
                used[d] = used[d] + move
                load = load + partner(move) - move
    first = look(mark, (used[0] * allow)[:, :1].astype(f32))
    second = look(mark, (used[1] * allow)[:, :1].astype(f32))
    leaves_x = order < first
    leaves_y = jnp.logical_and(order >= first, order < first + second)
    way = leaves_y.astype(i32)
    guest = order - jnp.where(leaves_y, first, 0.0)
    home_x = home & 1
    home_y = home >> 1
    via = jnp.where(leaves_x, home_y * 2 + 1 - home_x, jnp.where(leaves_y, (1 - home_y) * 2 + home_x, home))

    flow = marks(source * pairs + via)
    line = marks(via * rows + row)
    both = ranks(jnp.concatenate([flow, line], axis=0))
    rank = look(flow, both[:bins])
    place = look(line, both[bins:])
    flows = jnp.broadcast_to(tally(flow), (bins, 128))
    lines = jnp.broadcast_to(tally(line), (bins, 128))
    halves = lines + flip(lines, 0)
    stays = at_home == at_row
    chosen = jnp.zeros((1, 128), f32)
    for wide, end, far in sizes:
        over = jnp.where(flows > jnp.where(stays, per_pair, wide).astype(f32), 1.0, 0.0)
        over = jnp.maximum(over, jnp.where(lines > jnp.where(edge, end, tall).astype(f32), 1.0, 0.0))
        over = jnp.maximum(over, jnp.where(halves > jnp.float32(far), 1.0, 0.0))
        chosen = chosen + jnp.max(over, axis=0, keepdims=True)

    my_x, my_y = pair % 2, pair // 2

    def offset(other):
        other_y = other >> 1
        other_x = other - 2 * other_y
        return jnp.where(other_x == my_x, 0, 1) + jnp.where(other_y == my_y, 0, 2)

    def invert(here, key, value):
        key = jnp.where(jnp.logical_and(valid, here), key, -1)
        hit = jnp.where(lax.broadcasted_iota(i32, (128, width), 0) == key, 1.0, 0.0).astype(bf16)
        value = jnp.broadcast_to(value.astype(bf16), (16, width))
        return lax.dot_general(value, hit, (((1,), (1,)), ((), ())), preferred_element_type=f32)[:1]

    rank = rank.astype(i32)
    place = place.astype(i32)
    guest = guest.astype(i32)
    landing = offset(source) * per_pair + rank
    mine = via == pair
    ours = home == pair
    return chosen, [
        invert(source == pair, offset(via) * per_pair + rank, (lane - group * pair).astype(f32)),
        invert(mine, row * tall + place, landing.astype(f32)),
        invert(jnp.logical_and(mine, home != pair), (way * rows + row) * extra + guest, place.astype(f32)),
        invert(ours, (side * rows + row) * cap + slot, jnp.where(mine, place, tall + way * extra + guest).astype(f32)),
        invert(mine, row, jnp.ones((1, width), f32)),
        invert(ours, side * rows + row, jnp.ones((1, width), f32)),
    ]


def prepare_balanced(dims, sizes, zone, slot, table, choice, padded):
    pair = lax.axis_index("gx") // 2
    padded[...] = jnp.full_like(padded, -1)
    padded[0:1, 0:zone.shape[1]] = zone[...]
    padded[1:2, 0:zone.shape[1]] = slot[...]

    def fill(sizes, allow):
        chosen, lines = plan_tables(dims, sizes, pair, padded[0:1], padded[1:2], allow)
        for k, line in enumerate(lines):
            table[k:k + 1] = line.astype(jnp.int32)
        return jnp.max(chosen).astype(jnp.int32)

    chosen = fill(sizes, 1)
    choice[0] = jnp.minimum(chosen, len(sizes) - 1)

    @pl.when(chosen == len(sizes))
    def _():
        fill(sizes[:0], 0)


def mirror_rows(block):
    side = block.shape[0]
    row = PART - 1 - lax.broadcasted_iota(jnp.int32, (PART, block.shape[1]), 0)
    parts = [block[r - PART:r] for r in range(side, 0, -PART)]
    return jnp.concatenate([jnp.take_along_axis(part, row, axis=0) for part in parts], axis=0)


def turn(block, code):
    block = jnp.where(jnp.logical_or(code == 1, code == 2), mirror_lanes(block), block)
    block = jnp.where(code >= 2, mirror_rows(block), block)
    return jnp.where(jnp.logical_or(code == 1, code == 3), block.T, block)


def exchange_balanced(dims, chunks, table, spins, field, regional, *scratch):
    pairs, rows, per_group, per_pair, cap, extra, wide, end, far = dims
    tall = 2 * cap
    count = len(chunks)
    times, _, side, _ = field.shape
    strips = side // (2 * PART)
    kinds = 11
    groups = [scratch[i * count:(i + 1) * count] for i in range(kinds)]
    held, swapped, packed, landed, lifted, risen, pooled, crossed, passed, leaving, visiting = groups
    raw, given, far_list, *sems = scratch[kinds * count:]
    raw_sem, swap_send, swap_recv, pair_send, pair_recv, near_send, near_recv = sems[:7]
    give_send, give_recv, far_send, far_recv, pass_send, pass_recv, side_send, side_recv = sems[7:]
    unit_at = {unit: (c, i) for c, chunk in enumerate(chunks) for i, unit in enumerate(chunk)}
    gx = lax.axis_index("gx")
    z = lax.axis_index("gy")
    pair = gx // 2
    half = lax.rem(gx, 2)
    mate = (2 * pair + 1 - half, z)
    pair_x = lax.rem(pair, 2)
    pair_y = pair // 2
    near, far_in, far_out = (origin_of(z, rows, k, True) for k in (1, 2, 3))
    inner = jnp.logical_or(z == 1, z == 2)
    outer = jnp.logical_not(inner)
    role = jnp.where(inner, 0, 1)

    def across(o):
        x = 1 - pair_x if o % 2 else pair_x
        y = 1 - pair_y if o // 2 else pair_y
        return (2 * (2 * y + x) + half, z)

    bundle = per_group // LOADS
    loads = {}
    for t in range(times):
        for k in range(LOADS):
            part = pl.ds(k * bundle, bundle)
            loads[t, k] = pltpu.make_async_copy(field.at[t, part], raw.at[t, part], raw_sem.at[t, k])
            loads[t, k].start()

    barrier = pltpu.get_barrier_semaphore()
    friends = [mate] + [across(o) for o in range(1, pairs)] + [(gx, lax.rem(z + o, rows)) for o in range(1, rows)]
    for friend in friends:
        pl.semaphore_signal(barrier, inc=1, device_id=friend, device_id_type=MESH)

    def turn_time(t):
        for k in range(LOADS):
            loads[t, k].wait()

            def one(b, carry, k=k):
                b = b + k * bundle
                block = turn(raw[t, b], spins[gx * per_group + b])
                for r in range(strips):
                    c, i = unit_at[r, t]
                    top = block[r * PART:(r + 1) * PART]
                    bottom = block[side // 2 + r * PART:side // 2 + (r + 1) * PART]
                    held[c][half * per_group + b, i] = jnp.where(half == 0, top, bottom)
                    swapped[c][b, i] = jnp.where(half == 0, bottom, top)
                return carry
            lax.fori_loop(0, bundle, one, 0, unroll=4)

    turn_time(0)
    pl.semaphore_wait(barrier, len(friends))

    swaps = {}

    def swap_time(t):
        for c in sorted({unit_at[r, t][0] for r in range(strips)}):
            swaps[c] = pltpu.make_async_remote_copy(
                src_ref=swapped[c], dst_ref=held[c].at[pl.ds(half * per_group, per_group)],
                send_sem=swap_send.at[c], recv_sem=swap_recv.at[c], device_id=mate, device_id_type=MESH)
            swaps[c].start()

    swap_time(0)

    unsent = []
    pair_copies = {}

    def send_pairs(c):
        for t in range(1, times):
            if c == unit_at[0, t][0]:
                turn_time(t)
                swap_time(t)
        swaps[c].wait_recv()
        unsent.append(swaps[c])
        sent = []
        for o in range(1, pairs):
            def pack(k, carry, o=o):
                packed[c][o - 1, k] = held[c][table[0, o * per_pair + k]]
                return carry
            lax.fori_loop(0, wide, pack, 0, unroll=4)
            sent.append(pltpu.make_async_remote_copy(
                src_ref=packed[c].at[o - 1], dst_ref=landed[c].at[pl.ds(o * per_pair, wide)],
                send_sem=pair_send.at[c, o - 1], recv_sem=pair_recv.at[c, o - 1],
                device_id=across(o), device_id_type=MESH))
        unsent.extend(sent)
        pair_copies[c] = sent

        @pl.when(half == 0)
        def _():
            for copy in sent:
                copy.start()

        @pl.when(half == 1)
        def _():
            for copy in sent[::-1]:
                copy.start()

        def stay(k, carry):
            landed[c][k] = held[c][table[0, k]]
            return carry
        lax.fori_loop(0, per_pair, stay, 0, unroll=4)

        if c == 0:
            lead = table[4, far_in]

            def gather_far(k, carry):
                at = jnp.where(k < lead, far_in * tall + k, far_out * tall + k - lead)
                far_list[k] = table[1, jnp.minimum(at, rows * tall - 1)]
                return carry
            lax.fori_loop(0, far, gather_far, 0, unroll=4)

    skip = table[4, z]

    def near_copy(c, size):
        return pltpu.make_async_remote_copy(
            src_ref=lifted[c].at[pl.ds(0, size)], dst_ref=risen[c].at[1, pl.ds(0, size)],
            send_sem=near_send.at[c], recv_sem=near_recv.at[c],
            device_id=(gx, near), device_id_type=MESH)

    def far_copy(c, place):
        return pltpu.make_async_remote_copy(
            src_ref=pooled[c], dst_ref=crossed[c].at[place],
            send_sem=far_send.at[c], recv_sem=far_recv.at[c, place],
            device_id=(gx, far_in), device_id_type=MESH)

    def pass_copy(c, place):
        return pltpu.make_async_remote_copy(
            src_ref=passed[c].at[place], dst_ref=risen[c].at[2 + place, pl.ds(0, end)],
            send_sem=pass_send.at[c, place], recv_sem=pass_recv.at[c, place],
            device_id=(gx, near), device_id_type=MESH)

    def side_copy(c, d):
        return pltpu.make_async_remote_copy(
            src_ref=leaving[c].at[d], dst_ref=visiting[c].at[d],
            send_sem=side_send.at[c, d], recv_sem=side_recv.at[c, d],
            device_id=across(1 + d), device_id_type=MESH)

    def send_rows(c):
        for copy in pair_copies[c]:
            copy.wait_recv()

        def pool(k, carry):
            pooled[c][k] = landed[c][far_list[k]]
            return carry
        lax.fori_loop(0, far, pool, 0, unroll=4)

        def lift(k, carry):
            lifted[c][k] = landed[c][table[1, near * tall + k]]
            return carry
        lax.fori_loop(0, tall, lift, 0, unroll=4)
        unsent.append(far_copy(c, role))

        @pl.when(half == 0)
        def _():
            far_copy(c, role).start()

        @pl.when(inner)
        def _():
            near_copy(c, end).start()

        @pl.when(outer)
        def _():
            near_copy(c, tall).start()

        @pl.when(half == 1)
        def _():
            far_copy(c, role).start()

        def own(k, carry):
            risen[c][0, k] = landed[c][table[1, z * tall + k]]
            return carry
        lax.fori_loop(0, tall, own, 0, unroll=4)

    def hand_on(c):
        @pl.when(inner)
        def _():
            for place in range(2):
                far_copy(c, place).wait_recv()
            for place in range(2):
                def onward(k, carry, place=place):
                    passed[c][place, k] = crossed[c][place, jnp.minimum(skip + k, far - 1)]
                    return carry
                lax.fori_loop(0, end, onward, 0, unroll=4)
                pass_copy(c, place).start()

                def land(k, carry, place=place):
                    risen[c][2 + place, k] = crossed[c][place, k]
                    return carry
                lax.fori_loop(0, tall, land, 0, unroll=4)

    def send_sides(c):
        @pl.when(inner)
        def _():
            near_copy(c, tall).wait_recv()

        @pl.when(outer)
        def _():
            near_copy(c, end).wait_recv()
            for place in range(2):
                pass_copy(c, place).wait_recv()

        for d in range(2):
            def leave(k, carry, d=d):
                at = table[2, (d * rows + z) * extra + k]
                for o in range(rows):
                    leaving[c][d, o, k] = risen[c][o, at]
                return carry
            lax.fori_loop(0, extra, leave, 0)
            side_copy(c, d).start()
            unsent.append(side_copy(c, d))

    gives = []

    def settle(c):
        for d in range(2):
            side_copy(c, d).wait_recv()
        for r, _ in chunks[c]:
            if max(unit_at[r, t][0] for t in range(times)) == c:
                settle_strip(r)

    def settle_strip(r):
        span = pl.ds(pl.multiple_of(half * (side // 2) + r * PART, PART), PART)

        def place(s, carry):
            for core in (1 - half, half):
                at = table[3, (core * rows + z) * cap + s]
                live = s < table[5, core * rows + z]
                guest = jnp.maximum(at - tall, 0)
                way = guest // extra
                tiles = {}
                for t in range(times):
                    c, i = unit_at[r, t]
                    for o in range(rows):
                        home = risen[c][o, jnp.minimum(at, tall - 1), i]
                        visitor = visiting[c][way, o, guest - way * extra, i]
                        tiles[o, t] = jnp.where(at < tall, home, visitor)
                mean = sum(tiles.values()) * jnp.float32(1.0 / (rows * times))
                for (o, t), tile in tiles.items():
                    value = jnp.where(live, tile - mean, 0.0)
                    if core is half:
                        regional[origin_of(z, rows, o, True) * times + t, 0, s, span, :] = value
                    else:
                        given[r, origin_of(z, rows, o, True) * times + t, s] = value
            return carry
        lax.fori_loop(0, cap, place, 0)
        give = pltpu.make_async_remote_copy(
            src_ref=given.at[r], dst_ref=regional.at[:, 0, :, span, :],
            send_sem=give_send.at[r], recv_sem=give_recv.at[r], device_id=mate, device_id_type=MESH)
        give.start()
        gives.append(give)

    starts = []
    for chunk in chunks:
        begin = starts[-1][1] if starts else 0
        starts.append((begin, begin + len(chunk)))
    for _, _, c, act in timetable(starts, wide, end, far, extra, (send_pairs, send_rows, hand_on, send_sides, settle)):
        act(c)

    @pl.when(inner)
    def _():
        for c in range(count):
            near_copy(c, end).wait_send()
            for place in range(2):
                pass_copy(c, place).wait_send()

    @pl.when(outer)
    def _():
        for c in range(count):
            near_copy(c, tall).wait_send()

    for copy in unsent:
        copy.wait_send()
    for give in gives:
        give.wait()


def timetable(starts, wide, end, far, extra, acts):
    hop = 60
    sent = crossed = passed = 0.0
    busy = 4 * wide * starts[-1][1]
    events = []
    for c, (begin, close) in enumerate(starts):
        size = close - begin
        sent = sent + 4 * wide * size
        landed = sent + hop
        crossed = max(crossed, landed) + 4 * far * size
        passed = max(passed, crossed + hop) + 4 * end * size
        sides = passed + hop
        busy = max(busy, sides) + 8 * extra * size
        for k, at in enumerate((0.0, landed, crossed + hop, sides, busy + 2 * hop)):
            events.append((at, k, c, acts[k]))
    return sorted(events, key=lambda e: e[:3])


def on_device(field, zone, slot, spins, tally):
    times, per_group, side, _ = field.shape
    columns = lax.axis_size("gx")
    rows = lax.axis_size("gy")
    pairs = columns // 2
    cap = 2 * per_group // rows
    per_pair = 4 * (2 * per_group // columns)
    balanced = rows == 4 and pairs == 4 and columns * per_group < 256 and 2 * rows * cap <= 128 and pairs * per_pair <= 128
    if balanced:
        return balanced_exchange(field, zone, slot, spins, cap, per_pair)
    chunks = chunk_units(times, side)
    tiles = [(len(chunk), PART, side) for chunk in chunks]
    final = plain_exchange(field, zone, slot, spins, chunks, tiles, cap, per_pair)
    return pl.pallas_call(
        functools.partial(finish, rows, chunks),
        grid_spec=pltpu.PrefetchScalarGridSpec(
            num_scalar_prefetch=1,
            grid=(cap,),
            in_specs=[pl.BlockSpec(
                (2, 1, rows) + tile,
                lambda s, count: (0, jnp.maximum(jnp.minimum(s, count[0] - 1), 0), 0, 0, 0, 0)) for tile in tiles],
            out_specs=pl.BlockSpec((rows * times, 1, 1, side, side), lambda s, count: (0, 0, s, 0, 0)),
        ),
        out_shape=jax.ShapeDtypeStruct((rows * times, 1, cap, side, side), jnp.float32),
        name="finish",
    )(tally, *final)


def scratch_of(tiles, *shapes):
    return [pltpu.VMEM(lead + tile, jnp.float32) for lead in shapes for tile in tiles]


def balanced_exchange(field, zone, slot, spins, cap, per_pair):
    times, per_group, side, _ = field.shape
    columns = lax.axis_size("gx")
    rows = lax.axis_size("gy")
    pairs = columns // 2
    tall = 2 * cap
    extra = cap // 3
    chunks = time_major(times, side)
    tiles = [(len(chunk), PART, side) for chunk in chunks]
    count = len(chunks)
    strips = side // (2 * PART)
    smem = pl.BlockSpec(memory_space=pltpu.SMEM)
    vmem = pl.BlockSpec(memory_space=pltpu.VMEM)
    sizes = balanced_sizes(per_pair, tall)
    lanes = -(-columns * per_group // 128) * 128
    table, choice = pl.pallas_call(
        functools.partial(prepare_balanced, (pairs, rows, per_group, per_pair, cap, extra), sizes),
        in_specs=[vmem, vmem],
        out_specs=[vmem, smem],
        out_shape=[jax.ShapeDtypeStruct((8, 128), jnp.int32), jax.ShapeDtypeStruct((1,), jnp.int32)],
        scratch_shapes=[pltpu.VMEM((8, lanes), jnp.int32)],
        name="prepare",
    )(zone.reshape(1, -1), slot.reshape(1, -1))

    def moved(wide, end, far, tag):
        dma = pltpu.SemaphoreType.DMA
        buffers = [
            *scratch_of(
                tiles, (2 * per_group,), (per_group,), (pairs - 1, wide), (pairs * per_pair,), (tall,), (rows, tall),
                (far,), (2, far), (2, end), (2, rows, extra), (2, rows, extra)),
            pltpu.VMEM((times, per_group, side, side), jnp.float32),
            pltpu.VMEM((strips, rows * times, cap, PART, side), jnp.float32),
            pltpu.SMEM((far,), jnp.int32),
            dma((times, LOADS)), dma((count,)), dma((count,)),
            dma((count, pairs - 1)), dma((count, pairs - 1)),
            dma((count,)), dma((count,)),
            dma((strips,)), dma((strips,)),
            dma((count,)), dma((count, 2)),
            dma((count, 2)), dma((count, 2)), dma((count, 2)), dma((count, 2)),
        ]
        return lambda: pl.pallas_call(
            functools.partial(
                exchange_balanced, (pairs, rows, per_group, per_pair, cap, extra, wide, end, far), chunks),
            in_specs=[smem, smem, pl.BlockSpec(memory_space=pl.ANY)],
            out_specs=vmem,
            out_shape=pltpu.VMEM((rows * times, 1, cap, side, side), jnp.float32),
            scratch_shapes=buffers,
            compiler_params=pltpu.CompilerParams(collective_id=tag, has_side_effects=True, vmem_limit_bytes=VMEM_BYTES),
            name=f"exchange_{tag}",
        )(table, spins, field)

    return lax.switch(choice[0], [moved(*size, tag) for tag, size in enumerate(sizes)])


def plain_exchange(field, zone, slot, spins, chunks, tiles, cap, per_pair):
    times, per_group, side, _ = field.shape
    columns = lax.axis_size("gx")
    rows = lax.axis_size("gy")
    pairs = columns // 2
    per_row = 2 * cap
    smem = pl.BlockSpec(memory_space=pltpu.SMEM)
    anywhere = pl.BlockSpec(memory_space=pl.ANY)
    i32 = jnp.int32
    narrow = levels(per_pair, (40,))[0]
    sizes = [(narrow, tall) for tall in levels(per_row, (36, 42))]
    sizes.append((per_pair, per_row))
    *turned, send_table, pick_table, tallies, choice = pl.pallas_call(
        functools.partial(prepare, (pairs, rows, per_group, per_pair, cap, chunks, sizes)),
        grid=(per_group // STEP_BLOCKS,),
        in_specs=[smem, smem, smem, pl.BlockSpec((times, STEP_BLOCKS, side, side), lambda i: (0, i, 0, 0))],
        out_specs=[
            *[pl.BlockSpec((2, STEP_BLOCKS) + tile, lambda i: (0, i, 0, 0, 0)) for tile in tiles],
            smem, smem, smem, smem,
        ],
        out_shape=[
            *[jax.ShapeDtypeStruct((2, per_group) + tile, jnp.float32) for tile in tiles],
            jax.ShapeDtypeStruct((pairs * per_pair + 1,), i32),
            jax.ShapeDtypeStruct((per_row * rows + 1,), i32),
            jax.ShapeDtypeStruct((2 * rows,), i32),
            jax.ShapeDtypeStruct((1,), i32),
        ],
        scratch_shapes=[pltpu.SMEM((columns * rows,), i32), pltpu.SMEM((pairs * pairs,), i32)],
        name="prepare",
    )(zone, slot, spins, field)
    count = len(chunks)

    def moved(wide, tall, tag):
        dma = pltpu.SemaphoreType.DMA
        buffers = [
            *scratch_of(
                tiles, (2 * per_group,), (pairs - 1, wide), (pairs * per_pair,), (rows - 1, tall), (rows, tall),
                (cap, rows), (cap, rows)),
            pltpu.SMEM((rows * tall,), i32),
            dma((count,)), dma((count,)), dma((count,)),
            dma((count, pairs - 1)), dma((count, pairs - 1)),
            dma((count, rows - 1)), dma((count, rows - 1)),
            dma((count,)), dma((count,)), dma((count,)),
        ]
        return lambda: pl.pallas_call(
            functools.partial(exchange, (pairs, rows, per_group, per_pair, wide, tall, cap, count)),
            in_specs=[smem, smem, smem] + [anywhere] * count,
            out_specs=[anywhere] * count,
            out_shape=[jax.ShapeDtypeStruct((2, cap, rows) + tile, jnp.float32) for tile in tiles],
            scratch_shapes=buffers,
            compiler_params=pltpu.CompilerParams(collective_id=tag, has_side_effects=True, vmem_limit_bytes=60 * 2**20),
            name=f"exchange_{tag}",
        )(send_table, pick_table, tallies, *turned)

    return lax.switch(choice[0], [moved(*size, tag) for tag, size in enumerate(sizes)])


def solution(mesh):
    placed = (P("gy", "gx", None, None), P(), P(), P(), P(("gx", "gy")))
    return jax.shard_map(
        on_device,
        mesh=mesh,
        in_specs=placed,
        out_specs=P(None, ("gx", "gy"), None, None, None),
        check_vma=False,
    )
```

```python
import functools

import jax
import jax.numpy as jnp
from jax import lax
from jax.experimental import pallas as pl
from jax.experimental.pallas import tpu as pltpu
from jax.sharding import PartitionSpec as P

MESH = pl.DeviceIdType.MESH
PART = 8
STEP_BLOCKS = 4
LOADS = 2
VMEM_BYTES = 52 * 2**20


def chunk_units(times, side):
    units = [(r, t) for r in range(side // (2 * PART)) for t in range(times)]
    small = 2 * (times // 2 + times % 2)
    cuts = list(range(0, small + 1, max(times // 2, 1)))
    cuts += list(range(small + times, len(units) - small + 1, times))
    cuts += list(range(len(units) - small + max(times // 2, 1), len(units) + 1, max(times // 2, 1)))
    return [units[a:b] for a, b in zip(cuts[:-1], cuts[1:])]


def time_major(times, side):
    units = [(r, t) for t in range(times) for r in range(side // (2 * PART))]
    sizes = [1, 1] + [2] * ((len(units) - 4) // 2) + [1, 1]
    cuts = [sum(sizes[:c]) for c in range(len(sizes) + 1)]
    return [units[a:b] for a, b in zip(cuts[:-1], cuts[1:])]


def mirror_lanes(block):
    side = block.shape[1]
    lane = side - 1 - lax.broadcasted_iota(jnp.int32, block.shape, 1)
    return jnp.take_along_axis(block, lane, axis=1)


def turn_blocks(first, chunks, spins, field, turned):
    times, blocks, side, _ = field.shape
    for b in range(blocks):
        code = spins[first + b]
        for kind in range(4):
            @pl.when(code == kind)
            def _(kind=kind, b=b):
                for t in range(times):
                    block = field[t, b]
                    if kind == 1:
                        block = mirror_lanes(block).T
                    elif kind == 2:
                        block = mirror_lanes(mirror_lanes(block).T).T
                    elif kind == 3:
                        block = mirror_lanes(block.T)
                    for c, chunk in enumerate(chunks):
                        for i, (r, at) in enumerate(chunk):
                            if at == t:
                                for h in range(2):
                                    top = h * (side // 2) + r * PART
                                    turned[c][h, b, i] = block[top:top + PART]


def prepare(dims, zone, slot, spins, field, *refs):
    pairs, rows, per_group, per_pair, cap, chunks, sizes = dims
    turned = refs[:len(chunks)]
    send_table, pick_table, tallies, choice, counts, fills = refs[len(chunks):]
    gx = lax.axis_index("gx")
    pair = gx // 2
    group = 2 * per_group
    local = 2 * rows
    step = pl.program_id(0)

    @pl.when(step == 0)
    def _():
        def clear(ref, size):
            def body(i, c):
                ref[i] = 0
                return c
            lax.fori_loop(0, size, body, 0, unroll=8)
        clear(send_table, pairs * per_pair + 1)
        clear(pick_table, local * cap + 1)
        clear(counts, pairs * local)
        clear(fills, pairs * pairs)

        for source in range(pairs):
            behind = lax.rem(pair - source + pairs, pairs) * per_pair

            def place(j, c, source=source, behind=behind):
                region = zone[source * group + j]
                counts[region] = counts[region] + 1
                target = region // local
                cell = source * pairs + target
                rank = fills[cell]
                fills[cell] = rank + 1
                ahead = lax.rem(target - source + pairs, pairs) * per_pair
                send_table[jnp.where(source == pair, ahead + rank, pairs * per_pair)] = j
                at = (region - target * local) * cap + slot[source * group + j]
                pick_table[jnp.where(target == pair, at, local * cap)] = behind + rank
                return c
            lax.fori_loop(0, group, place, 0, unroll=4)
        most_pair = jnp.int32(0)
        most_row = jnp.int32(0)
        for q in range(pairs):
            for r in range(pairs):
                if q != r:
                    most_pair = jnp.maximum(most_pair, fills[q * pairs + r])
            pooled = [counts[q * local + r] + counts[q * local + rows + r] for r in range(rows)]
            for value in pooled:
                most_row = jnp.maximum(most_row, value)
        for r in range(local):
            tallies[r] = counts[pair * local + r]
        chosen = jnp.int32(len(sizes) - 1)
        for at in range(len(sizes) - 2, -1, -1):
            wide, tall = sizes[at]
            fits = jnp.logical_and(most_pair <= wide, most_row <= tall)
            chosen = jnp.where(fits, at, chosen)
        choice[0] = chosen

    turn_blocks(gx * per_group + step * field.shape[1], chunks, spins, field, turned)


def origin_of(z, rows, k, relay):
    if not relay:
        return lax.rem(z - k + rows, rows)
    low = z < 2
    return [z, z + 1 - 2 * lax.rem(z, 2), jnp.where(low, 2, 1), jnp.where(low, 3, 0)][k]


def exchange(dims, send_table, pick_table, tallies, *refs):
    pairs, rows, per_group, per_pair, wide, tall, cap, chunks = dims
    turned, final, scratch = refs[:chunks], refs[chunks:2 * chunks], refs[2 * chunks:]
    kinds = 7
    groups = [scratch[i * chunks:(i + 1) * chunks] for i in range(kinds)]
    held, packed, landed, lifted, risen, given, kept = groups
    sems = list(scratch[kinds * chunks:])
    row_list = sems.pop(0)
    own_sem, swap_send, swap_recv, pair_send, pair_recv, row_send, row_recv, give_send, give_recv, keep_sem = sems
    gx = lax.axis_index("gx")
    z = lax.axis_index("gy")
    pair = gx // 2
    half = lax.rem(gx, 2)
    mate = (2 * pair + 1 - half, z)

    def across(o):
        return (2 * lax.rem(pair + o, pairs) + half, z)

    def along(o):
        return (gx, lax.rem(z + o, rows))

    barrier = pltpu.get_barrier_semaphore()
    friends = [mate] + [across(o) for o in range(1, pairs)] + [along(o) for o in range(1, rows)]
    for friend in friends:
        pl.semaphore_signal(barrier, inc=1, device_id=friend, device_id_type=MESH)
    own_copies = []
    for c in range(chunks):
        own = pltpu.make_async_copy(turned[c].at[half], held[c].at[pl.ds(half * per_group, per_group)], own_sem.at[c])
        own.start()
        own_copies.append(own)
    pl.semaphore_wait(barrier, len(friends))

    swaps = []
    for c in range(chunks):
        swap = pltpu.make_async_remote_copy(
            src_ref=turned[c].at[1 - half], dst_ref=held[c].at[pl.ds(half * per_group, per_group)],
            send_sem=swap_send.at[c], recv_sem=swap_recv.at[c], device_id=mate, device_id_type=MESH)
        swap.start()
        swaps.append(swap)

    unsent = []
    pair_copies = []
    for c in range(chunks):
        own_copies[c].wait()
        swaps[c].wait_recv()
        unsent.append(swaps[c])
        sent = []
        for o in range(1, pairs):
            def pack(k, carry, o=o, c=c):
                packed[c][o - 1, k] = held[c][send_table[o * per_pair + k]]
                return carry
            lax.fori_loop(0, wide, pack, 0, unroll=4)
            copy = pltpu.make_async_remote_copy(
                src_ref=packed[c].at[o - 1], dst_ref=landed[c].at[pl.ds(o * per_pair, wide)],
                send_sem=pair_send.at[c, o - 1], recv_sem=pair_recv.at[c, o - 1],
                device_id=across(o), device_id_type=MESH)
            copy.start()
            sent.append(copy)
        unsent.extend(sent)

        def stay(k, carry, c=c):
            landed[c][k] = held[c][send_table[k]]
            return carry
        lax.fori_loop(0, per_pair, stay, 0, unroll=4)
        pair_copies.append(sent)

    for r in range(rows):
        first = tallies[r]

        def compact(k, carry, r=r, first=first):
            at = jnp.minimum(jnp.where(k < first, r * cap + k, (rows + r) * cap + k - first), 2 * rows * cap - 1)
            row_list[r * tall + k] = pick_table[at]
            return carry
        lax.fori_loop(0, tall, compact, 0, unroll=4)

    gives = []

    def settle_all(c):
        first = tallies[z]

        def settle(s, carry, c=c):
            mine = jnp.minimum(s + half * first, tall - 1)
            other = jnp.minimum(s + (1 - half) * first, tall - 1)
            for o in range(rows):
                given[c][s, o] = risen[c][o, other]
                kept[c][s, o] = risen[c][o, mine]
            return carry
        lax.fori_loop(0, cap, settle, 0)
        give = pltpu.make_async_remote_copy(
            src_ref=given[c], dst_ref=final[c].at[half],
            send_sem=give_send.at[c], recv_sem=give_recv.at[c], device_id=mate, device_id_type=MESH)
        give.start()
        keep = pltpu.make_async_copy(kept[c], final[c].at[half], keep_sem.at[c])
        keep.start()
        gives.append((give, keep))

    row_copies = []
    for c in range(chunks):
        for copy in pair_copies[c]:
            copy.wait_recv()
        sent = []
        for o in list(range(rows - 1, 0, -1)) + [0]:
            row = lax.rem(z + o, rows)

            def lift(k, carry, o=o, c=c, row=row):
                tile = landed[c][row_list[row * tall + k]]
                if o > 0:
                    lifted[c][o - 1, k] = tile
                else:
                    risen[c][0, k] = tile
                return carry
            lax.fori_loop(0, tall, lift, 0, unroll=4)
            if o > 0:
                copy = pltpu.make_async_remote_copy(
                    src_ref=lifted[c].at[o - 1], dst_ref=risen[c].at[o],
                    send_sem=row_send.at[c, o - 1], recv_sem=row_recv.at[c, o - 1],
                    device_id=along(o), device_id_type=MESH)
                copy.start()
                sent.append(copy)
        row_copies.append(sent)
        unsent.extend(sent)
    for c in range(chunks):
        for copy in row_copies[c]:
            copy.wait_recv()
        settle_all(c)
    for copy in unsent:
        copy.wait_send()
    for give, keep in gives:
        give.wait()
        keep.wait()


def finish(rows, chunks, tally, *refs):
    final, regional = refs[:-1], refs[-1]
    z = lax.axis_index("gy")
    slot = pl.program_id(0)
    side = regional.shape[3]
    times = regional.shape[0] // rows
    place = {unit: (c, i) for c, chunk in enumerate(chunks) for i, unit in enumerate(chunk)}

    @pl.when(slot < tally[0])
    def _():
        for h in range(2):
            for r in range(side // (2 * PART)):
                span = pl.ds(h * (side // 2) + r * PART, PART)
                tiles = {}
                for t in range(times):
                    c, i = place[(r, t)]
                    for o in range(rows):
                        tiles[o, t] = final[c][h, 0, o, i]
                mean = sum(tiles.values()) * jnp.float32(1.0 / (rows * times))
                for o in range(rows):
                    start = origin_of(z, rows, o, False) * times
                    for t in range(times):
                        regional[start + t, 0, 0, span, :] = tiles[o, t] - mean

    @pl.when(slot >= tally[0])
    def _():
        regional[...] = jnp.zeros_like(regional)


def levels(most, steps):
    return sorted({-(-most * s // 48) for s in steps})


def balanced_sizes(per_pair, tall):
    steps = ((38, 34, 52), (38, 36, 54), (40, 36, 56), (40, 38, 58), (42, 40, 60), (44, 44, 66), (48, 48, 96))
    return [(-(-per_pair * w // 48), -(-tall * e // 48), -(-tall * f // 48)) for w, e, f in steps]

def beside(x, step):
    return jnp.concatenate([x[step:], x[:step]], axis=0)


def plan_tables(dims, sizes, pair, zone, slot, allow):
    pairs, rows, per_group, per_pair, cap, extra = dims
    group, local, tall = 2 * per_group, 2 * rows, 2 * cap
    bins = pairs * rows
    width = zone.shape[1]
    i32, f32, bf16 = jnp.int32, jnp.float32, jnp.bfloat16
    lane = lax.broadcasted_iota(i32, (1, width), 1)
    valid = zone >= 0
    source = sum((lane >= group * k).astype(i32) for k in range(1, pairs))
    home = sum((zone >= local * k).astype(i32) for k in range(1, pairs))
    inside = zone - home * local
    side = (inside >= rows).astype(i32)
    row = inside - side * rows
    bin_at = lax.broadcasted_iota(i32, (bins, width), 0)
    before = (lax.broadcasted_iota(i32, (width, width), 0) < lax.broadcasted_iota(i32, (width, width), 1)).astype(bf16)

    def marks(key):
        return jnp.where(bin_at == jnp.where(valid, key, -1), 1.0, 0.0).astype(f32)

    def tally(mark):
        return jnp.sum(mark, axis=1, keepdims=True)

    def look(mark, table):
        return jnp.sum(mark * table, axis=0, keepdims=True)

    def ranks(mark):
        return jnp.dot(mark.astype(bf16), before, preferred_element_type=f32)

    at = lax.broadcasted_iota(i32, (bins, 128), 0)
    at_row = at & (rows - 1)
    at_home = at >> (rows.bit_length() - 1)
    edge = jnp.logical_or(at_row == 0, at_row == rows - 1)

    def flip(x, bit):
        step = 1 << bit
        if 2 * step == bins:
            return beside(x, step)
        return jnp.where((at & step) == 0, beside(x, step), beside(x, bins - step))

    across_x = lambda x: flip(x, 2)
    across_y = lambda x: flip(x, 3)
    mark = marks(home * rows + row)
    order = look(mark, ranks(mark))
    native = jnp.broadcast_to(tally(mark), (bins, 128)).astype(i32)

    def whole(x):
        x = x + across_x(x)
        return x + across_y(x)

    load = native
    half_sum = whole(native + flip(native, 0))
    goal = (jnp.maximum(half_sum, flip(half_sum, 1)) + pairs - 1) >> (pairs.bit_length() - 1)
    row_sum = (whole(native) + pairs - 1) >> (pairs.bit_length() - 1)
    end_goal = jnp.maximum(jnp.maximum(row_sum, flip(flip(row_sum, 0), 1)), (9 * goal) >> 4)
    used = [jnp.zeros_like(native), jnp.zeros_like(native)]
    for _ in range(2):
        for d, partner in enumerate((across_x, across_y)):
            for stage in range(3):
                now, want = (load, end_goal) if stage == 0 else (load + flip(load, 0), goal)
                here = jnp.logical_not(edge) if stage == 1 else edge
                move = jnp.minimum((now - partner(now)) >> 1, now - want)
                move = jnp.minimum(move, jnp.minimum(extra - used[d], native - used[0] - used[1]))
                move = jnp.where(here, jnp.maximum(move, 0), 0)
                used[d] = used[d] + move
                load = load + partner(move) - move
    first = look(mark, (used[0] * allow)[:, :1].astype(f32))
    second = look(mark, (used[1] * allow)[:, :1].astype(f32))
    leaves_x = order < first
    leaves_y = jnp.logical_and(order >= first, order < first + second)
    way = leaves_y.astype(i32)
    guest = order - jnp.where(leaves_y, first, 0.0)
    home_x = home & 1
    home_y = home >> 1
    via = jnp.where(leaves_x, home_y * 2 + 1 - home_x, jnp.where(leaves_y, (1 - home_y) * 2 + home_x, home))

    flow = marks(source * pairs + via)
    line = marks(via * rows + row)
    both = ranks(jnp.concatenate([flow, line], axis=0))
    rank = look(flow, both[:bins])
    place = look(line, both[bins:])
    flows = jnp.broadcast_to(tally(flow), (bins, 128))
    lines = jnp.broadcast_to(tally(line), (bins, 128))
    halves = lines + flip(lines, 0)
    stays = at_home == at_row
    chosen = jnp.zeros((1, 128), f32)
    for wide, end, far in sizes:
        over = jnp.where(flows > jnp.where(stays, per_pair, wide).astype(f32), 1.0, 0.0)
        over = jnp.maximum(over, jnp.where(lines > jnp.where(edge, end, tall).astype(f32), 1.0, 0.0))
        over = jnp.maximum(over, jnp.where(halves > jnp.float32(far), 1.0, 0.0))
        chosen = chosen + jnp.max(over, axis=0, keepdims=True)

    my_x, my_y = pair % 2, pair // 2

    def offset(other):
        other_y = other >> 1
        other_x = other - 2 * other_y
        return jnp.where(other_x == my_x, 0, 1) + jnp.where(other_y == my_y, 0, 2)

    def invert(here, key, value):
        key = jnp.where(jnp.logical_and(valid, here), key, -1)
        hit = jnp.where(lax.broadcasted_iota(i32, (128, width), 0) == key, 1.0, 0.0).astype(bf16)
        value = jnp.broadcast_to(value.astype(bf16), (16, width))
        return lax.dot_general(value, hit, (((1,), (1,)), ((), ())), preferred_element_type=f32)[:1]

    rank = rank.astype(i32)
    place = place.astype(i32)
    guest = guest.astype(i32)
    landing = offset(source) * per_pair + rank
    mine = via == pair
    ours = home == pair
    return chosen, [
        invert(source == pair, offset(via) * per_pair + rank, (lane - group * pair).astype(f32)),
        invert(mine, row * tall + place, landing.astype(f32)),
        invert(jnp.logical_and(mine, home != pair), (way * rows + row) * extra + guest, place.astype(f32)),
        invert(ours, (side * rows + row) * cap + slot, jnp.where(mine, place, tall + way * extra + guest).astype(f32)),
        invert(mine, row, jnp.ones((1, width), f32)),
        invert(ours, side * rows + row, jnp.ones((1, width), f32)),
    ]


def prepare_balanced(dims, sizes, zone, slot, table, choice, padded):
    pair = lax.axis_index("gx") // 2
    padded[...] = jnp.full_like(padded, -1)
    padded[0:1, 0:zone.shape[1]] = zone[...]
    padded[1:2, 0:zone.shape[1]] = slot[...]

    def fill(sizes, allow):
        chosen, lines = plan_tables(dims, sizes, pair, padded[0:1], padded[1:2], allow)
        for k, line in enumerate(lines):
            table[k:k + 1] = line.astype(jnp.int32)
        return jnp.max(chosen).astype(jnp.int32)

    chosen = fill(sizes, 1)
    choice[0] = jnp.minimum(chosen, len(sizes) - 1)

    @pl.when(chosen == len(sizes))
    def _():
        fill(sizes[:0], 0)


def mirror_rows(block):
    side = block.shape[0]
    row = PART - 1 - lax.broadcasted_iota(jnp.int32, (PART, block.shape[1]), 0)
    parts = [block[r - PART:r] for r in range(side, 0, -PART)]
    return jnp.concatenate([jnp.take_along_axis(part, row, axis=0) for part in parts], axis=0)


def turn(block, code):
    block = jnp.where(jnp.logical_or(code == 1, code == 2), mirror_lanes(block), block)
    block = jnp.where(code >= 2, mirror_rows(block), block)
    return jnp.where(jnp.logical_or(code == 1, code == 3), block.T, block)


def exchange_balanced(dims, chunks, table, spins, field, regional, *scratch):
    pairs, rows, per_group, per_pair, cap, extra, wide, end, far = dims
    tall = 2 * cap
    count = len(chunks)
    times, _, side, _ = field.shape
    strips = side // (2 * PART)
    kinds = 12
    groups = [scratch[i * count:(i + 1) * count] for i in range(kinds)]
    held, swapped, packed, landed, lifted, risen, pooled, crossed_in, crossed_out, passed, leaving, visiting = groups
    crossed = (crossed_in, crossed_out)
    raw, given, far_list, *sems = scratch[kinds * count:]
    raw_sem, swap_send, swap_recv, pair_send, pair_recv, near_send, near_recv = sems[:7]
    give_send, give_recv, far_send, far_recv, pass_send, pass_recv, side_send, side_recv = sems[7:]
    unit_at = {unit: (c, i) for c, chunk in enumerate(chunks) for i, unit in enumerate(chunk)}
    gx = lax.axis_index("gx")
    z = lax.axis_index("gy")
    pair = gx // 2
    half = lax.rem(gx, 2)
    mate = (2 * pair + 1 - half, z)
    pair_x = lax.rem(pair, 2)
    pair_y = pair // 2
    near, far_in, far_out = (origin_of(z, rows, k, True) for k in (1, 2, 3))
    inner = jnp.logical_or(z == 1, z == 2)
    outer = jnp.logical_not(inner)

    def across(o):
        x = 1 - pair_x if o % 2 else pair_x
        y = 1 - pair_y if o // 2 else pair_y
        return (2 * (2 * y + x) + half, z)

    bundle = per_group // LOADS
    loads = {}
    for t in range(times):
        for k in range(LOADS):
            part = pl.ds(k * bundle, bundle)
            loads[t, k] = pltpu.make_async_copy(field.at[t, part], raw.at[t, part], raw_sem.at[t, k])
            loads[t, k].start()

    barrier = pltpu.get_barrier_semaphore()
    friends = [mate] + [across(o) for o in range(1, pairs)] + [(gx, lax.rem(z + o, rows)) for o in range(1, rows)]
    for friend in friends:
        pl.semaphore_signal(barrier, inc=1, device_id=friend, device_id_type=MESH)

    def turn_time(t):
        for k in range(LOADS):
            loads[t, k].wait()

            def one(b, carry, k=k):
                b = b + k * bundle
                block = turn(raw[t, b], spins[gx * per_group + b])
                for r in range(strips):
                    c, i = unit_at[r, t]
                    top = block[r * PART:(r + 1) * PART]
                    bottom = block[side // 2 + r * PART:side // 2 + (r + 1) * PART]
                    held[c][half * per_group + b, i] = jnp.where(half == 0, top, bottom)
                    swapped[c][b, i] = jnp.where(half == 0, bottom, top)
                return carry
            lax.fori_loop(0, bundle, one, 0, unroll=4)

    turn_time(0)
    pl.semaphore_wait(barrier, len(friends))

    swaps = {}

    def swap_time(t):
        for c in sorted({unit_at[r, t][0] for r in range(strips)}):
            swaps[c] = pltpu.make_async_remote_copy(
                src_ref=swapped[c], dst_ref=held[c].at[pl.ds(half * per_group, per_group)],
                send_sem=swap_send.at[c], recv_sem=swap_recv.at[c], device_id=mate, device_id_type=MESH)
            swaps[c].start()

    swap_time(0)

    unsent = []
    pair_copies = {}

    def send_pairs(c):
        if c == 1:
            for t in range(1, times):
                turn_time(t)
                swap_time(t)
        swaps[c].wait_recv()
        unsent.append(swaps[c])
        sent = []
        for o in range(1, pairs):
            def pack(k, carry, o=o):
                packed[c][o - 1, k] = held[c][table[0, o * per_pair + k]]
                return carry
            lax.fori_loop(0, wide, pack, 0, unroll=4)
            sent.append(pltpu.make_async_remote_copy(
                src_ref=packed[c].at[o - 1], dst_ref=landed[c].at[pl.ds(o * per_pair, wide)],
                send_sem=pair_send.at[c, o - 1], recv_sem=pair_recv.at[c, o - 1],
                device_id=across(o), device_id_type=MESH))
        unsent.extend(sent)
        pair_copies[c] = sent

        @pl.when(half == 0)
        def _():
            for copy in sent:
                copy.start()

        @pl.when(half == 1)
        def _():
            for copy in sent[::-1]:
                copy.start()

        def stay(k, carry):
            landed[c][k] = held[c][table[0, k]]
            return carry
        lax.fori_loop(0, per_pair, stay, 0, unroll=4)

        if c == 0:
            lead = table[4, far_in]

            def gather_far(k, carry):
                at = jnp.where(k < lead, far_in * tall + k, far_out * tall + k - lead)
                far_list[k] = table[1, jnp.minimum(at, rows * tall - 1)]
                return carry
            lax.fori_loop(0, far, gather_far, 0, unroll=4)

    skip = table[4, z]

    def near_copy(c, size):
        return pltpu.make_async_remote_copy(
            src_ref=lifted[c].at[pl.ds(0, size)], dst_ref=risen[c].at[1, pl.ds(0, size)],
            send_sem=near_send.at[c], recv_sem=near_recv.at[c],
            device_id=(gx, near), device_id_type=MESH)

    def far_copy(c, place):
        return pltpu.make_async_remote_copy(
            src_ref=pooled[c], dst_ref=crossed[place][c],
            send_sem=far_send.at[c], recv_sem=far_recv.at[c, place],
            device_id=(gx, far_in), device_id_type=MESH)

    def pass_copy(c, place):
        return pltpu.make_async_remote_copy(
            src_ref=passed[c].at[place], dst_ref=risen[c].at[2 + place, pl.ds(0, end)],
            send_sem=pass_send.at[c, place], recv_sem=pass_recv.at[c, place],
            device_id=(gx, near), device_id_type=MESH)

    def side_copy(c, d):
        return pltpu.make_async_remote_copy(
            src_ref=leaving[c].at[d], dst_ref=visiting[c].at[d],
            send_sem=side_send.at[c, d], recv_sem=side_recv.at[c, d],
            device_id=across(1 + d), device_id_type=MESH)

    def send_rows(c):
        for copy in pair_copies[c]:
            copy.wait_recv()

        def pool(k, carry):
            pooled[c][k] = landed[c][far_list[k]]
            return carry
        lax.fori_loop(0, far, pool, 0, unroll=4)

        def lift(k, carry):
            lifted[c][k] = landed[c][table[1, near * tall + k]]
            return carry
        lax.fori_loop(0, tall, lift, 0, unroll=4)

        def send_far():
            for place, mine in enumerate((inner, outer)):
                @pl.when(mine)
                def _(place=place):
                    far_copy(c, place).start()

        @pl.when(half == 0)
        def _():
            send_far()

        @pl.when(inner)
        def _():
            near_copy(c, end).start()

        @pl.when(outer)
        def _():
            near_copy(c, tall).start()

        @pl.when(half == 1)
        def _():
            send_far()

        def own(k, carry):
            risen[c][0, k] = landed[c][table[1, z * tall + k]]
            return carry
        lax.fori_loop(0, tall, own, 0, unroll=4)

    def hand_on(c, place):
        @pl.when(inner)
        def _():
            far_copy(c, place).wait_recv()

            def onward(k, carry):
                passed[c][place, k] = crossed[place][c][jnp.minimum(skip + k, far - 1)]
                return carry
            lax.fori_loop(0, end, onward, 0, unroll=4)
            pass_copy(c, place).start()

            def land(k, carry):
                risen[c][2 + place, k] = crossed[place][c][k]
                return carry
            lax.fori_loop(0, tall, land, 0, unroll=4)

    def hand_on_inner(c):
        hand_on(c, 0)

    def hand_on_outer(c):
        hand_on(c, 1)

    def send_sides(c):
        @pl.when(inner)
        def _():
            near_copy(c, tall).wait_recv()

        @pl.when(outer)
        def _():
            near_copy(c, end).wait_recv()
            for place in range(2):
                pass_copy(c, place).wait_recv()

        for d in range(2):
            def leave(k, carry, d=d):
                at = table[2, (d * rows + z) * extra + k]
                for o in range(rows):
                    leaving[c][d, o, k] = risen[c][o, at]
                return carry
            lax.fori_loop(0, extra, leave, 0)
            side_copy(c, d).start()
            unsent.append(side_copy(c, d))

    gives = []

    def settle(c):
        for d in range(2):
            side_copy(c, d).wait_recv()
        for r, _ in chunks[c]:
            if max(unit_at[r, t][0] for t in range(times)) == c:
                settle_strip(r)

    def settle_strip(r):
        span = pl.ds(pl.multiple_of(half * (side // 2) + r * PART, PART), PART)

        def place(s, carry):
            for core in (1 - half, half):
                at = table[3, (core * rows + z) * cap + s]
                live = s < table[5, core * rows + z]
                guest = jnp.maximum(at - tall, 0)
                way = guest // extra
                tiles = {}
                for t in range(times):
                    c, i = unit_at[r, t]
                    for o in range(rows):
                        home = risen[c][o, jnp.minimum(at, tall - 1), i]
                        visitor = visiting[c][way, o, guest - way * extra, i]
                        tiles[o, t] = jnp.where(at < tall, home, visitor)
                mean = sum(tiles.values()) * jnp.float32(1.0 / (rows * times))
                for (o, t), tile in tiles.items():
                    value = jnp.where(live, tile - mean, 0.0)
                    if core is half:
                        regional[origin_of(z, rows, o, True) * times + t, 0, s, span, :] = value
                    else:
                        given[r, origin_of(z, rows, o, True) * times + t, s] = value
            return carry
        lax.fori_loop(0, cap, place, 0)
        give = pltpu.make_async_remote_copy(
            src_ref=given.at[r], dst_ref=regional.at[:, 0, :, span, :],
            send_sem=give_send.at[r], recv_sem=give_recv.at[r], device_id=mate, device_id_type=MESH)
        give.start()
        gives.append(give)

    starts = []
    for chunk in chunks:
        begin = starts[-1][1] if starts else 0
        starts.append((begin, begin + len(chunk)))
    for _, _, c, act in timetable(starts, wide, tall, end, far, extra, (send_pairs, send_rows, hand_on_outer, hand_on_inner, send_sides, settle)):
        act(c)

    @pl.when(inner)
    def _():
        for c in range(count):
            near_copy(c, end).wait_send()
            far_copy(c, 0).wait_send()
            for place in range(2):
                pass_copy(c, place).wait_send()

    @pl.when(outer)
    def _():
        for c in range(count):
            near_copy(c, tall).wait_send()
            far_copy(c, 1).wait_send()

    for copy in unsent:
        copy.wait_send()
    for give in gives:
        give.wait()


def timetable(starts, wide, tall, end, far, extra, acts):
    hop = 60
    sent = soon = crossed = passed = 0.0
    busy = 4 * wide * starts[-1][1]
    events = []
    for c, (begin, close) in enumerate(starts):
        size = close - begin
        sent = sent + 4 * wide * size
        landed = sent + hop
        soon = max(soon, landed) + 1.9 * (tall + far) * size
        crossed = max(crossed, landed) + 4 * far * size
        passed = max(passed, crossed + hop) + 4 * end * size
        sides = passed + hop
        busy = max(busy, sides) + 8 * extra * size
        for k, at in enumerate((0.0, landed, soon + hop, crossed + hop, sides, busy + 2 * hop)):
            events.append((at, k, c, acts[k]))
    return sorted(events, key=lambda e: e[:3])


def on_device(field, zone, slot, spins, tally):
    times, per_group, side, _ = field.shape
    columns = lax.axis_size("gx")
    rows = lax.axis_size("gy")
    pairs = columns // 2
    cap = 2 * per_group // rows
    per_pair = 4 * (2 * per_group // columns)
    balanced = rows == 4 and pairs == 4 and columns * per_group < 256 and 2 * rows * cap <= 128 and pairs * per_pair <= 128
    if balanced:
        return balanced_exchange(field, zone, slot, spins, cap, per_pair)
    chunks = chunk_units(times, side)
    tiles = [(len(chunk), PART, side) for chunk in chunks]
    final = plain_exchange(field, zone, slot, spins, chunks, tiles, cap, per_pair)
    return pl.pallas_call(
        functools.partial(finish, rows, chunks),
        grid_spec=pltpu.PrefetchScalarGridSpec(
            num_scalar_prefetch=1,
            grid=(cap,),
            in_specs=[pl.BlockSpec(
                (2, 1, rows) + tile,
                lambda s, count: (0, jnp.maximum(jnp.minimum(s, count[0] - 1), 0), 0, 0, 0, 0)) for tile in tiles],
            out_specs=pl.BlockSpec((rows * times, 1, 1, side, side), lambda s, count: (0, 0, s, 0, 0)),
        ),
        out_shape=jax.ShapeDtypeStruct((rows * times, 1, cap, side, side), jnp.float32),
        name="finish",
    )(tally, *final)


def scratch_of(tiles, *shapes):
    return [pltpu.VMEM(lead + tile, jnp.float32) for lead in shapes for tile in tiles]


def balanced_exchange(field, zone, slot, spins, cap, per_pair):
    times, per_group, side, _ = field.shape
    columns = lax.axis_size("gx")
    rows = lax.axis_size("gy")
    pairs = columns // 2
    tall = 2 * cap
    extra = cap // 3
    chunks = time_major(times, side)
    tiles = [(len(chunk), PART, side) for chunk in chunks]
    count = len(chunks)
    strips = side // (2 * PART)
    smem = pl.BlockSpec(memory_space=pltpu.SMEM)
    vmem = pl.BlockSpec(memory_space=pltpu.VMEM)
    sizes = balanced_sizes(per_pair, tall)
    lanes = -(-columns * per_group // 128) * 128
    table, choice = pl.pallas_call(
        functools.partial(prepare_balanced, (pairs, rows, per_group, per_pair, cap, extra), sizes),
        in_specs=[vmem, vmem],
        out_specs=[vmem, smem],
        out_shape=[jax.ShapeDtypeStruct((8, 128), jnp.int32), jax.ShapeDtypeStruct((1,), jnp.int32)],
        scratch_shapes=[pltpu.VMEM((8, lanes), jnp.int32)],
        name="prepare",
    )(zone.reshape(1, -1), slot.reshape(1, -1))

    def moved(wide, end, far, tag):
        dma = pltpu.SemaphoreType.DMA
        buffers = [
            *scratch_of(
                tiles, (2 * per_group,), (per_group,), (pairs - 1, wide), (pairs * per_pair,), (tall,), (rows, tall),
                (far,), (far,), (far,), (2, end), (2, rows, extra), (2, rows, extra)),
            pltpu.VMEM((times, per_group, side, side), jnp.float32),
            pltpu.VMEM((strips, rows * times, cap, PART, side), jnp.float32),
            pltpu.SMEM((far,), jnp.int32),
            dma((times, LOADS)), dma((count,)), dma((count,)),
            dma((count, pairs - 1)), dma((count, pairs - 1)),
            dma((count,)), dma((count,)),
            dma((strips,)), dma((strips,)),
            dma((count,)), dma((count, 2)),
            dma((count, 2)), dma((count, 2)), dma((count, 2)), dma((count, 2)),
        ]
        return lambda: pl.pallas_call(
            functools.partial(
                exchange_balanced, (pairs, rows, per_group, per_pair, cap, extra, wide, end, far), chunks),
            in_specs=[smem, smem, pl.BlockSpec(memory_space=pl.ANY)],
            out_specs=vmem,
            out_shape=pltpu.VMEM((rows * times, 1, cap, side, side), jnp.float32),
            scratch_shapes=buffers,
            compiler_params=pltpu.CompilerParams(collective_id=tag, has_side_effects=True, vmem_limit_bytes=VMEM_BYTES),
            name=f"exchange_{tag}",
        )(table, spins, field)

    return lax.switch(choice[0], [moved(*size, tag) for tag, size in enumerate(sizes)])


def plain_exchange(field, zone, slot, spins, chunks, tiles, cap, per_pair):
    times, per_group, side, _ = field.shape
    columns = lax.axis_size("gx")
    rows = lax.axis_size("gy")
    pairs = columns // 2
    per_row = 2 * cap
    smem = pl.BlockSpec(memory_space=pltpu.SMEM)
    anywhere = pl.BlockSpec(memory_space=pl.ANY)
    i32 = jnp.int32
    narrow = levels(per_pair, (40,))[0]
    sizes = [(narrow, tall) for tall in levels(per_row, (36, 42))]
    sizes.append((per_pair, per_row))
    *turned, send_table, pick_table, tallies, choice = pl.pallas_call(
        functools.partial(prepare, (pairs, rows, per_group, per_pair, cap, chunks, sizes)),
        grid=(per_group // STEP_BLOCKS,),
        in_specs=[smem, smem, smem, pl.BlockSpec((times, STEP_BLOCKS, side, side), lambda i: (0, i, 0, 0))],
        out_specs=[
            *[pl.BlockSpec((2, STEP_BLOCKS) + tile, lambda i: (0, i, 0, 0, 0)) for tile in tiles],
            smem, smem, smem, smem,
        ],
        out_shape=[
            *[jax.ShapeDtypeStruct((2, per_group) + tile, jnp.float32) for tile in tiles],
            jax.ShapeDtypeStruct((pairs * per_pair + 1,), i32),
            jax.ShapeDtypeStruct((per_row * rows + 1,), i32),
            jax.ShapeDtypeStruct((2 * rows,), i32),
            jax.ShapeDtypeStruct((1,), i32),
        ],
        scratch_shapes=[pltpu.SMEM((columns * rows,), i32), pltpu.SMEM((pairs * pairs,), i32)],
        name="prepare",
    )(zone, slot, spins, field)
    count = len(chunks)

    def moved(wide, tall, tag):
        dma = pltpu.SemaphoreType.DMA
        buffers = [
            *scratch_of(
                tiles, (2 * per_group,), (pairs - 1, wide), (pairs * per_pair,), (rows - 1, tall), (rows, tall),
                (cap, rows), (cap, rows)),
            pltpu.SMEM((rows * tall,), i32),
            dma((count,)), dma((count,)), dma((count,)),
            dma((count, pairs - 1)), dma((count, pairs - 1)),
            dma((count, rows - 1)), dma((count, rows - 1)),
            dma((count,)), dma((count,)), dma((count,)),
        ]
        return lambda: pl.pallas_call(
            functools.partial(exchange, (pairs, rows, per_group, per_pair, wide, tall, cap, count)),
            in_specs=[smem, smem, smem] + [anywhere] * count,
            out_specs=[anywhere] * count,
            out_shape=[jax.ShapeDtypeStruct((2, cap, rows) + tile, jnp.float32) for tile in tiles],
            scratch_shapes=buffers,
            compiler_params=pltpu.CompilerParams(collective_id=tag, has_side_effects=True, vmem_limit_bytes=60 * 2**20),
            name=f"exchange_{tag}",
        )(send_table, pick_table, tallies, *turned)

    return lax.switch(choice[0], [moved(*size, tag) for tag, size in enumerate(sizes)])


def solution(mesh):
    placed = (P("gy", "gx", None, None), P(), P(), P(), P(("gx", "gy")))
    return jax.shard_map(
        on_device,
        mesh=mesh,
        in_specs=placed,
        out_specs=P(None, ("gx", "gy"), None, None, None),
        check_vma=False,
    )
```

```python
import functools

import jax
import jax.numpy as jnp
from jax import lax
from jax.experimental import pallas as pl
from jax.experimental.pallas import tpu as pltpu
from jax.sharding import PartitionSpec as P

MESH = pl.DeviceIdType.MESH
PART = 8
STEP_BLOCKS = 4
VMEM_BYTES = 52 * 2**20


def chunk_units(times, side):
    units = [(r, t) for r in range(side // (2 * PART)) for t in range(times)]
    small = 2 * (times // 2 + times % 2)
    cuts = list(range(0, small + 1, max(times // 2, 1)))
    cuts += list(range(small + times, len(units) - small + 1, times))
    cuts += list(range(len(units) - small + max(times // 2, 1), len(units) + 1, max(times // 2, 1)))
    return [units[a:b] for a, b in zip(cuts[:-1], cuts[1:])]


def time_major(times, side):
    units = [(r, t) for t in range(times) for r in range(side // (2 * PART))]
    sizes = [1, 1] + [2] * ((len(units) - 4) // 2) + [1, 1]
    cuts = [sum(sizes[:c]) for c in range(len(sizes) + 1)]
    return [units[a:b] for a, b in zip(cuts[:-1], cuts[1:])]


def mirror_lanes(block):
    side = block.shape[1]
    lane = side - 1 - lax.broadcasted_iota(jnp.int32, block.shape, 1)
    return jnp.take_along_axis(block, lane, axis=1)


def turn_blocks(first, chunks, spins, field, turned):
    times, blocks, side, _ = field.shape
    for b in range(blocks):
        code = spins[first + b]
        for kind in range(4):
            @pl.when(code == kind)
            def _(kind=kind, b=b):
                for t in range(times):
                    block = field[t, b]
                    if kind == 1:
                        block = mirror_lanes(block).T
                    elif kind == 2:
                        block = mirror_lanes(mirror_lanes(block).T).T
                    elif kind == 3:
                        block = mirror_lanes(block.T)
                    for c, chunk in enumerate(chunks):
                        for i, (r, at) in enumerate(chunk):
                            if at == t:
                                for h in range(2):
                                    top = h * (side // 2) + r * PART
                                    turned[c][h, b, i] = block[top:top + PART]


def prepare(dims, zone, slot, spins, field, *refs):
    pairs, rows, per_group, per_pair, cap, chunks, sizes = dims
    turned = refs[:len(chunks)]
    send_table, pick_table, tallies, choice, counts, fills = refs[len(chunks):]
    gx = lax.axis_index("gx")
    pair = gx // 2
    group = 2 * per_group
    local = 2 * rows
    step = pl.program_id(0)

    @pl.when(step == 0)
    def _():
        def clear(ref, size):
            def body(i, c):
                ref[i] = 0
                return c
            lax.fori_loop(0, size, body, 0, unroll=8)
        clear(send_table, pairs * per_pair + 1)
        clear(pick_table, local * cap + 1)
        clear(counts, pairs * local)
        clear(fills, pairs * pairs)

        for source in range(pairs):
            behind = lax.rem(pair - source + pairs, pairs) * per_pair

            def place(j, c, source=source, behind=behind):
                region = zone[source * group + j]
                counts[region] = counts[region] + 1
                target = region // local
                cell = source * pairs + target
                rank = fills[cell]
                fills[cell] = rank + 1
                ahead = lax.rem(target - source + pairs, pairs) * per_pair
                send_table[jnp.where(source == pair, ahead + rank, pairs * per_pair)] = j
                at = (region - target * local) * cap + slot[source * group + j]
                pick_table[jnp.where(target == pair, at, local * cap)] = behind + rank
                return c
            lax.fori_loop(0, group, place, 0, unroll=4)
        most_pair = jnp.int32(0)
        most_row = jnp.int32(0)
        for q in range(pairs):
            for r in range(pairs):
                if q != r:
                    most_pair = jnp.maximum(most_pair, fills[q * pairs + r])
            pooled = [counts[q * local + r] + counts[q * local + rows + r] for r in range(rows)]
            for value in pooled:
                most_row = jnp.maximum(most_row, value)
        for r in range(local):
            tallies[r] = counts[pair * local + r]
        chosen = jnp.int32(len(sizes) - 1)
        for at in range(len(sizes) - 2, -1, -1):
            wide, tall = sizes[at]
            fits = jnp.logical_and(most_pair <= wide, most_row <= tall)
            chosen = jnp.where(fits, at, chosen)
        choice[0] = chosen

    turn_blocks(gx * per_group + step * field.shape[1], chunks, spins, field, turned)


def origin_of(z, rows, k, relay):
    if not relay:
        return lax.rem(z - k + rows, rows)
    low = z < 2
    return [z, z + 1 - 2 * lax.rem(z, 2), jnp.where(low, 2, 1), jnp.where(low, 3, 0)][k]


def exchange(dims, send_table, pick_table, tallies, *refs):
    pairs, rows, per_group, per_pair, wide, tall, cap, chunks = dims
    turned, final, scratch = refs[:chunks], refs[chunks:2 * chunks], refs[2 * chunks:]
    kinds = 7
    groups = [scratch[i * chunks:(i + 1) * chunks] for i in range(kinds)]
    held, packed, landed, lifted, risen, given, kept = groups
    sems = list(scratch[kinds * chunks:])
    row_list = sems.pop(0)
    own_sem, swap_send, swap_recv, pair_send, pair_recv, row_send, row_recv, give_send, give_recv, keep_sem = sems
    gx = lax.axis_index("gx")
    z = lax.axis_index("gy")
    pair = gx // 2
    half = lax.rem(gx, 2)
    mate = (2 * pair + 1 - half, z)

    def across(o):
        return (2 * lax.rem(pair + o, pairs) + half, z)

    def along(o):
        return (gx, lax.rem(z + o, rows))

    barrier = pltpu.get_barrier_semaphore()
    friends = [mate] + [across(o) for o in range(1, pairs)] + [along(o) for o in range(1, rows)]
    for friend in friends:
        pl.semaphore_signal(barrier, inc=1, device_id=friend, device_id_type=MESH)
    own_copies = []
    for c in range(chunks):
        own = pltpu.make_async_copy(turned[c].at[half], held[c].at[pl.ds(half * per_group, per_group)], own_sem.at[c])
        own.start()
        own_copies.append(own)
    pl.semaphore_wait(barrier, len(friends))

    swaps = []
    for c in range(chunks):
        swap = pltpu.make_async_remote_copy(
            src_ref=turned[c].at[1 - half], dst_ref=held[c].at[pl.ds(half * per_group, per_group)],
            send_sem=swap_send.at[c], recv_sem=swap_recv.at[c], device_id=mate, device_id_type=MESH)
        swap.start()
        swaps.append(swap)

    unsent = []
    pair_copies = []
    for c in range(chunks):
        own_copies[c].wait()
        swaps[c].wait_recv()
        unsent.append(swaps[c])
        sent = []
        for o in range(1, pairs):
            def pack(k, carry, o=o, c=c):
                packed[c][o - 1, k] = held[c][send_table[o * per_pair + k]]
                return carry
            lax.fori_loop(0, wide, pack, 0, unroll=4)
            copy = pltpu.make_async_remote_copy(
                src_ref=packed[c].at[o - 1], dst_ref=landed[c].at[pl.ds(o * per_pair, wide)],
                send_sem=pair_send.at[c, o - 1], recv_sem=pair_recv.at[c, o - 1],
                device_id=across(o), device_id_type=MESH)
            copy.start()
            sent.append(copy)
        unsent.extend(sent)

        def stay(k, carry, c=c):
            landed[c][k] = held[c][send_table[k]]
            return carry
        lax.fori_loop(0, per_pair, stay, 0, unroll=4)
        pair_copies.append(sent)

    for r in range(rows):
        first = tallies[r]

        def compact(k, carry, r=r, first=first):
            at = jnp.minimum(jnp.where(k < first, r * cap + k, (rows + r) * cap + k - first), 2 * rows * cap - 1)
            row_list[r * tall + k] = pick_table[at]
            return carry
        lax.fori_loop(0, tall, compact, 0, unroll=4)

    gives = []

    def settle_all(c):
        first = tallies[z]

        def settle(s, carry, c=c):
            mine = jnp.minimum(s + half * first, tall - 1)
            other = jnp.minimum(s + (1 - half) * first, tall - 1)
            for o in range(rows):
                given[c][s, o] = risen[c][o, other]
                kept[c][s, o] = risen[c][o, mine]
            return carry
        lax.fori_loop(0, cap, settle, 0)
        give = pltpu.make_async_remote_copy(
            src_ref=given[c], dst_ref=final[c].at[half],
            send_sem=give_send.at[c], recv_sem=give_recv.at[c], device_id=mate, device_id_type=MESH)
        give.start()
        keep = pltpu.make_async_copy(kept[c], final[c].at[half], keep_sem.at[c])
        keep.start()
        gives.append((give, keep))

    row_copies = []
    for c in range(chunks):
        for copy in pair_copies[c]:
            copy.wait_recv()
        sent = []
        for o in list(range(rows - 1, 0, -1)) + [0]:
            row = lax.rem(z + o, rows)

            def lift(k, carry, o=o, c=c, row=row):
                tile = landed[c][row_list[row * tall + k]]
                if o > 0:
                    lifted[c][o - 1, k] = tile
                else:
                    risen[c][0, k] = tile
                return carry
            lax.fori_loop(0, tall, lift, 0, unroll=4)
            if o > 0:
                copy = pltpu.make_async_remote_copy(
                    src_ref=lifted[c].at[o - 1], dst_ref=risen[c].at[o],
                    send_sem=row_send.at[c, o - 1], recv_sem=row_recv.at[c, o - 1],
                    device_id=along(o), device_id_type=MESH)
                copy.start()
                sent.append(copy)
        row_copies.append(sent)
        unsent.extend(sent)
    for c in range(chunks):
        for copy in row_copies[c]:
            copy.wait_recv()
        settle_all(c)
    for copy in unsent:
        copy.wait_send()
    for give, keep in gives:
        give.wait()
        keep.wait()


def finish(rows, chunks, tally, *refs):
    final, regional = refs[:-1], refs[-1]
    z = lax.axis_index("gy")
    slot = pl.program_id(0)
    side = regional.shape[3]
    times = regional.shape[0] // rows
    place = {unit: (c, i) for c, chunk in enumerate(chunks) for i, unit in enumerate(chunk)}

    @pl.when(slot < tally[0])
    def _():
        for h in range(2):
            for r in range(side // (2 * PART)):
                span = pl.ds(h * (side // 2) + r * PART, PART)
                tiles = {}
                for t in range(times):
                    c, i = place[(r, t)]
                    for o in range(rows):
                        tiles[o, t] = final[c][h, 0, o, i]
                mean = sum(tiles.values()) * jnp.float32(1.0 / (rows * times))
                for o in range(rows):
                    start = origin_of(z, rows, o, False) * times
                    for t in range(times):
                        regional[start + t, 0, 0, span, :] = tiles[o, t] - mean

    @pl.when(slot >= tally[0])
    def _():
        regional[...] = jnp.zeros_like(regional)


def levels(most, steps):
    return sorted({-(-most * s // 48) for s in steps})


def balanced_sizes(per_pair, tall):
    steps = ((38, 34, 52), (38, 36, 54), (40, 36, 56), (40, 38, 58), (42, 40, 60), (48, 46, 68), (48, 48, 96))
    return [(-(-per_pair * w // 48), -(-tall * e // 48), -(-tall * f // 48)) for w, e, f in steps]

def beside(x, step):
    return jnp.concatenate([x[step:], x[:step]], axis=0)


def plan_tables(dims, sizes, pair, zone, slot, allow):
    pairs, rows, per_group, per_pair, cap, extra = dims
    group, local, tall = 2 * per_group, 2 * rows, 2 * cap
    bins = pairs * rows
    width = zone.shape[1]
    i32, f32, bf16 = jnp.int32, jnp.float32, jnp.bfloat16
    lane = lax.broadcasted_iota(i32, (1, width), 1)
    valid = zone >= 0
    source = sum((lane >= group * k).astype(i32) for k in range(1, pairs))
    home = sum((zone >= local * k).astype(i32) for k in range(1, pairs))
    inside = zone - home * local
    side = (inside >= rows).astype(i32)
    row = inside - side * rows
    bin_at = lax.broadcasted_iota(i32, (bins, width), 0)
    before = (lax.broadcasted_iota(i32, (width, width), 0) < lax.broadcasted_iota(i32, (width, width), 1)).astype(bf16)

    def marks(key):
        return jnp.where(bin_at == jnp.where(valid, key, -1), 1.0, 0.0).astype(f32)

    def tally(mark):
        return jnp.sum(mark, axis=1, keepdims=True)

    def look(mark, table):
        return jnp.sum(mark * table, axis=0, keepdims=True)

    def ranks(mark):
        return jnp.dot(mark.astype(bf16), before, preferred_element_type=f32)

    at = lax.broadcasted_iota(i32, (bins, 128), 0)
    at_row = at & (rows - 1)
    at_home = at >> (rows.bit_length() - 1)
    edge = jnp.logical_or(at_row == 0, at_row == rows - 1)

    def flip(x, bit):
        step = 1 << bit
        if 2 * step == bins:
            return beside(x, step)
        return jnp.where((at & step) == 0, beside(x, step), beside(x, bins - step))

    across_x = lambda x: flip(x, 2)
    across_y = lambda x: flip(x, 3)
    mark = marks(home * rows + row)
    order = look(mark, ranks(mark))
    native = jnp.broadcast_to(tally(mark), (bins, 128)).astype(i32)

    def whole(x):
        x = x + across_x(x)
        return x + across_y(x)

    load = native
    half_sum = whole(native + flip(native, 0))
    goal = (jnp.maximum(half_sum, flip(half_sum, 1)) + pairs - 1) >> (pairs.bit_length() - 1)
    row_sum = (whole(native) + pairs - 1) >> (pairs.bit_length() - 1)
    end_goal = jnp.maximum(jnp.maximum(row_sum, flip(flip(row_sum, 0), 1)), (9 * goal) >> 4)
    used = [jnp.zeros_like(native), jnp.zeros_like(native)]
    for _ in range(2):
        for d, partner in enumerate((across_x, across_y)):
            for stage in range(3):
                now, want = (load, end_goal) if stage == 0 else (load + flip(load, 0), goal)
                here = jnp.logical_not(edge) if stage == 1 else edge
                move = jnp.minimum((now - partner(now)) >> 1, now - want)
                move = jnp.minimum(move, jnp.minimum(extra - used[d], native - used[0] - used[1]))
                move = jnp.where(here, jnp.maximum(move, 0), 0)
                used[d] = used[d] + move
                load = load + partner(move) - move
    first = look(mark, (used[0] * allow)[:, :1].astype(f32))
    second = look(mark, (used[1] * allow)[:, :1].astype(f32))
    leaves_x = order < first
    leaves_y = jnp.logical_and(order >= first, order < first + second)
    way = leaves_y.astype(i32)
    guest = order - jnp.where(leaves_y, first, 0.0)
    home_x = home & 1
    home_y = home >> 1
    via = jnp.where(leaves_x, home_y * 2 + 1 - home_x, jnp.where(leaves_y, (1 - home_y) * 2 + home_x, home))

    flow = marks(source * pairs + via)
    line = marks(via * rows + row)
    both = ranks(jnp.concatenate([flow, line], axis=0))
    rank = look(flow, both[:bins])
    place = look(line, both[bins:])
    flows = jnp.broadcast_to(tally(flow), (bins, 128))
    lines = jnp.broadcast_to(tally(line), (bins, 128))
    halves = lines + flip(lines, 0)
    stays = at_home == at_row
    chosen = jnp.zeros((1, 128), f32)
    for wide, end, far in sizes:
        over = jnp.where(flows > jnp.where(stays, per_pair, wide).astype(f32), 1.0, 0.0)
        over = jnp.maximum(over, jnp.where(lines > jnp.where(edge, end, tall).astype(f32), 1.0, 0.0))
        over = jnp.maximum(over, jnp.where(halves > jnp.float32(far), 1.0, 0.0))
        chosen = chosen + jnp.max(over, axis=0, keepdims=True)

    my_x, my_y = pair % 2, pair // 2

    def offset(other):
        other_y = other >> 1
        other_x = other - 2 * other_y
        return jnp.where(other_x == my_x, 0, 1) + jnp.where(other_y == my_y, 0, 2)

    def invert(here, key, value):
        key = jnp.where(jnp.logical_and(valid, here), key, -1)
        hit = jnp.where(lax.broadcasted_iota(i32, (128, width), 0) == key, 1.0, 0.0).astype(bf16)
        value = jnp.broadcast_to(value.astype(bf16), (16, width))
        return lax.dot_general(value, hit, (((1,), (1,)), ((), ())), preferred_element_type=f32)[:1]

    rank = rank.astype(i32)
    place = place.astype(i32)
    guest = guest.astype(i32)
    landing = offset(source) * per_pair + rank
    mine = via == pair
    ours = home == pair
    return chosen, [
        invert(source == pair, offset(via) * per_pair + rank, (lane - group * pair).astype(f32)),
        invert(mine, row * tall + place, landing.astype(f32)),
        invert(jnp.logical_and(mine, home != pair), (way * rows + row) * extra + guest, place.astype(f32)),
        invert(ours, (side * rows + row) * cap + slot, jnp.where(mine, place, tall + way * extra + guest).astype(f32)),
        invert(mine, row, jnp.ones((1, width), f32)),
        invert(ours, side * rows + row, jnp.ones((1, width), f32)),
    ]


def prepare_balanced(dims, sizes, zone, slot, table, choice, padded):
    pair = lax.axis_index("gx") // 2
    padded[...] = jnp.full_like(padded, -1)
    padded[0:1, 0:zone.shape[1]] = zone[...]
    padded[1:2, 0:zone.shape[1]] = slot[...]

    def fill(sizes, allow):
        chosen, lines = plan_tables(dims, sizes, pair, padded[0:1], padded[1:2], allow)
        for k, line in enumerate(lines):
            table[k:k + 1] = line.astype(jnp.int32)
        return jnp.max(chosen).astype(jnp.int32)

    chosen = fill(sizes, 1)
    choice[0] = jnp.minimum(chosen, len(sizes) - 1)

    @pl.when(chosen == len(sizes))
    def _():
        fill(sizes[:0], 0)


def mirror_rows(block):
    side = block.shape[0]
    row = PART - 1 - lax.broadcasted_iota(jnp.int32, (PART, block.shape[1]), 0)
    parts = [block[r - PART:r] for r in range(side, 0, -PART)]
    return jnp.concatenate([jnp.take_along_axis(part, row, axis=0) for part in parts], axis=0)


def turn(block, code):
    block = jnp.where(jnp.logical_or(code == 1, code == 2), mirror_lanes(block), block)
    block = jnp.where(code >= 2, mirror_rows(block), block)
    return jnp.where(jnp.logical_or(code == 1, code == 3), block.T, block)


def exchange_balanced(dims, chunks, table, spins, field, regional, *scratch):
    pairs, rows, per_group, per_pair, cap, extra, wide, end, far = dims
    tall = 2 * cap
    count = len(chunks)
    times, _, side, _ = field.shape
    strips = side // (2 * PART)
    kinds = 12
    groups = [scratch[i * count:(i + 1) * count] for i in range(kinds)]
    held, swapped, packed, landed, lifted, risen, pooled, crossed_in, crossed_out, passed, leaving, visiting = groups
    crossed = (crossed_in, crossed_out)
    raw, given, far_list, *sems = scratch[kinds * count:]
    raw_sem, swap_send, swap_recv, pair_send, pair_recv, near_send, near_recv = sems[:7]
    give_send, give_recv, far_send, far_recv, pass_send, pass_recv, side_send, side_recv = sems[7:]
    unit_at = {unit: (c, i) for c, chunk in enumerate(chunks) for i, unit in enumerate(chunk)}
    gx = lax.axis_index("gx")
    z = lax.axis_index("gy")
    pair = gx // 2
    half = lax.rem(gx, 2)
    mate = (2 * pair + 1 - half, z)
    pair_x = lax.rem(pair, 2)
    pair_y = pair // 2
    near, far_in, far_out = (origin_of(z, rows, k, True) for k in (1, 2, 3))
    inner = jnp.logical_or(z == 1, z == 2)
    outer = jnp.logical_not(inner)

    def across(o):
        x = 1 - pair_x if o % 2 else pair_x
        y = 1 - pair_y if o // 2 else pair_y
        return (2 * (2 * y + x) + half, z)

    loads = []
    for t in range(times):
        loads.append(pltpu.make_async_copy(field.at[t], raw.at[pl.ds(t * per_group, per_group)], raw_sem.at[t]))
        loads[t].start()

    barrier = pltpu.get_barrier_semaphore()
    friends = [mate] + [across(o) for o in range(1, pairs)] + [(gx, lax.rem(z + o, rows)) for o in range(1, rows)]
    for friend in friends:
        pl.semaphore_signal(barrier, inc=1, device_id=friend, device_id_type=MESH)

    def turn_time(t):
        loads[t].wait()

        def one(b, carry):
            block = turn(raw[t * per_group + b], spins[gx * per_group + b])
            for r in range(strips):
                c, i = unit_at[r, t]
                top = block[r * PART:(r + 1) * PART]
                bottom = block[side // 2 + r * PART:side // 2 + (r + 1) * PART]
                held[c][half * per_group + b, i] = jnp.where(half == 0, top, bottom)
                swapped[c][b, i] = jnp.where(half == 0, bottom, top)
            return carry
        lax.fori_loop(0, per_group, one, 0, unroll=4)

    def wait_sent(sem, blocks):
        span = raw.at[pl.ds(0, blocks)]
        pltpu.make_async_copy(span, span, sem).wait()

    turn_time(0)
    pl.semaphore_wait(barrier, len(friends))

    swaps = {}

    def swap_time(t):
        for c in sorted({unit_at[r, t][0] for r in range(strips)}):
            swaps[c] = pltpu.make_async_remote_copy(
                src_ref=swapped[c], dst_ref=held[c].at[pl.ds(half * per_group, per_group)],
                send_sem=swap_send.at[0], recv_sem=swap_recv.at[c], device_id=mate, device_id_type=MESH)
            swaps[c].start()

    swap_time(0)

    def send_pairs(c):
        if c == 1:
            for t in range(1, times):
                turn_time(t)
                swap_time(t)
        swaps[c].wait_recv()
        sent = []
        for o in range(1, pairs):
            def pack(k, carry, o=o):
                packed[c][o - 1, k] = held[c][table[0, o * per_pair + k]]
                return carry
            lax.fori_loop(0, wide, pack, 0, unroll=4)
            sent.append(pltpu.make_async_remote_copy(
                src_ref=packed[c].at[o - 1], dst_ref=landed[c].at[pl.ds(o * per_pair, wide)],
                send_sem=pair_send.at[o - 1], recv_sem=pair_recv.at[c],
                device_id=across(o), device_id_type=MESH))

        @pl.when(half == 0)
        def _():
            for copy in sent:
                copy.start()

        @pl.when(half == 1)
        def _():
            for copy in sent[::-1]:
                copy.start()

        def stay(k, carry):
            landed[c][k] = held[c][table[0, k]]
            return carry
        lax.fori_loop(0, per_pair, stay, 0, unroll=4)

        if c == 0:
            lead = table[4, far_in]

            def gather_far(k, carry):
                at = jnp.where(k < lead, far_in * tall + k, far_out * tall + k - lead)
                far_list[k] = table[1, jnp.minimum(at, rows * tall - 1)]
                return carry
            lax.fori_loop(0, far, gather_far, 0, unroll=4)

    skip = table[4, z]

    def near_copy(c, size):
        return pltpu.make_async_remote_copy(
            src_ref=lifted[c].at[pl.ds(0, size)], dst_ref=risen[c].at[1, pl.ds(0, size)],
            send_sem=near_send.at[0], recv_sem=near_recv.at[c],
            device_id=(gx, near), device_id_type=MESH)

    def far_copy(c, place):
        return pltpu.make_async_remote_copy(
            src_ref=pooled[c], dst_ref=crossed[place][c],
            send_sem=far_send.at[0], recv_sem=far_recv.at[c, place],
            device_id=(gx, far_in), device_id_type=MESH)

    def pass_copy(c, place):
        return pltpu.make_async_remote_copy(
            src_ref=passed[c].at[place], dst_ref=risen[c].at[2 + place, pl.ds(0, end)],
            send_sem=pass_send.at[0], recv_sem=pass_recv.at[c],
            device_id=(gx, near), device_id_type=MESH)

    def side_copy(c, d):
        return pltpu.make_async_remote_copy(
            src_ref=leaving[c].at[d], dst_ref=visiting[c].at[d],
            send_sem=side_send.at[0], recv_sem=side_recv.at[c],
            device_id=across(1 + d), device_id_type=MESH)

    def send_rows(c):
        pltpu.make_async_copy(packed[c], packed[c], pair_recv.at[c]).wait()

        def pool(k, carry):
            pooled[c][k] = landed[c][far_list[k]]
            return carry
        lax.fori_loop(0, far, pool, 0, unroll=4)

        def lift(k, carry):
            lifted[c][k] = landed[c][table[1, near * tall + k]]
            return carry
        lax.fori_loop(0, tall, lift, 0, unroll=4)

        def send_far():
            for place, mine in enumerate((inner, outer)):
                @pl.when(mine)
                def _(place=place):
                    far_copy(c, place).start()

        @pl.when(half == 0)
        def _():
            send_far()

        @pl.when(inner)
        def _():
            near_copy(c, end).start()

        @pl.when(outer)
        def _():
            near_copy(c, tall).start()

        @pl.when(half == 1)
        def _():
            send_far()

        def own(k, carry):
            risen[c][0, k] = landed[c][table[1, z * tall + k]]
            return carry
        lax.fori_loop(0, tall, own, 0, unroll=4)

    def hand_on(c, place):
        @pl.when(inner)
        def _():
            far_copy(c, place).wait_recv()

            def onward(k, carry):
                passed[c][place, k] = crossed[place][c][jnp.minimum(skip + k, far - 1)]
                return carry
            lax.fori_loop(0, end, onward, 0, unroll=4)
            pass_copy(c, place).start()

            def land(k, carry):
                risen[c][2 + place, k] = crossed[place][c][k]
                return carry
            lax.fori_loop(0, tall, land, 0, unroll=4)

    def hand_on_inner(c):
        hand_on(c, 0)

    def hand_on_outer(c):
        hand_on(c, 1)

    def send_sides(c):
        @pl.when(inner)
        def _():
            near_copy(c, tall).wait_recv()

        @pl.when(outer)
        def _():
            near_copy(c, end).wait_recv()
            pltpu.make_async_copy(passed[c], passed[c], pass_recv.at[c]).wait()

        for d in range(2):
            def leave(k, carry, d=d):
                at = table[2, (d * rows + z) * extra + k]
                for o in range(rows):
                    leaving[c][d, o, k] = risen[c][o, at]
                return carry
            lax.fori_loop(0, extra, leave, 0)
            side_copy(c, d).start()

    def settle(c):
        pltpu.make_async_copy(visiting[c], visiting[c], side_recv.at[c]).wait()
        for r, _ in chunks[c]:
            if max(unit_at[r, t][0] for t in range(times)) == c:
                settle_strip(r)

    def settle_strip(r):
        span = pl.ds(pl.multiple_of(half * (side // 2) + r * PART, PART), PART)

        def place(s, carry):
            for core in (1 - half, half):
                at = table[3, (core * rows + z) * cap + s]
                live = s < table[5, core * rows + z]
                guest = jnp.maximum(at - tall, 0)
                way = guest // extra
                tiles = {}
                for t in range(times):
                    c, i = unit_at[r, t]
                    for o in range(rows):
                        home = risen[c][o, jnp.minimum(at, tall - 1), i]
                        visitor = visiting[c][way, o, guest - way * extra, i]
                        tiles[o, t] = jnp.where(at < tall, home, visitor)
                mean = sum(tiles.values()) * jnp.float32(1.0 / (rows * times))
                for (o, t), tile in tiles.items():
                    value = jnp.where(live, tile - mean, 0.0)
                    if core is half:
                        regional[origin_of(z, rows, o, True) * times + t, 0, s, span, :] = value
                    else:
                        given[r, origin_of(z, rows, o, True) * times + t, s] = value
            return carry
        lax.fori_loop(0, cap, place, 0)
        give = pltpu.make_async_remote_copy(
            src_ref=given.at[r], dst_ref=regional.at[:, 0, :, span, :],
            send_sem=give_send.at[0], recv_sem=give_recv.at[0], device_id=mate, device_id_type=MESH)
        give.start()

    starts = []
    for chunk in chunks:
        begin = starts[-1][1] if starts else 0
        starts.append((begin, begin + len(chunk)))
    for _, _, c, act in timetable(starts, wide, tall, end, far, extra, (send_pairs, send_rows, hand_on_outer, hand_on_inner, send_sides, settle)):
        act(c)

    wait_sent(swap_send.at[0], per_group)
    for o in range(1, pairs):
        wait_sent(pair_send.at[o - 1], wide)
    wait_sent(far_send.at[0], far)
    wait_sent(side_send.at[0], 2 * rows * extra)

    @pl.when(inner)
    def _():
        wait_sent(near_send.at[0], end)
        wait_sent(pass_send.at[0], 2 * end)

    @pl.when(outer)
    def _():
        wait_sent(near_send.at[0], tall)

    wait_sent(give_send.at[0], rows * cap)
    wait_sent(give_recv.at[0], rows * cap)


def timetable(starts, wide, tall, end, far, extra, acts):
    hop = 60
    sent = soon = crossed = passed = 0.0
    busy = 4 * wide * starts[-1][1]
    events = []
    for c, (begin, close) in enumerate(starts):
        size = close - begin
        sent = sent + 4 * wide * size
        landed = sent + hop
        soon = max(soon, landed) + 1.9 * (tall + far) * size
        crossed = max(crossed, landed) + 4 * far * size
        passed = max(passed, crossed + hop) + 4 * end * size
        sides = passed + hop
        busy = max(busy, sides) + 8 * extra * size
        for k, at in enumerate((0.0, landed, soon + hop, crossed + hop, sides, busy + 2 * hop)):
            events.append((at, k, c, acts[k]))
    return sorted(events, key=lambda e: e[:3])


def on_device(field, zone, slot, spins, tally):
    times, per_group, side, _ = field.shape
    columns = lax.axis_size("gx")
    rows = lax.axis_size("gy")
    pairs = columns // 2
    cap = 2 * per_group // rows
    per_pair = 4 * (2 * per_group // columns)
    balanced = rows == 4 and pairs == 4 and times == 2 and columns * per_group < 256 and 2 * rows * cap <= 128 and pairs * per_pair <= 128
    if balanced:
        return balanced_exchange(field, zone, slot, spins, cap, per_pair)
    chunks = chunk_units(times, side)
    tiles = [(len(chunk), PART, side) for chunk in chunks]
    final = plain_exchange(field, zone, slot, spins, chunks, tiles, cap, per_pair)
    return pl.pallas_call(
        functools.partial(finish, rows, chunks),
        grid_spec=pltpu.PrefetchScalarGridSpec(
            num_scalar_prefetch=1,
            grid=(cap,),
            in_specs=[pl.BlockSpec(
                (2, 1, rows) + tile,
                lambda s, count: (0, jnp.maximum(jnp.minimum(s, count[0] - 1), 0), 0, 0, 0, 0)) for tile in tiles],
            out_specs=pl.BlockSpec((rows * times, 1, 1, side, side), lambda s, count: (0, 0, s, 0, 0)),
        ),
        out_shape=jax.ShapeDtypeStruct((rows * times, 1, cap, side, side), jnp.float32),
        name="finish",
    )(tally, *final)


def scratch_of(tiles, *shapes):
    return [pltpu.VMEM(lead + tile, jnp.float32) for lead in shapes for tile in tiles]


def balanced_exchange(field, zone, slot, spins, cap, per_pair):
    times, per_group, side, _ = field.shape
    columns = lax.axis_size("gx")
    rows = lax.axis_size("gy")
    pairs = columns // 2
    tall = 2 * cap
    extra = cap // 3
    chunks = time_major(times, side)
    tiles = [(len(chunk), PART, side) for chunk in chunks]
    count = len(chunks)
    strips = side // (2 * PART)
    smem = pl.BlockSpec(memory_space=pltpu.SMEM)
    vmem = pl.BlockSpec(memory_space=pltpu.VMEM)
    sizes = balanced_sizes(per_pair, tall)
    lanes = -(-columns * per_group // 128) * 128
    table, choice = pl.pallas_call(
        functools.partial(prepare_balanced, (pairs, rows, per_group, per_pair, cap, extra), sizes),
        in_specs=[vmem, vmem],
        out_specs=[vmem, smem],
        out_shape=[jax.ShapeDtypeStruct((8, 128), jnp.int32), jax.ShapeDtypeStruct((1,), jnp.int32)],
        scratch_shapes=[pltpu.VMEM((8, lanes), jnp.int32)],
        name="prepare",
    )(zone.reshape(1, -1), slot.reshape(1, -1))

    def moved(wide, end, far, tag):
        dma = pltpu.SemaphoreType.DMA
        buffers = [
            *scratch_of(
                tiles, (2 * per_group,), (per_group,), (pairs - 1, wide), (pairs * per_pair,), (tall,), (rows, tall),
                (far,), (far,), (far,), (2, end), (2, rows, extra), (2, rows, extra)),
            pltpu.VMEM((max(times * per_group, rows * cap, 2 * end, far), side, side), jnp.float32),
            pltpu.VMEM((strips, rows * times, cap, PART, side), jnp.float32),
            pltpu.SMEM((far,), jnp.int32),
            dma((times,)), dma((1,)), dma((count,)), dma((pairs - 1,)), dma((count,)), dma((1,)), dma((count,)),
            dma((1,)), dma((1,)), dma((1,)), dma((count, 2)), dma((1,)), dma((count,)), dma((1,)), dma((count,)),
        ]
        return lambda: pl.pallas_call(
            functools.partial(
                exchange_balanced, (pairs, rows, per_group, per_pair, cap, extra, wide, end, far), chunks),
            in_specs=[smem, smem, pl.BlockSpec(memory_space=pl.ANY)],
            out_specs=vmem,
            out_shape=pltpu.VMEM((rows * times, 1, cap, side, side), jnp.float32),
            scratch_shapes=buffers,
            compiler_params=pltpu.CompilerParams(collective_id=tag, has_side_effects=True, vmem_limit_bytes=VMEM_BYTES),
            name=f"exchange_{tag}",
        )(table, spins, field)

    return lax.switch(choice[0], [moved(*size, tag) for tag, size in enumerate(sizes)])


def plain_exchange(field, zone, slot, spins, chunks, tiles, cap, per_pair):
    times, per_group, side, _ = field.shape
    columns = lax.axis_size("gx")
    rows = lax.axis_size("gy")
    pairs = columns // 2
    per_row = 2 * cap
    smem = pl.BlockSpec(memory_space=pltpu.SMEM)
    anywhere = pl.BlockSpec(memory_space=pl.ANY)
    i32 = jnp.int32
    narrow = levels(per_pair, (40,))[0]
    sizes = [(narrow, tall) for tall in levels(per_row, (36, 42))]
    sizes.append((per_pair, per_row))
    *turned, send_table, pick_table, tallies, choice = pl.pallas_call(
        functools.partial(prepare, (pairs, rows, per_group, per_pair, cap, chunks, sizes)),
        grid=(per_group // STEP_BLOCKS,),
        in_specs=[smem, smem, smem, pl.BlockSpec((times, STEP_BLOCKS, side, side), lambda i: (0, i, 0, 0))],
        out_specs=[
            *[pl.BlockSpec((2, STEP_BLOCKS) + tile, lambda i: (0, i, 0, 0, 0)) for tile in tiles],
            smem, smem, smem, smem,
        ],
        out_shape=[
            *[jax.ShapeDtypeStruct((2, per_group) + tile, jnp.float32) for tile in tiles],
            jax.ShapeDtypeStruct((pairs * per_pair + 1,), i32),
            jax.ShapeDtypeStruct((per_row * rows + 1,), i32),
            jax.ShapeDtypeStruct((2 * rows,), i32),
            jax.ShapeDtypeStruct((1,), i32),
        ],
        scratch_shapes=[pltpu.SMEM((columns * rows,), i32), pltpu.SMEM((pairs * pairs,), i32)],
        name="prepare",
    )(zone, slot, spins, field)
    count = len(chunks)

    def moved(wide, tall, tag):
        dma = pltpu.SemaphoreType.DMA
        buffers = [
            *scratch_of(
                tiles, (2 * per_group,), (pairs - 1, wide), (pairs * per_pair,), (rows - 1, tall), (rows, tall),
                (cap, rows), (cap, rows)),
            pltpu.SMEM((rows * tall,), i32),
            dma((count,)), dma((count,)), dma((count,)),
            dma((count, pairs - 1)), dma((count, pairs - 1)),
            dma((count, rows - 1)), dma((count, rows - 1)),
            dma((count,)), dma((count,)), dma((count,)),
        ]
        return lambda: pl.pallas_call(
            functools.partial(exchange, (pairs, rows, per_group, per_pair, wide, tall, cap, count)),
            in_specs=[smem, smem, smem] + [anywhere] * count,
            out_specs=[anywhere] * count,
            out_shape=[jax.ShapeDtypeStruct((2, cap, rows) + tile, jnp.float32) for tile in tiles],
            scratch_shapes=buffers,
            compiler_params=pltpu.CompilerParams(collective_id=tag, has_side_effects=True, vmem_limit_bytes=60 * 2**20),
            name=f"exchange_{tag}",
        )(send_table, pick_table, tallies, *turned)

    return lax.switch(choice[0], [moved(*size, tag) for tag, size in enumerate(sizes)])


def solution(mesh):
    placed = (P("gy", "gx", None, None), P(), P(), P(), P(("gx", "gy")))
    return jax.shard_map(
        on_device,
        mesh=mesh,
        in_specs=placed,
        out_specs=P(None, ("gx", "gy"), None, None, None),
        check_vma=False,
    )
```

```python
import functools

import jax
import jax.numpy as jnp
from jax import lax
from jax.experimental import pallas as pl
from jax.experimental.pallas import tpu as pltpu
from jax.sharding import PartitionSpec as P

MESH = pl.DeviceIdType.MESH
PART = 8
STEP_BLOCKS = 4
VMEM_BYTES = 52 * 2**20


def chunk_units(times, side):
    units = [(r, t) for r in range(side // (2 * PART)) for t in range(times)]
    small = 2 * (times // 2 + times % 2)
    cuts = list(range(0, small + 1, max(times // 2, 1)))
    cuts += list(range(small + times, len(units) - small + 1, times))
    cuts += list(range(len(units) - small + max(times // 2, 1), len(units) + 1, max(times // 2, 1)))
    return [units[a:b] for a, b in zip(cuts[:-1], cuts[1:])]


def time_major(times, side):
    units = [(r, t) for t in range(times) for r in range(side // (2 * PART))]
    sizes = [1, 1] + [2] * ((len(units) - 4) // 2) + [1, 1]
    cuts = [sum(sizes[:c]) for c in range(len(sizes) + 1)]
    return [units[a:b] for a, b in zip(cuts[:-1], cuts[1:])]


def mirror_lanes(block):
    side = block.shape[1]
    lane = side - 1 - lax.broadcasted_iota(jnp.int32, block.shape, 1)
    return jnp.take_along_axis(block, lane, axis=1)


def turn_blocks(first, chunks, spins, field, turned):
    times, blocks, side, _ = field.shape
    for b in range(blocks):
        code = spins[first + b]
        for kind in range(4):
            @pl.when(code == kind)
            def _(kind=kind, b=b):
                for t in range(times):
                    block = field[t, b]
                    if kind == 1:
                        block = mirror_lanes(block).T
                    elif kind == 2:
                        block = mirror_lanes(mirror_lanes(block).T).T
                    elif kind == 3:
                        block = mirror_lanes(block.T)
                    for c, chunk in enumerate(chunks):
                        for i, (r, at) in enumerate(chunk):
                            if at == t:
                                for h in range(2):
                                    top = h * (side // 2) + r * PART
                                    turned[c][h, b, i] = block[top:top + PART]


def prepare(dims, zone, slot, spins, field, *refs):
    pairs, rows, per_group, per_pair, cap, chunks, sizes = dims
    turned = refs[:len(chunks)]
    send_table, pick_table, tallies, choice, counts, fills = refs[len(chunks):]
    gx = lax.axis_index("gx")
    pair = gx // 2
    group = 2 * per_group
    local = 2 * rows
    step = pl.program_id(0)

    @pl.when(step == 0)
    def _():
        def clear(ref, size):
            def body(i, c):
                ref[i] = 0
                return c
            lax.fori_loop(0, size, body, 0, unroll=8)
        clear(send_table, pairs * per_pair + 1)
        clear(pick_table, local * cap + 1)
        clear(counts, pairs * local)
        clear(fills, pairs * pairs)

        for source in range(pairs):
            behind = lax.rem(pair - source + pairs, pairs) * per_pair

            def place(j, c, source=source, behind=behind):
                region = zone[source * group + j]
                counts[region] = counts[region] + 1
                target = region // local
                cell = source * pairs + target
                rank = fills[cell]
                fills[cell] = rank + 1
                ahead = lax.rem(target - source + pairs, pairs) * per_pair
                send_table[jnp.where(source == pair, ahead + rank, pairs * per_pair)] = j
                at = (region - target * local) * cap + slot[source * group + j]
                pick_table[jnp.where(target == pair, at, local * cap)] = behind + rank
                return c
            lax.fori_loop(0, group, place, 0, unroll=4)
        most_pair = jnp.int32(0)
        most_row = jnp.int32(0)
        for q in range(pairs):
            for r in range(pairs):
                if q != r:
                    most_pair = jnp.maximum(most_pair, fills[q * pairs + r])
            pooled = [counts[q * local + r] + counts[q * local + rows + r] for r in range(rows)]
            for value in pooled:
                most_row = jnp.maximum(most_row, value)
        for r in range(local):
            tallies[r] = counts[pair * local + r]
        chosen = jnp.int32(len(sizes) - 1)
        for at in range(len(sizes) - 2, -1, -1):
            wide, tall = sizes[at]
            fits = jnp.logical_and(most_pair <= wide, most_row <= tall)
            chosen = jnp.where(fits, at, chosen)
        choice[0] = chosen

    turn_blocks(gx * per_group + step * field.shape[1], chunks, spins, field, turned)


def origin_of(z, rows, k, relay):
    if not relay:
        return lax.rem(z - k + rows, rows)
    low = z < 2
    return [z, z + 1 - 2 * lax.rem(z, 2), jnp.where(low, 2, 1), jnp.where(low, 3, 0)][k]


def exchange(dims, send_table, pick_table, tallies, *refs):
    pairs, rows, per_group, per_pair, wide, tall, cap, chunks = dims
    turned, final, scratch = refs[:chunks], refs[chunks:2 * chunks], refs[2 * chunks:]
    kinds = 7
    groups = [scratch[i * chunks:(i + 1) * chunks] for i in range(kinds)]
    held, packed, landed, lifted, risen, given, kept = groups
    sems = list(scratch[kinds * chunks:])
    row_list = sems.pop(0)
    own_sem, swap_send, swap_recv, pair_send, pair_recv, row_send, row_recv, give_send, give_recv, keep_sem = sems
    gx = lax.axis_index("gx")
    z = lax.axis_index("gy")
    pair = gx // 2
    half = lax.rem(gx, 2)
    mate = (2 * pair + 1 - half, z)

    def across(o):
        return (2 * lax.rem(pair + o, pairs) + half, z)

    def along(o):
        return (gx, lax.rem(z + o, rows))

    barrier = pltpu.get_barrier_semaphore()
    friends = [mate] + [across(o) for o in range(1, pairs)] + [along(o) for o in range(1, rows)]
    for friend in friends:
        pl.semaphore_signal(barrier, inc=1, device_id=friend, device_id_type=MESH)
    own_copies = []
    for c in range(chunks):
        own = pltpu.make_async_copy(turned[c].at[half], held[c].at[pl.ds(half * per_group, per_group)], own_sem.at[c])
        own.start()
        own_copies.append(own)
    pl.semaphore_wait(barrier, len(friends))

    swaps = []
    for c in range(chunks):
        swap = pltpu.make_async_remote_copy(
            src_ref=turned[c].at[1 - half], dst_ref=held[c].at[pl.ds(half * per_group, per_group)],
            send_sem=swap_send.at[c], recv_sem=swap_recv.at[c], device_id=mate, device_id_type=MESH)
        swap.start()
        swaps.append(swap)

    unsent = []
    pair_copies = []
    for c in range(chunks):
        own_copies[c].wait()
        swaps[c].wait_recv()
        unsent.append(swaps[c])
        sent = []
        for o in range(1, pairs):
            def pack(k, carry, o=o, c=c):
                packed[c][o - 1, k] = held[c][send_table[o * per_pair + k]]
                return carry
            lax.fori_loop(0, wide, pack, 0, unroll=4)
            copy = pltpu.make_async_remote_copy(
                src_ref=packed[c].at[o - 1], dst_ref=landed[c].at[pl.ds(o * per_pair, wide)],
                send_sem=pair_send.at[c, o - 1], recv_sem=pair_recv.at[c, o - 1],
                device_id=across(o), device_id_type=MESH)
            copy.start()
            sent.append(copy)
        unsent.extend(sent)

        def stay(k, carry, c=c):
            landed[c][k] = held[c][send_table[k]]
            return carry
        lax.fori_loop(0, per_pair, stay, 0, unroll=4)
        pair_copies.append(sent)

    for r in range(rows):
        first = tallies[r]

        def compact(k, carry, r=r, first=first):
            at = jnp.minimum(jnp.where(k < first, r * cap + k, (rows + r) * cap + k - first), 2 * rows * cap - 1)
            row_list[r * tall + k] = pick_table[at]
            return carry
        lax.fori_loop(0, tall, compact, 0, unroll=4)

    gives = []

    def settle_all(c):
        first = tallies[z]

        def settle(s, carry, c=c):
            mine = jnp.minimum(s + half * first, tall - 1)
            other = jnp.minimum(s + (1 - half) * first, tall - 1)
            for o in range(rows):
                given[c][s, o] = risen[c][o, other]
                kept[c][s, o] = risen[c][o, mine]
            return carry
        lax.fori_loop(0, cap, settle, 0)
        give = pltpu.make_async_remote_copy(
            src_ref=given[c], dst_ref=final[c].at[half],
            send_sem=give_send.at[c], recv_sem=give_recv.at[c], device_id=mate, device_id_type=MESH)
        give.start()
        keep = pltpu.make_async_copy(kept[c], final[c].at[half], keep_sem.at[c])
        keep.start()
        gives.append((give, keep))

    row_copies = []
    for c in range(chunks):
        for copy in pair_copies[c]:
            copy.wait_recv()
        sent = []
        for o in list(range(rows - 1, 0, -1)) + [0]:
            row = lax.rem(z + o, rows)

            def lift(k, carry, o=o, c=c, row=row):
                tile = landed[c][row_list[row * tall + k]]
                if o > 0:
                    lifted[c][o - 1, k] = tile
                else:
                    risen[c][0, k] = tile
                return carry
            lax.fori_loop(0, tall, lift, 0, unroll=4)
            if o > 0:
                copy = pltpu.make_async_remote_copy(
                    src_ref=lifted[c].at[o - 1], dst_ref=risen[c].at[o],
                    send_sem=row_send.at[c, o - 1], recv_sem=row_recv.at[c, o - 1],
                    device_id=along(o), device_id_type=MESH)
                copy.start()
                sent.append(copy)
        row_copies.append(sent)
        unsent.extend(sent)
    for c in range(chunks):
        for copy in row_copies[c]:
            copy.wait_recv()
        settle_all(c)
    for copy in unsent:
        copy.wait_send()
    for give, keep in gives:
        give.wait()
        keep.wait()


def finish(rows, chunks, tally, *refs):
    final, regional = refs[:-1], refs[-1]
    z = lax.axis_index("gy")
    slot = pl.program_id(0)
    side = regional.shape[3]
    times = regional.shape[0] // rows
    place = {unit: (c, i) for c, chunk in enumerate(chunks) for i, unit in enumerate(chunk)}

    @pl.when(slot < tally[0])
    def _():
        for h in range(2):
            for r in range(side // (2 * PART)):
                span = pl.ds(h * (side // 2) + r * PART, PART)
                tiles = {}
                for t in range(times):
                    c, i = place[(r, t)]
                    for o in range(rows):
                        tiles[o, t] = final[c][h, 0, o, i]
                mean = sum(tiles.values()) * jnp.float32(1.0 / (rows * times))
                for o in range(rows):
                    start = origin_of(z, rows, o, False) * times
                    for t in range(times):
                        regional[start + t, 0, 0, span, :] = tiles[o, t] - mean

    @pl.when(slot >= tally[0])
    def _():
        regional[...] = jnp.zeros_like(regional)


def levels(most, steps):
    return sorted({-(-most * s // 48) for s in steps})


def balanced_sizes(per_pair, tall):
    steps = (
        (36, 34, 52), (36, 36, 54), (38, 36, 56), (42, 38, 56), (38, 38, 58), (40, 40, 60), (44, 44, 64), (48, 48, 70),
        (48, 48, 96))
    return [(-(-per_pair * w // 48), -(-tall * e // 48), -(-tall * f // 48)) for w, e, f in steps]

def beside(x, step):
    return jnp.concatenate([x[step:], x[:step]], axis=0)


def plan_tables(dims, sizes, pair, zone, slot, allow):
    pairs, rows, per_group, per_pair, cap, extra = dims
    group, local, tall = 2 * per_group, 2 * rows, 2 * cap
    bins = pairs * rows
    width = zone.shape[1]
    i32, f32, bf16 = jnp.int32, jnp.float32, jnp.bfloat16
    lane = lax.broadcasted_iota(i32, (1, width), 1)
    valid = zone >= 0
    source = sum((lane >= group * k).astype(i32) for k in range(1, pairs))
    home = sum((zone >= local * k).astype(i32) for k in range(1, pairs))
    inside = zone - home * local
    side = (inside >= rows).astype(i32)
    row = inside - side * rows
    bin_at = lax.broadcasted_iota(i32, (bins, width), 0)
    before = (lax.broadcasted_iota(i32, (width, width), 0) < lax.broadcasted_iota(i32, (width, width), 1)).astype(bf16)

    def marks(key):
        return jnp.where(bin_at == jnp.where(valid, key, -1), 1.0, 0.0).astype(f32)

    def tally(mark):
        return jnp.sum(mark, axis=1, keepdims=True)

    def look(mark, table):
        return jnp.sum(mark * table, axis=0, keepdims=True)

    def ranks(mark):
        return jnp.dot(mark.astype(bf16), before, preferred_element_type=f32)

    spot = lax.broadcasted_iota(i32, (bins, 128), 0)
    at_row = spot & (rows - 1)
    at_home = spot >> (rows.bit_length() - 1)
    edge = jnp.logical_or(at_row == 0, at_row == rows - 1)

    def flip(x, bit):
        step = 1 << bit
        if 2 * step == bins:
            return beside(x, step)
        return jnp.where((spot & step) == 0, beside(x, step), beside(x, bins - step))

    across_x = lambda x: flip(x, 2)
    across_y = lambda x: flip(x, 3)
    mark = marks(home * rows + row)
    home_x = home & 1
    home_y = home >> 1
    beside_x = home_y * 2 + 1 - home_x
    beside_y = (1 - home_y) * 2 + home_x
    kinds = [source == beside_x, jnp.logical_and(source != beside_x, source != beside_y), source == beside_y]
    split = [jnp.where(kind, mark, 0.0) for kind in kinds]
    split_ranks = ranks(jnp.concatenate(split, axis=0))
    counts = [tally(part) for part in split]
    order = sum(look(part, split_ranks[k * bins:(k + 1) * bins] + sum(counts[:k])) for k, part in enumerate(split))
    total = sum(counts)
    native = jnp.broadcast_to(total, (bins, 128)).astype(i32)

    def whole(x):
        x = x + across_x(x)
        return x + across_y(x)

    load = native
    half_sum = whole(native + flip(native, 0))
    goal = (jnp.maximum(half_sum, flip(half_sum, 1)) + pairs - 1) >> (pairs.bit_length() - 1)
    row_sum = (whole(native) + pairs - 1) >> (pairs.bit_length() - 1)
    end_goal = jnp.maximum(jnp.maximum(row_sum, flip(flip(row_sum, 0), 1)), (9 * goal) >> 4)
    used = [jnp.zeros_like(native), jnp.zeros_like(native)]
    for _ in range(2):
        for d, partner in enumerate((across_x, across_y)):
            for stage in range(3):
                now, want = (load, end_goal) if stage == 0 else (load + flip(load, 0), goal)
                here = jnp.logical_not(edge) if stage == 1 else edge
                move = jnp.minimum((now - partner(now)) >> 1, now - want)
                move = jnp.minimum(move, jnp.minimum(extra - used[d], native - used[0] - used[1]))
                move = jnp.where(here, jnp.maximum(move, 0), 0)
                used[d] = used[d] + move
                load = load + partner(move) - move
    first = look(mark, (used[0] * allow)[:, :1].astype(f32))
    second = look(mark, (used[1] * allow)[:, :1].astype(f32))
    leaves_x = order < first
    keeps = look(mark, total) - second
    leaves_y = order >= keeps
    way = leaves_y.astype(i32)
    guest = order - jnp.where(leaves_y, keeps, 0.0)
    via = jnp.where(leaves_x, beside_x, jnp.where(leaves_y, beside_y, home))

    flow = marks(source * pairs + via)
    line = marks(via * rows + row)
    both = ranks(jnp.concatenate([flow, line], axis=0))
    rank = look(flow, both[:bins])
    place = look(line, both[bins:])
    flows = jnp.broadcast_to(tally(flow), (bins, 128))
    lines = jnp.broadcast_to(tally(line), (bins, 128))
    halves = lines + flip(lines, 0)
    stays = at_home == at_row
    chosen = jnp.full((1, 128), len(sizes), i32)
    for at, (wide, end, far) in reversed(list(enumerate(sizes))):
        over = jnp.where(flows > jnp.where(stays, per_pair + 2 * extra, wide).astype(f32), 1.0, 0.0)
        over = jnp.maximum(over, jnp.where(lines > jnp.where(edge, end, tall).astype(f32), 1.0, 0.0))
        over = jnp.maximum(over, jnp.where(halves > jnp.float32(far), 1.0, 0.0))
        chosen = jnp.where(jnp.max(over, axis=0, keepdims=True) > 0.0, chosen, at)

    my_x, my_y = pair % 2, pair // 2

    def offset(other):
        other_y = other >> 1
        other_x = other - 2 * other_y
        return jnp.where(other_x == my_x, 0, 1) + jnp.where(other_y == my_y, 0, 2)

    def invert(here, key, value):
        key = jnp.where(jnp.logical_and(valid, here), key, -1)
        hit = jnp.where(lax.broadcasted_iota(i32, (128, width), 0) == key, 1.0, 0.0).astype(bf16)
        value = jnp.broadcast_to(value.astype(bf16), (16, width))
        return lax.dot_general(value, hit, (((1,), (1,)), ((), ())), preferred_element_type=f32)[:1]

    rank = rank.astype(i32)
    place = place.astype(i32)
    guest = guest.astype(i32)

    def based(hop):
        return hop * per_pair + jnp.where(hop > 0, 2 * extra, 0)

    landing = based(offset(source)) + rank
    mine = via == pair
    ours = home == pair
    return chosen, [
        invert(source == pair, based(offset(via)) + rank, (lane - group * pair).astype(f32)),
        invert(mine, row * tall + place, landing.astype(f32)),
        invert(jnp.logical_and(mine, home != pair), (way * rows + row) * extra + guest, place.astype(f32)),
        invert(ours, (side * rows + row) * cap + slot, jnp.where(mine, place, tall + way * extra + guest).astype(f32)),
        invert(mine, row, jnp.ones((1, width), f32)),
        invert(ours, side * rows + row, jnp.ones((1, width), f32)),
    ]


def prepare_balanced(dims, sizes, zone, slot, table, choice, padded):
    pair = lax.axis_index("gx") // 2
    padded[...] = jnp.full_like(padded, -1)
    padded[0:1, 0:zone.shape[1]] = zone[...]
    padded[1:2, 0:zone.shape[1]] = slot[...]

    def fill(sizes, allow):
        chosen, lines = plan_tables(dims, sizes, pair, padded[0:1], padded[1:2], allow)
        for k, line in enumerate(lines):
            table[k:k + 1] = line.astype(jnp.int32)
        return jnp.max(chosen)

    chosen = fill(sizes, 1)
    choice[0] = jnp.minimum(chosen, len(sizes) - 1)

    @pl.when(chosen == len(sizes))
    def _():
        fill(sizes[:0], 0)


def mirror_rows(block):
    side = block.shape[0]
    row = PART - 1 - lax.broadcasted_iota(jnp.int32, (PART, block.shape[1]), 0)
    parts = [block[r - PART:r] for r in range(side, 0, -PART)]
    return jnp.concatenate([jnp.take_along_axis(part, row, axis=0) for part in parts], axis=0)


def turn(block, code):
    block = jnp.where(jnp.logical_or(code == 1, code == 2), mirror_lanes(block), block)
    block = jnp.where(code >= 2, mirror_rows(block), block)
    return jnp.where(jnp.logical_or(code == 1, code == 3), block.T, block)


def exchange_balanced(dims, chunks, table, spins, field, regional, *scratch):
    pairs, rows, per_group, per_pair, cap, extra, wide, end, far = dims
    tall = 2 * cap
    count = len(chunks)
    times, _, side, _ = field.shape
    strips = side // (2 * PART)
    kinds = 12
    groups = [scratch[i * count:(i + 1) * count] for i in range(kinds)]
    held, swapped, packed, landed, lifted, risen, pooled, crossed_in, crossed_out, passed, leaving, visiting = groups
    crossed = (crossed_in, crossed_out)
    raw, given, far_list, *sems = scratch[kinds * count:]
    raw_sem, swap_send, swap_recv, pair_send, pair_recv, near_send, near_recv = sems[:7]
    give_send, give_recv, far_send, far_recv, pass_send, pass_recv, side_send, side_recv = sems[7:]
    unit_at = {unit: (c, i) for c, chunk in enumerate(chunks) for i, unit in enumerate(chunk)}
    gx = lax.axis_index("gx")
    z = lax.axis_index("gy")
    pair = gx // 2
    half = lax.rem(gx, 2)
    mate = (2 * pair + 1 - half, z)
    pair_x = lax.rem(pair, 2)
    pair_y = pair // 2
    near, far_in, far_out = (origin_of(z, rows, k, True) for k in (1, 2, 3))
    inner = jnp.logical_or(z == 1, z == 2)
    outer = jnp.logical_not(inner)

    def across(o):
        x = 1 - pair_x if o % 2 else pair_x
        y = 1 - pair_y if o // 2 else pair_y
        return (2 * (2 * y + x) + half, z)

    loads = []
    for t in range(times):
        loads.append(pltpu.make_async_copy(field.at[t], raw.at[pl.ds(t * per_group, per_group)], raw_sem.at[t]))
        loads[t].start()

    barrier = pltpu.get_barrier_semaphore()
    friends = [mate] + [across(o) for o in range(1, pairs)] + [(gx, lax.rem(z + o, rows)) for o in range(1, rows)]
    for friend in friends:
        pl.semaphore_signal(barrier, inc=1, device_id=friend, device_id_type=MESH)

    def turn_time(t):
        loads[t].wait()

        def one(b, carry):
            block = turn(raw[t * per_group + b], spins[gx * per_group + b])
            for r in range(strips):
                c, i = unit_at[r, t]
                top = block[r * PART:(r + 1) * PART]
                bottom = block[side // 2 + r * PART:side // 2 + (r + 1) * PART]
                held[c][half * per_group + b, i] = jnp.where(half == 0, top, bottom)
                swapped[c][b, i] = jnp.where(half == 0, bottom, top)
            return carry
        lax.fori_loop(0, per_group, one, 0, unroll=4)

    def wait_sent(sem, blocks):
        span = raw.at[pl.ds(0, blocks)]
        pltpu.make_async_copy(span, span, sem).wait()

    turn_time(0)
    pl.semaphore_wait(barrier, len(friends))

    swaps = {}

    def swap_time(t):
        for c in sorted({unit_at[r, t][0] for r in range(strips)}):
            swaps[c] = pltpu.make_async_remote_copy(
                src_ref=swapped[c], dst_ref=held[c].at[pl.ds(half * per_group, per_group)],
                send_sem=swap_send.at[0], recv_sem=swap_recv.at[c], device_id=mate, device_id_type=MESH)
            swaps[c].start()

    swap_time(0)

    def send_pairs(c):
        if c == 1:
            for t in range(1, times):
                turn_time(t)
                swap_time(t)
        swaps[c].wait_recv()
        sent = []
        for o in range(1, pairs):
            def pack(k, carry, o=o):
                packed[c][o - 1, k] = held[c][table[0, o * per_pair + 2 * extra + k]]
                return carry
            lax.fori_loop(0, wide, pack, 0, unroll=4)
            sent.append(pltpu.make_async_remote_copy(
                src_ref=packed[c].at[o - 1], dst_ref=landed[c].at[pl.ds(o * per_pair + 2 * extra, wide)],
                send_sem=pair_send.at[o - 1], recv_sem=pair_recv.at[c],
                device_id=across(o), device_id_type=MESH))

        @pl.when(half == 0)
        def _():
            for copy in sent:
                copy.start()

        @pl.when(half == 1)
        def _():
            for copy in sent[::-1]:
                copy.start()

        def stay(k, carry):
            landed[c][k] = held[c][table[0, k]]
            return carry
        lax.fori_loop(0, per_pair + 2 * extra, stay, 0, unroll=4)

        if c == 0:
            lead = table[4, far_in]

            def gather_far(k, carry):
                at = jnp.where(k < lead, far_in * tall + k, far_out * tall + k - lead)
                far_list[k] = table[1, jnp.minimum(at, rows * tall - 1)]
                return carry
            lax.fori_loop(0, far, gather_far, 0, unroll=4)

    skip = table[4, z]

    def near_copy(c, size):
        return pltpu.make_async_remote_copy(
            src_ref=lifted[c].at[pl.ds(0, size)], dst_ref=risen[c].at[1, pl.ds(0, size)],
            send_sem=near_send.at[0], recv_sem=near_recv.at[c],
            device_id=(gx, near), device_id_type=MESH)

    def far_copy(c, place):
        return pltpu.make_async_remote_copy(
            src_ref=pooled[c], dst_ref=crossed[place][c],
            send_sem=far_send.at[0], recv_sem=far_recv.at[c, place],
            device_id=(gx, far_in), device_id_type=MESH)

    def pass_copy(c, place):
        return pltpu.make_async_remote_copy(
            src_ref=passed[c].at[place], dst_ref=risen[c].at[2 + place, pl.ds(0, end)],
            send_sem=pass_send.at[0], recv_sem=pass_recv.at[c],
            device_id=(gx, near), device_id_type=MESH)

    def side_copy(c, d):
        return pltpu.make_async_remote_copy(
            src_ref=leaving[c].at[d], dst_ref=visiting[c].at[d],
            send_sem=side_send.at[0], recv_sem=side_recv.at[c],
            device_id=across(1 + d), device_id_type=MESH)

    def send_rows(c):
        pltpu.make_async_copy(packed[c], packed[c], pair_recv.at[c]).wait()

        def pool(k, carry):
            pooled[c][k] = landed[c][far_list[k]]
            return carry
        lax.fori_loop(0, far, pool, 0, unroll=4)

        def lift(k, carry):
            lifted[c][k] = landed[c][table[1, near * tall + k]]
            return carry
        lax.fori_loop(0, tall, lift, 0, unroll=4)

        def send_far():
            for place, mine in enumerate((inner, outer)):
                @pl.when(mine)
                def _(place=place):
                    far_copy(c, place).start()

        @pl.when(half == 0)
        def _():
            send_far()

        @pl.when(inner)
        def _():
            near_copy(c, end).start()

        @pl.when(outer)
        def _():
            near_copy(c, tall).start()

        @pl.when(half == 1)
        def _():
            send_far()

        def own(k, carry):
            risen[c][0, k] = landed[c][table[1, z * tall + k]]
            return carry
        lax.fori_loop(0, tall, own, 0, unroll=4)

    def hand_on(c, place):
        @pl.when(inner)
        def _():
            far_copy(c, place).wait_recv()

            def onward(k, carry):
                passed[c][place, k] = crossed[place][c][jnp.minimum(skip + k, far - 1)]
                return carry
            lax.fori_loop(0, end, onward, 0, unroll=4)
            pass_copy(c, place).start()

            def land(k, carry):
                risen[c][2 + place, k] = crossed[place][c][k]
                return carry
            lax.fori_loop(0, tall, land, 0, unroll=4)

    def hand_on_inner(c):
        hand_on(c, 0)

    def hand_on_outer(c):
        hand_on(c, 1)

    def send_sides(c):
        @pl.when(inner)
        def _():
            near_copy(c, tall).wait_recv()

        @pl.when(outer)
        def _():
            near_copy(c, end).wait_recv()
            pltpu.make_async_copy(passed[c], passed[c], pass_recv.at[c]).wait()

        for d in range(2):
            def leave(k, carry, d=d):
                at = table[2, (d * rows + z) * extra + k]
                for o in range(rows):
                    leaving[c][d, o, k] = risen[c][o, at]
                return carry
            lax.fori_loop(0, extra, leave, 0)
            side_copy(c, d).start()

    def settle(c):
        pltpu.make_async_copy(visiting[c], visiting[c], side_recv.at[c]).wait()
        for r, _ in chunks[c]:
            if max(unit_at[r, t][0] for t in range(times)) == c:
                settle_strip(r)

    def settle_strip(r):
        span = pl.ds(pl.multiple_of(half * (side // 2) + r * PART, PART), PART)

        def place(s, carry):
            for core in (1 - half, half):
                at = table[3, (core * rows + z) * cap + s]
                live = s < table[5, core * rows + z]
                guest = jnp.maximum(at - tall, 0)
                way = guest // extra
                tiles = {}
                for t in range(times):
                    c, i = unit_at[r, t]
                    for o in range(rows):
                        home = risen[c][o, jnp.minimum(at, tall - 1), i]
                        visitor = visiting[c][way, o, guest - way * extra, i]
                        tiles[o, t] = jnp.where(at < tall, home, visitor)
                mean = sum(tiles.values()) * jnp.float32(1.0 / (rows * times))
                for (o, t), tile in tiles.items():
                    value = jnp.where(live, tile - mean, 0.0)
                    if core is half:
                        regional[origin_of(z, rows, o, True) * times + t, 0, s, span, :] = value
                    else:
                        given[r, origin_of(z, rows, o, True) * times + t, s] = value
            return carry
        lax.fori_loop(0, cap, place, 0)
        give = pltpu.make_async_remote_copy(
            src_ref=given.at[r], dst_ref=regional.at[:, 0, :, span, :],
            send_sem=give_send.at[0], recv_sem=give_recv.at[0], device_id=mate, device_id_type=MESH)
        give.start()

    starts = []
    for chunk in chunks:
        begin = starts[-1][1] if starts else 0
        starts.append((begin, begin + len(chunk)))
    for _, _, c, act in timetable(starts, wide, tall, end, far, extra, (send_pairs, send_rows, hand_on_outer, hand_on_inner, send_sides, settle)):
        act(c)

    wait_sent(swap_send.at[0], per_group)
    for o in range(1, pairs):
        wait_sent(pair_send.at[o - 1], wide)
    wait_sent(far_send.at[0], far)
    wait_sent(side_send.at[0], 2 * rows * extra)

    @pl.when(inner)
    def _():
        wait_sent(near_send.at[0], end)
        wait_sent(pass_send.at[0], 2 * end)

    @pl.when(outer)
    def _():
        wait_sent(near_send.at[0], tall)

    wait_sent(give_send.at[0], rows * cap)
    wait_sent(give_recv.at[0], rows * cap)


def timetable(starts, wide, tall, end, far, extra, acts):
    hop = 60
    sent = soon = crossed = passed = 0.0
    busy = 4 * wide * starts[-1][1]
    events = []
    for c, (begin, close) in enumerate(starts):
        size = close - begin
        sent = sent + 4 * wide * size
        landed = sent + hop
        soon = max(soon, landed) + 1.95 * (tall + far) * size
        crossed = max(crossed, landed) + 4 * far * size
        passed = max(passed, crossed + hop) + 4 * end * size
        sides = passed + hop
        busy = max(busy, sides) + 8 * extra * size
        for k, at in enumerate((0.0, landed, soon + hop, crossed + hop, sides, busy + 2 * hop)):
            events.append((at, k, c, acts[k]))
    return sorted(events, key=lambda e: e[:3])


def on_device(field, zone, slot, spins, tally):
    times, per_group, side, _ = field.shape
    columns = lax.axis_size("gx")
    rows = lax.axis_size("gy")
    pairs = columns // 2
    cap = 2 * per_group // rows
    per_pair = 4 * (2 * per_group // columns)
    balanced = rows == 4 and pairs == 4 and times == 2 and columns * per_group < 256 and 2 * rows * cap <= 128 and pairs * per_pair + 2 * (cap // 3) <= 128
    if balanced:
        return balanced_exchange(field, zone, slot, spins, cap, per_pair)
    chunks = chunk_units(times, side)
    tiles = [(len(chunk), PART, side) for chunk in chunks]
    final = plain_exchange(field, zone, slot, spins, chunks, tiles, cap, per_pair)
    return pl.pallas_call(
        functools.partial(finish, rows, chunks),
        grid_spec=pltpu.PrefetchScalarGridSpec(
            num_scalar_prefetch=1,
            grid=(cap,),
            in_specs=[pl.BlockSpec(
                (2, 1, rows) + tile,
                lambda s, count: (0, jnp.maximum(jnp.minimum(s, count[0] - 1), 0), 0, 0, 0, 0)) for tile in tiles],
            out_specs=pl.BlockSpec((rows * times, 1, 1, side, side), lambda s, count: (0, 0, s, 0, 0)),
        ),
        out_shape=jax.ShapeDtypeStruct((rows * times, 1, cap, side, side), jnp.float32),
        name="finish",
    )(tally, *final)


def scratch_of(tiles, *shapes):
    return [pltpu.VMEM(lead + tile, jnp.float32) for lead in shapes for tile in tiles]


def balanced_exchange(field, zone, slot, spins, cap, per_pair):
    times, per_group, side, _ = field.shape
    columns = lax.axis_size("gx")
    rows = lax.axis_size("gy")
    pairs = columns // 2
    tall = 2 * cap
    extra = cap // 3
    chunks = time_major(times, side)
    tiles = [(len(chunk), PART, side) for chunk in chunks]
    count = len(chunks)
    strips = side // (2 * PART)
    smem = pl.BlockSpec(memory_space=pltpu.SMEM)
    vmem = pl.BlockSpec(memory_space=pltpu.VMEM)
    sizes = balanced_sizes(per_pair, tall)
    lanes = -(-columns * per_group // 128) * 128
    table, choice = pl.pallas_call(
        functools.partial(prepare_balanced, (pairs, rows, per_group, per_pair, cap, extra), sizes),
        in_specs=[vmem, vmem],
        out_specs=[vmem, smem],
        out_shape=[jax.ShapeDtypeStruct((8, 128), jnp.int32), jax.ShapeDtypeStruct((1,), jnp.int32)],
        scratch_shapes=[pltpu.VMEM((8, lanes), jnp.int32)],
        name="prepare",
    )(zone.reshape(1, -1), slot.reshape(1, -1))

    def moved(wide, end, far, tag):
        dma = pltpu.SemaphoreType.DMA
        buffers = [
            *scratch_of(
                tiles, (2 * per_group,), (per_group,), (pairs - 1, wide), (pairs * per_pair + 2 * extra,), (tall,), (rows, tall),
                (far,), (far,), (far,), (2, end), (2, rows, extra), (2, rows, extra)),
            pltpu.VMEM((max(times * per_group, rows * cap, 2 * end, far), side, side), jnp.float32),
            pltpu.VMEM((strips, rows * times, cap, PART, side), jnp.float32),
            pltpu.SMEM((far,), jnp.int32),
            dma((times,)), dma((1,)), dma((count,)), dma((pairs - 1,)), dma((count,)), dma((1,)), dma((count,)),
            dma((1,)), dma((1,)), dma((1,)), dma((count, 2)), dma((1,)), dma((count,)), dma((1,)), dma((count,)),
        ]
        return lambda: pl.pallas_call(
            functools.partial(
                exchange_balanced, (pairs, rows, per_group, per_pair, cap, extra, wide, end, far), chunks),
            in_specs=[smem, smem, pl.BlockSpec(memory_space=pl.ANY)],
            out_specs=vmem,
            out_shape=pltpu.VMEM((rows * times, 1, cap, side, side), jnp.float32),
            scratch_shapes=buffers,
            compiler_params=pltpu.CompilerParams(collective_id=tag, has_side_effects=True, vmem_limit_bytes=VMEM_BYTES),
            name=f"exchange_{tag}",
        )(table, spins, field)

    return lax.switch(choice[0], [moved(*size, tag) for tag, size in enumerate(sizes)])


def plain_exchange(field, zone, slot, spins, chunks, tiles, cap, per_pair):
    times, per_group, side, _ = field.shape
    columns = lax.axis_size("gx")
    rows = lax.axis_size("gy")
    pairs = columns // 2
    per_row = 2 * cap
    smem = pl.BlockSpec(memory_space=pltpu.SMEM)
    anywhere = pl.BlockSpec(memory_space=pl.ANY)
    i32 = jnp.int32
    narrow = levels(per_pair, (40,))[0]
    sizes = [(narrow, tall) for tall in levels(per_row, (36, 42))]
    sizes.append((per_pair, per_row))
    *turned, send_table, pick_table, tallies, choice = pl.pallas_call(
        functools.partial(prepare, (pairs, rows, per_group, per_pair, cap, chunks, sizes)),
        grid=(per_group // STEP_BLOCKS,),
        in_specs=[smem, smem, smem, pl.BlockSpec((times, STEP_BLOCKS, side, side), lambda i: (0, i, 0, 0))],
        out_specs=[
            *[pl.BlockSpec((2, STEP_BLOCKS) + tile, lambda i: (0, i, 0, 0, 0)) for tile in tiles],
            smem, smem, smem, smem,
        ],
        out_shape=[
            *[jax.ShapeDtypeStruct((2, per_group) + tile, jnp.float32) for tile in tiles],
            jax.ShapeDtypeStruct((pairs * per_pair + 1,), i32),
            jax.ShapeDtypeStruct((per_row * rows + 1,), i32),
            jax.ShapeDtypeStruct((2 * rows,), i32),
            jax.ShapeDtypeStruct((1,), i32),
        ],
        scratch_shapes=[pltpu.SMEM((columns * rows,), i32), pltpu.SMEM((pairs * pairs,), i32)],
        name="prepare",
    )(zone, slot, spins, field)
    count = len(chunks)

    def moved(wide, tall, tag):
        dma = pltpu.SemaphoreType.DMA
        buffers = [
            *scratch_of(
                tiles, (2 * per_group,), (pairs - 1, wide), (pairs * per_pair,), (rows - 1, tall), (rows, tall),
                (cap, rows), (cap, rows)),
            pltpu.SMEM((rows * tall,), i32),
            dma((count,)), dma((count,)), dma((count,)),
            dma((count, pairs - 1)), dma((count, pairs - 1)),
            dma((count, rows - 1)), dma((count, rows - 1)),
            dma((count,)), dma((count,)), dma((count,)),
        ]
        return lambda: pl.pallas_call(
            functools.partial(exchange, (pairs, rows, per_group, per_pair, wide, tall, cap, count)),
            in_specs=[smem, smem, smem] + [anywhere] * count,
            out_specs=[anywhere] * count,
            out_shape=[jax.ShapeDtypeStruct((2, cap, rows) + tile, jnp.float32) for tile in tiles],
            scratch_shapes=buffers,
            compiler_params=pltpu.CompilerParams(collective_id=tag, has_side_effects=True, vmem_limit_bytes=60 * 2**20),
            name=f"exchange_{tag}",
        )(send_table, pick_table, tallies, *turned)

    return lax.switch(choice[0], [moved(*size, tag) for tag, size in enumerate(sizes)])


def solution(mesh):
    placed = (P("gy", "gx", None, None), P(), P(), P(), P(("gx", "gy")))
    return jax.shard_map(
        on_device,
        mesh=mesh,
        in_specs=placed,
        out_specs=P(None, ("gx", "gy"), None, None, None),
        check_vma=False,
    )
```

```python
import functools

import jax
import jax.numpy as jnp
from jax import lax
from jax.experimental import pallas as pl
from jax.experimental.pallas import tpu as pltpu
from jax.sharding import PartitionSpec as P

MESH = pl.DeviceIdType.MESH
PART = 8
STEP_BLOCKS = 4
VMEM_BYTES = 52 * 2**20


def chunk_units(times, side):
    units = [(r, t) for r in range(side // (2 * PART)) for t in range(times)]
    small = 2 * (times // 2 + times % 2)
    cuts = list(range(0, small + 1, max(times // 2, 1)))
    cuts += list(range(small + times, len(units) - small + 1, times))
    cuts += list(range(len(units) - small + max(times // 2, 1), len(units) + 1, max(times // 2, 1)))
    return [units[a:b] for a, b in zip(cuts[:-1], cuts[1:])]


def time_major(times, side):
    units = [(r, t) for t in range(times) for r in range(side // (2 * PART))]
    sizes = [1, 1] + [2] * ((len(units) - 4) // 2) + [1, 1]
    cuts = [sum(sizes[:c]) for c in range(len(sizes) + 1)]
    return [units[a:b] for a, b in zip(cuts[:-1], cuts[1:])]


def mirror_lanes(block):
    side = block.shape[1]
    lane = side - 1 - lax.broadcasted_iota(jnp.int32, block.shape, 1)
    return jnp.take_along_axis(block, lane, axis=1)


def turn_blocks(first, chunks, spins, field, turned):
    times, blocks, side, _ = field.shape
    for b in range(blocks):
        code = spins[first + b]
        for kind in range(4):
            @pl.when(code == kind)
            def _(kind=kind, b=b):
                for t in range(times):
                    block = field[t, b]
                    if kind == 1:
                        block = mirror_lanes(block).T
                    elif kind == 2:
                        block = mirror_lanes(mirror_lanes(block).T).T
                    elif kind == 3:
                        block = mirror_lanes(block.T)
                    for c, chunk in enumerate(chunks):
                        for i, (r, at) in enumerate(chunk):
                            if at == t:
                                for h in range(2):
                                    top = h * (side // 2) + r * PART
                                    turned[c][h, b, i] = block[top:top + PART]


def prepare(dims, zone, slot, spins, field, *refs):
    pairs, rows, per_group, per_pair, cap, chunks, sizes = dims
    turned = refs[:len(chunks)]
    send_table, pick_table, tallies, choice, counts, fills = refs[len(chunks):]
    gx = lax.axis_index("gx")
    pair = gx // 2
    group = 2 * per_group
    local = 2 * rows
    step = pl.program_id(0)

    @pl.when(step == 0)
    def _():
        def clear(ref, size):
            def body(i, c):
                ref[i] = 0
                return c
            lax.fori_loop(0, size, body, 0, unroll=8)
        clear(send_table, pairs * per_pair + 1)
        clear(pick_table, local * cap + 1)
        clear(counts, pairs * local)
        clear(fills, pairs * pairs)

        for source in range(pairs):
            behind = lax.rem(pair - source + pairs, pairs) * per_pair

            def place(j, c, source=source, behind=behind):
                region = zone[source * group + j]
                counts[region] = counts[region] + 1
                target = region // local
                cell = source * pairs + target
                rank = fills[cell]
                fills[cell] = rank + 1
                ahead = lax.rem(target - source + pairs, pairs) * per_pair
                send_table[jnp.where(source == pair, ahead + rank, pairs * per_pair)] = j
                at = (region - target * local) * cap + slot[source * group + j]
                pick_table[jnp.where(target == pair, at, local * cap)] = behind + rank
                return c
            lax.fori_loop(0, group, place, 0, unroll=4)
        most_pair = jnp.int32(0)
        most_row = jnp.int32(0)
        for q in range(pairs):
            for r in range(pairs):
                if q != r:
                    most_pair = jnp.maximum(most_pair, fills[q * pairs + r])
            pooled = [counts[q * local + r] + counts[q * local + rows + r] for r in range(rows)]
            for value in pooled:
                most_row = jnp.maximum(most_row, value)
        for r in range(local):
            tallies[r] = counts[pair * local + r]
        chosen = jnp.int32(len(sizes) - 1)
        for at in range(len(sizes) - 2, -1, -1):
            wide, tall = sizes[at]
            fits = jnp.logical_and(most_pair <= wide, most_row <= tall)
            chosen = jnp.where(fits, at, chosen)
        choice[0] = chosen

    turn_blocks(gx * per_group + step * field.shape[1], chunks, spins, field, turned)


def origin_of(z, rows, k, relay):
    if not relay:
        return lax.rem(z - k + rows, rows)
    low = z < 2
    return [z, z + 1 - 2 * lax.rem(z, 2), jnp.where(low, 2, 1), jnp.where(low, 3, 0)][k]


def exchange(dims, send_table, pick_table, tallies, *refs):
    pairs, rows, per_group, per_pair, wide, tall, cap, chunks = dims
    turned, final, scratch = refs[:chunks], refs[chunks:2 * chunks], refs[2 * chunks:]
    kinds = 7
    groups = [scratch[i * chunks:(i + 1) * chunks] for i in range(kinds)]
    held, packed, landed, lifted, risen, given, kept = groups
    sems = list(scratch[kinds * chunks:])
    row_list = sems.pop(0)
    own_sem, swap_send, swap_recv, pair_send, pair_recv, row_send, row_recv, give_send, give_recv, keep_sem = sems
    gx = lax.axis_index("gx")
    z = lax.axis_index("gy")
    pair = gx // 2
    half = lax.rem(gx, 2)
    mate = (2 * pair + 1 - half, z)

    def across(o):
        return (2 * lax.rem(pair + o, pairs) + half, z)

    def along(o):
        return (gx, lax.rem(z + o, rows))

    barrier = pltpu.get_barrier_semaphore()
    friends = [mate] + [across(o) for o in range(1, pairs)] + [along(o) for o in range(1, rows)]
    for friend in friends:
        pl.semaphore_signal(barrier, inc=1, device_id=friend, device_id_type=MESH)
    own_copies = []
    for c in range(chunks):
        own = pltpu.make_async_copy(turned[c].at[half], held[c].at[pl.ds(half * per_group, per_group)], own_sem.at[c])
        own.start()
        own_copies.append(own)
    pl.semaphore_wait(barrier, len(friends))

    swaps = []
    for c in range(chunks):
        swap = pltpu.make_async_remote_copy(
            src_ref=turned[c].at[1 - half], dst_ref=held[c].at[pl.ds(half * per_group, per_group)],
            send_sem=swap_send.at[c], recv_sem=swap_recv.at[c], device_id=mate, device_id_type=MESH)
        swap.start()
        swaps.append(swap)

    unsent = []
    pair_copies = []
    for c in range(chunks):
        own_copies[c].wait()
        swaps[c].wait_recv()
        unsent.append(swaps[c])
        sent = []
        for o in range(1, pairs):
            def pack(k, carry, o=o, c=c):
                packed[c][o - 1, k] = held[c][send_table[o * per_pair + k]]
                return carry
            lax.fori_loop(0, wide, pack, 0, unroll=4)
            copy = pltpu.make_async_remote_copy(
                src_ref=packed[c].at[o - 1], dst_ref=landed[c].at[pl.ds(o * per_pair, wide)],
                send_sem=pair_send.at[c, o - 1], recv_sem=pair_recv.at[c, o - 1],
                device_id=across(o), device_id_type=MESH)
            copy.start()
            sent.append(copy)
        unsent.extend(sent)

        def stay(k, carry, c=c):
            landed[c][k] = held[c][send_table[k]]
            return carry
        lax.fori_loop(0, per_pair, stay, 0, unroll=4)
        pair_copies.append(sent)

    for r in range(rows):
        first = tallies[r]

        def compact(k, carry, r=r, first=first):
            at = jnp.minimum(jnp.where(k < first, r * cap + k, (rows + r) * cap + k - first), 2 * rows * cap - 1)
            row_list[r * tall + k] = pick_table[at]
            return carry
        lax.fori_loop(0, tall, compact, 0, unroll=4)

    gives = []

    def settle_all(c):
        first = tallies[z]

        def settle(s, carry, c=c):
            mine = jnp.minimum(s + half * first, tall - 1)
            other = jnp.minimum(s + (1 - half) * first, tall - 1)
            for o in range(rows):
                given[c][s, o] = risen[c][o, other]
                kept[c][s, o] = risen[c][o, mine]
            return carry
        lax.fori_loop(0, cap, settle, 0)
        give = pltpu.make_async_remote_copy(
            src_ref=given[c], dst_ref=final[c].at[half],
            send_sem=give_send.at[c], recv_sem=give_recv.at[c], device_id=mate, device_id_type=MESH)
        give.start()
        keep = pltpu.make_async_copy(kept[c], final[c].at[half], keep_sem.at[c])
        keep.start()
        gives.append((give, keep))

    row_copies = []
    for c in range(chunks):
        for copy in pair_copies[c]:
            copy.wait_recv()
        sent = []
        for o in list(range(rows - 1, 0, -1)) + [0]:
            row = lax.rem(z + o, rows)

            def lift(k, carry, o=o, c=c, row=row):
                tile = landed[c][row_list[row * tall + k]]
                if o > 0:
                    lifted[c][o - 1, k] = tile
                else:
                    risen[c][0, k] = tile
                return carry
            lax.fori_loop(0, tall, lift, 0, unroll=4)
            if o > 0:
                copy = pltpu.make_async_remote_copy(
                    src_ref=lifted[c].at[o - 1], dst_ref=risen[c].at[o],
                    send_sem=row_send.at[c, o - 1], recv_sem=row_recv.at[c, o - 1],
                    device_id=along(o), device_id_type=MESH)
                copy.start()
                sent.append(copy)
        row_copies.append(sent)
        unsent.extend(sent)
    for c in range(chunks):
        for copy in row_copies[c]:
            copy.wait_recv()
        settle_all(c)
    for copy in unsent:
        copy.wait_send()
    for give, keep in gives:
        give.wait()
        keep.wait()


def finish(rows, chunks, tally, *refs):
    final, regional = refs[:-1], refs[-1]
    z = lax.axis_index("gy")
    slot = pl.program_id(0)
    side = regional.shape[3]
    times = regional.shape[0] // rows
    place = {unit: (c, i) for c, chunk in enumerate(chunks) for i, unit in enumerate(chunk)}

    @pl.when(slot < tally[0])
    def _():
        for h in range(2):
            for r in range(side // (2 * PART)):
                span = pl.ds(h * (side // 2) + r * PART, PART)
                tiles = {}
                for t in range(times):
                    c, i = place[(r, t)]
                    for o in range(rows):
                        tiles[o, t] = final[c][h, 0, o, i]
                mean = sum(tiles.values()) * jnp.float32(1.0 / (rows * times))
                for o in range(rows):
                    start = origin_of(z, rows, o, False) * times
                    for t in range(times):
                        regional[start + t, 0, 0, span, :] = tiles[o, t] - mean

    @pl.when(slot >= tally[0])
    def _():
        regional[...] = jnp.zeros_like(regional)


def levels(most, steps):
    return sorted({-(-most * s // 48) for s in steps})


def balanced_sizes(per_pair, tall):
    steps = (
        (36, 34, 50), (36, 34, 52), (36, 36, 54), (38, 38, 56), (40, 38, 58), (40, 40, 60), (44, 44, 64), (48, 48, 70),
        (48, 48, 96))
    return [(-(-per_pair * w // 48), -(-tall * e // 48), -(-tall * f // 48)) for w, e, f in steps]

def beside(x, step):
    return jnp.concatenate([x[step:], x[:step]], axis=0)


def plan_tables(dims, sizes, pair, zone, slot, allow):
    pairs, rows, per_group, per_pair, cap, extra = dims
    group, local, tall = 2 * per_group, 2 * rows, 2 * cap
    bins = pairs * rows
    width = zone.shape[1]
    i32, f32, bf16 = jnp.int32, jnp.float32, jnp.bfloat16
    lane = lax.broadcasted_iota(i32, (1, width), 1)
    valid = zone >= 0
    source = sum((lane >= group * k).astype(i32) for k in range(1, pairs))
    home = sum((zone >= local * k).astype(i32) for k in range(1, pairs))
    inside = zone - home * local
    side = (inside >= rows).astype(i32)
    row = inside - side * rows
    bin_at = lax.broadcasted_iota(i32, (bins, width), 0)
    before = (lax.broadcasted_iota(i32, (width, width), 0) < lax.broadcasted_iota(i32, (width, width), 1)).astype(bf16)

    def marks(key):
        return jnp.where(bin_at == jnp.where(valid, key, -1), 1.0, 0.0).astype(f32)

    def tally(mark):
        return jnp.sum(mark, axis=1, keepdims=True)

    def look(mark, table):
        return jnp.sum(mark * table, axis=0, keepdims=True)

    def ranks(mark):
        return jnp.dot(mark.astype(bf16), before, preferred_element_type=f32)

    spot = lax.broadcasted_iota(i32, (bins, 128), 0)
    at_row = spot & (rows - 1)
    at_home = spot >> (rows.bit_length() - 1)
    edge = jnp.logical_or(at_row == 0, at_row == rows - 1)

    def flip(x, bit):
        step = 1 << bit
        if 2 * step == bins:
            return beside(x, step)
        return jnp.where((spot & step) == 0, beside(x, step), beside(x, bins - step))

    across_x = lambda x: flip(x, 2)
    across_y = lambda x: flip(x, 3)
    mark = marks(home * rows + row)
    home_x = home & 1
    home_y = home >> 1
    beside_x = home_y * 2 + 1 - home_x
    beside_y = (1 - home_y) * 2 + home_x
    kinds = [source == beside_x, jnp.logical_and(source != beside_x, source != beside_y), source == beside_y]
    split = [jnp.where(kind, mark, 0.0) for kind in kinds]
    split_ranks = ranks(jnp.concatenate(split, axis=0))
    counts = [tally(part) for part in split]
    order = sum(look(part, split_ranks[k * bins:(k + 1) * bins] + sum(counts[:k])) for k, part in enumerate(split))
    total = sum(counts)
    native = jnp.broadcast_to(total, (bins, 128)).astype(i32)

    def whole(x):
        x = x + across_x(x)
        return x + across_y(x)

    load = native
    half_sum = whole(native + flip(native, 0))
    goal = (jnp.maximum(half_sum, flip(half_sum, 1)) + pairs - 1) >> (pairs.bit_length() - 1)
    row_sum = (whole(native) + pairs - 1) >> (pairs.bit_length() - 1)
    end_goal = jnp.maximum(jnp.maximum(row_sum, flip(flip(row_sum, 0), 1)), (9 * goal) >> 4)
    used = [jnp.zeros_like(native), jnp.zeros_like(native)]
    for _ in range(3):
        for d, partner in enumerate((across_x, across_y)):
            for stage in range(3):
                now, want = (load, end_goal) if stage == 0 else (load + flip(load, 0), goal)
                here = jnp.logical_not(edge) if stage == 1 else edge
                move = jnp.minimum((now - partner(now) + stage % 2) >> 1, now - want)
                move = jnp.minimum(move, jnp.minimum(extra - used[d], native - used[0] - used[1]))
                move = jnp.where(here, jnp.maximum(move, 0), 0)
                used[d] = used[d] + move
                load = load + partner(move) - move
    first = look(mark, (used[0] * allow)[:, :1].astype(f32))
    second = look(mark, (used[1] * allow)[:, :1].astype(f32))
    leaves_x = order < first
    keeps = look(mark, total) - second
    leaves_y = order >= keeps
    way = leaves_y.astype(i32)
    guest = order - jnp.where(leaves_y, keeps, 0.0)
    via = jnp.where(leaves_x, beside_x, jnp.where(leaves_y, beside_y, home))

    flow = marks(source * pairs + via)
    line = marks(via * rows + row)
    both = ranks(jnp.concatenate([flow, line], axis=0))
    rank = look(flow, both[:bins])
    place = look(line, both[bins:])
    flows = jnp.broadcast_to(tally(flow), (bins, 128))
    lines = jnp.broadcast_to(tally(line), (bins, 128))
    halves = lines + flip(lines, 0)
    stays = at_home == at_row
    chosen = jnp.full((1, 128), len(sizes), i32)
    for at, (wide, end, far) in reversed(list(enumerate(sizes))):
        over = jnp.where(flows > jnp.where(stays, per_pair + 2 * extra, wide).astype(f32), 1.0, 0.0)
        over = jnp.maximum(over, jnp.where(lines > jnp.where(edge, end, tall).astype(f32), 1.0, 0.0))
        over = jnp.maximum(over, jnp.where(halves > jnp.float32(far), 1.0, 0.0))
        chosen = jnp.where(jnp.max(over, axis=0, keepdims=True) > 0.0, chosen, at)

    my_x, my_y = pair % 2, pair // 2

    def offset(other):
        other_y = other >> 1
        other_x = other - 2 * other_y
        return jnp.where(other_x == my_x, 0, 1) + jnp.where(other_y == my_y, 0, 2)

    def invert(here, key, value):
        key = jnp.where(jnp.logical_and(valid, here), key, -1)
        hit = jnp.where(lax.broadcasted_iota(i32, (128, width), 0) == key, 1.0, 0.0).astype(bf16)
        value = jnp.broadcast_to(value.astype(bf16), (16, width))
        return lax.dot_general(value, hit, (((1,), (1,)), ((), ())), preferred_element_type=f32)[:1]

    rank = rank.astype(i32)
    place = place.astype(i32)
    guest = guest.astype(i32)

    def based(hop):
        return hop * per_pair + jnp.where(hop > 0, 2 * extra, 0)

    landing = based(offset(source)) + rank
    mine = via == pair
    ours = home == pair
    return chosen, [
        invert(source == pair, based(offset(via)) + rank, (lane - group * pair).astype(f32)),
        invert(mine, row * tall + place, landing.astype(f32)),
        invert(jnp.logical_and(mine, home != pair), (way * rows + row) * extra + guest, place.astype(f32)),
        invert(ours, (side * rows + row) * cap + slot, jnp.where(mine, place, tall + way * extra + guest).astype(f32)),
        invert(mine, row, jnp.ones((1, width), f32)),
        invert(ours, side * rows + row, jnp.ones((1, width), f32)),
    ]


def prepare_balanced(dims, sizes, zone, slot, table, choice, padded):
    pair = lax.axis_index("gx") // 2
    padded[...] = jnp.full_like(padded, -1)
    padded[0:1, 0:zone.shape[1]] = zone[...]
    padded[1:2, 0:zone.shape[1]] = slot[...]

    def fill(sizes, allow):
        chosen, lines = plan_tables(dims, sizes, pair, padded[0:1], padded[1:2], allow)
        for k, line in enumerate(lines):
            table[k:k + 1] = line.astype(jnp.int32)
        return jnp.max(chosen)

    chosen = fill(sizes, 1)
    choice[0] = jnp.minimum(chosen, len(sizes) - 1)

    @pl.when(chosen == len(sizes))
    def _():
        fill(sizes[:0], 0)


def mirror_rows(block):
    side = block.shape[0]
    row = PART - 1 - lax.broadcasted_iota(jnp.int32, (PART, block.shape[1]), 0)
    parts = [block[r - PART:r] for r in range(side, 0, -PART)]
    return jnp.concatenate([jnp.take_along_axis(part, row, axis=0) for part in parts], axis=0)


def turn(block, code):
    block = jnp.where(jnp.logical_or(code == 1, code == 2), mirror_lanes(block), block)
    block = jnp.where(code >= 2, mirror_rows(block), block)
    return jnp.where(jnp.logical_or(code == 1, code == 3), block.T, block)


def exchange_balanced(dims, chunks, table_in, spins_in, field, regional, *scratch):
    pairs, rows, per_group, per_pair, cap, extra, wide, end, far = dims
    tall = 2 * cap
    count = len(chunks)
    times, _, side, _ = field.shape
    strips = side // (2 * PART)
    kinds = 12
    groups = [scratch[i * count:(i + 1) * count] for i in range(kinds)]
    held, swapped, packed, landed, lifted, risen, pooled, crossed_in, crossed_out, passed, leaving, visiting = groups
    crossed = (crossed_in, crossed_out)
    raw, given, table, spins, far_list, *sems = scratch[kinds * count:]
    table_sem, spins_sem, raw_sem, swap_send, swap_recv, pair_send, pair_recv, near_send, near_recv = sems[:9]
    give_send, give_recv, far_send, far_recv, pass_send, pass_recv, side_send, side_recv = sems[9:]
    unit_at = {unit: (c, i) for c, chunk in enumerate(chunks) for i, unit in enumerate(chunk)}
    gx = lax.axis_index("gx")
    z = lax.axis_index("gy")
    pair = gx // 2
    half = lax.rem(gx, 2)
    mate = (2 * pair + 1 - half, z)
    pair_x = lax.rem(pair, 2)
    pair_y = pair // 2
    near, far_in, far_out = (origin_of(z, rows, k, True) for k in (1, 2, 3))
    inner = jnp.logical_or(z == 1, z == 2)
    outer = jnp.logical_not(inner)

    def across(o):
        x = 1 - pair_x if o % 2 else pair_x
        y = 1 - pair_y if o // 2 else pair_y
        return (2 * (2 * y + x) + half, z)

    spins_load = pltpu.make_async_copy(spins_in, spins, spins_sem)
    spins_load.start()
    table_load = pltpu.make_async_copy(table_in, table, table_sem)
    loads = []
    for t in range(times):
        loads.append(pltpu.make_async_copy(field.at[t], raw.at[pl.ds(t * per_group, per_group)], raw_sem.at[t]))
        loads[t].start()
    table_load.start()

    barrier = pltpu.get_barrier_semaphore()
    friends = [mate] + [across(o) for o in range(1, pairs)] + [(gx, lax.rem(z + o, rows)) for o in range(1, rows)]
    for friend in friends:
        pl.semaphore_signal(barrier, inc=1, device_id=friend, device_id_type=MESH)

    def turn_time(t):
        loads[t].wait()

        def one(b, carry):
            block = turn(raw[t * per_group + b], spins[gx * per_group + b])
            for r in range(strips):
                c, i = unit_at[r, t]
                top = block[r * PART:(r + 1) * PART]
                bottom = block[side // 2 + r * PART:side // 2 + (r + 1) * PART]
                held[c][half * per_group + b, i] = jnp.where(half == 0, top, bottom)
                swapped[c][b, i] = jnp.where(half == 0, bottom, top)
            return carry
        lax.fori_loop(0, per_group, one, 0, unroll=4)

    def wait_sent(sem, blocks):
        span = raw.at[pl.ds(0, blocks)]
        pltpu.make_async_copy(span, span, sem).wait()

    spins_load.wait()
    turn_time(0)
    table_load.wait()
    pl.semaphore_wait(barrier, len(friends))

    swaps = {}

    def swap_time(t):
        for c in sorted({unit_at[r, t][0] for r in range(strips)}):
            swaps[c] = pltpu.make_async_remote_copy(
                src_ref=swapped[c], dst_ref=held[c].at[pl.ds(half * per_group, per_group)],
                send_sem=swap_send.at[0], recv_sem=swap_recv.at[c], device_id=mate, device_id_type=MESH)
            swaps[c].start()

    swap_time(0)

    def send_pairs(c):
        if c == 1:
            for t in range(1, times):
                turn_time(t)
                swap_time(t)
        swaps[c].wait_recv()
        sent = []
        for o in range(1, pairs):
            def pack(k, carry, o=o):
                packed[c][o - 1, k] = held[c][table[0, o * per_pair + 2 * extra + k]]
                return carry
            lax.fori_loop(0, wide, pack, 0, unroll=4)
            sent.append(pltpu.make_async_remote_copy(
                src_ref=packed[c].at[o - 1], dst_ref=landed[c].at[pl.ds(o * per_pair + 2 * extra, wide)],
                send_sem=pair_send.at[o - 1], recv_sem=pair_recv.at[c],
                device_id=across(o), device_id_type=MESH))

        @pl.when(half == 0)
        def _():
            for copy in sent:
                copy.start()

        @pl.when(half == 1)
        def _():
            for copy in sent[::-1]:
                copy.start()

        def stay(k, carry):
            landed[c][k] = held[c][table[0, k]]
            return carry
        lax.fori_loop(0, per_pair + 2 * extra, stay, 0, unroll=4)

        if c == 0:
            lead = table[4, far_in]

            def gather_far(k, carry):
                at = jnp.where(k < lead, far_in * tall + k, far_out * tall + k - lead)
                far_list[k] = table[1, jnp.minimum(at, rows * tall - 1)]
                return carry
            lax.fori_loop(0, far, gather_far, 0, unroll=4)

    skip = table[4, z]

    def near_copy(c, size):
        return pltpu.make_async_remote_copy(
            src_ref=lifted[c].at[pl.ds(0, size)], dst_ref=risen[c].at[1, pl.ds(0, size)],
            send_sem=near_send.at[0], recv_sem=near_recv.at[c],
            device_id=(gx, near), device_id_type=MESH)

    def far_copy(c, place):
        return pltpu.make_async_remote_copy(
            src_ref=pooled[c], dst_ref=crossed[place][c],
            send_sem=far_send.at[0], recv_sem=far_recv.at[c, place],
            device_id=(gx, far_in), device_id_type=MESH)

    def pass_copy(c, place):
        return pltpu.make_async_remote_copy(
            src_ref=passed[c].at[place], dst_ref=risen[c].at[2 + place, pl.ds(0, end)],
            send_sem=pass_send.at[0], recv_sem=pass_recv.at[c],
            device_id=(gx, near), device_id_type=MESH)

    def side_copy(c, d):
        return pltpu.make_async_remote_copy(
            src_ref=leaving[c].at[d], dst_ref=visiting[c].at[d],
            send_sem=side_send.at[0], recv_sem=side_recv.at[c],
            device_id=across(1 + d), device_id_type=MESH)

    def send_rows(c):
        pltpu.make_async_copy(packed[c], packed[c], pair_recv.at[c]).wait()

        def pool(k, carry):
            pooled[c][k] = landed[c][far_list[k]]
            return carry
        lax.fori_loop(0, far, pool, 0, unroll=4)

        def lift(k, carry):
            lifted[c][k] = landed[c][table[1, near * tall + k]]
            return carry
        lax.fori_loop(0, tall, lift, 0, unroll=4)

        def send_far():
            for place, mine in enumerate((inner, outer)):
                @pl.when(mine)
                def _(place=place):
                    far_copy(c, place).start()

        @pl.when(half == 0)
        def _():
            send_far()

        @pl.when(inner)
        def _():
            near_copy(c, end).start()

        @pl.when(outer)
        def _():
            near_copy(c, tall).start()

        @pl.when(half == 1)
        def _():
            send_far()

        def own(k, carry):
            risen[c][0, k] = landed[c][table[1, z * tall + k]]
            return carry
        lax.fori_loop(0, tall, own, 0, unroll=4)

    def hand_on(c, place):
        @pl.when(inner)
        def _():
            far_copy(c, place).wait_recv()

            def onward(k, carry):
                passed[c][place, k] = crossed[place][c][jnp.minimum(skip + k, far - 1)]
                return carry
            lax.fori_loop(0, end, onward, 0, unroll=4)
            pass_copy(c, place).start()

            def land(k, carry):
                risen[c][2 + place, k] = crossed[place][c][k]
                return carry
            lax.fori_loop(0, tall, land, 0, unroll=4)

    def hand_on_inner(c):
        hand_on(c, 0)

    def hand_on_outer(c):
        hand_on(c, 1)

    def send_sides(c):
        @pl.when(inner)
        def _():
            near_copy(c, tall).wait_recv()

        @pl.when(outer)
        def _():
            near_copy(c, end).wait_recv()
            pltpu.make_async_copy(passed[c], passed[c], pass_recv.at[c]).wait()

        for d in range(2):
            def leave(k, carry, d=d):
                at = table[2, (d * rows + z) * extra + k]
                for o in range(rows):
                    leaving[c][d, o, k] = risen[c][o, at]
                return carry
            lax.fori_loop(0, extra, leave, 0)
            side_copy(c, d).start()

    def settle(c):
        pltpu.make_async_copy(visiting[c], visiting[c], side_recv.at[c]).wait()
        for r, _ in chunks[c]:
            if max(unit_at[r, t][0] for t in range(times)) == c:
                settle_strip(r)

    def settle_strip(r):
        span = pl.ds(pl.multiple_of(half * (side // 2) + r * PART, PART), PART)

        def place(s, carry):
            for core in (1 - half, half):
                at = table[3, (core * rows + z) * cap + s]
                live = s < table[5, core * rows + z]
                guest = jnp.maximum(at - tall, 0)
                way = guest // extra
                tiles = {}
                for t in range(times):
                    c, i = unit_at[r, t]
                    for o in range(rows):
                        home = risen[c][o, jnp.minimum(at, tall - 1), i]
                        visitor = visiting[c][way, o, guest - way * extra, i]
                        tiles[o, t] = jnp.where(at < tall, home, visitor)
                mean = sum(tiles.values()) * jnp.float32(1.0 / (rows * times))
                for (o, t), tile in tiles.items():
                    value = jnp.where(live, tile - mean, 0.0)
                    if core is half:
                        regional[origin_of(z, rows, o, True) * times + t, 0, s, span, :] = value
                    else:
                        given[r, origin_of(z, rows, o, True) * times + t, s] = value
            return carry
        lax.fori_loop(0, cap, place, 0)
        give = pltpu.make_async_remote_copy(
            src_ref=given.at[r], dst_ref=regional.at[:, 0, :, span, :],
            send_sem=give_send.at[0], recv_sem=give_recv.at[0], device_id=mate, device_id_type=MESH)
        give.start()

    starts = []
    for chunk in chunks:
        begin = starts[-1][1] if starts else 0
        starts.append((begin, begin + len(chunk)))
    for _, _, c, act in timetable(starts, wide, tall, end, far, extra, (send_pairs, send_rows, hand_on_outer, hand_on_inner, send_sides, settle)):
        act(c)

    wait_sent(swap_send.at[0], per_group)
    for o in range(1, pairs):
        wait_sent(pair_send.at[o - 1], wide)
    wait_sent(far_send.at[0], far)
    wait_sent(side_send.at[0], 2 * rows * extra)

    @pl.when(inner)
    def _():
        wait_sent(near_send.at[0], end)
        wait_sent(pass_send.at[0], 2 * end)

    @pl.when(outer)
    def _():
        wait_sent(near_send.at[0], tall)

    wait_sent(give_send.at[0], rows * cap)
    wait_sent(give_recv.at[0], rows * cap)


def timetable(starts, wide, tall, end, far, extra, acts):
    hop = 60
    sent = soon = crossed = passed = 0.0
    busy = 4 * wide * starts[-1][1]
    events = []
    for c, (begin, close) in enumerate(starts):
        size = close - begin
        sent = sent + 4 * wide * size
        landed = sent + hop
        soon = max(soon, landed) + 1.95 * (tall + far) * size
        crossed = max(crossed, landed) + 4 * far * size
        passed = max(passed, crossed + hop) + 4 * end * size
        sides = passed + hop
        busy = max(busy, sides) + 8 * extra * size
        for k, at in enumerate((0.0, landed, soon + hop, crossed + hop, sides, busy + 2 * hop)):
            events.append((at, k, c, acts[k]))
    return sorted(events, key=lambda e: e[:3])


def on_device(field, zone, slot, spins, tally):
    times, per_group, side, _ = field.shape
    columns = lax.axis_size("gx")
    rows = lax.axis_size("gy")
    pairs = columns // 2
    cap = 2 * per_group // rows
    per_pair = 4 * (2 * per_group // columns)
    balanced = rows == 4 and pairs == 4 and times == 2 and columns * per_group < 256 and 2 * rows * cap <= 128 and pairs * per_pair + 2 * (cap // 3) <= 128
    if balanced:
        return balanced_exchange(field, zone, slot, spins, cap, per_pair)
    chunks = chunk_units(times, side)
    tiles = [(len(chunk), PART, side) for chunk in chunks]
    final = plain_exchange(field, zone, slot, spins, chunks, tiles, cap, per_pair)
    return pl.pallas_call(
        functools.partial(finish, rows, chunks),
        grid_spec=pltpu.PrefetchScalarGridSpec(
            num_scalar_prefetch=1,
            grid=(cap,),
            in_specs=[pl.BlockSpec(
                (2, 1, rows) + tile,
                lambda s, count: (0, jnp.maximum(jnp.minimum(s, count[0] - 1), 0), 0, 0, 0, 0)) for tile in tiles],
            out_specs=pl.BlockSpec((rows * times, 1, 1, side, side), lambda s, count: (0, 0, s, 0, 0)),
        ),
        out_shape=jax.ShapeDtypeStruct((rows * times, 1, cap, side, side), jnp.float32),
        name="finish",
    )(tally, *final)


def scratch_of(tiles, *shapes):
    return [pltpu.VMEM(lead + tile, jnp.float32) for lead in shapes for tile in tiles]


def balanced_exchange(field, zone, slot, spins, cap, per_pair):
    times, per_group, side, _ = field.shape
    columns = lax.axis_size("gx")
    rows = lax.axis_size("gy")
    pairs = columns // 2
    tall = 2 * cap
    extra = cap // 3
    chunks = time_major(times, side)
    tiles = [(len(chunk), PART, side) for chunk in chunks]
    count = len(chunks)
    strips = side // (2 * PART)
    smem = pl.BlockSpec(memory_space=pltpu.SMEM)
    vmem = pl.BlockSpec(memory_space=pltpu.VMEM)
    sizes = balanced_sizes(per_pair, tall)
    lanes = -(-columns * per_group // 128) * 128
    table, choice = pl.pallas_call(
        functools.partial(prepare_balanced, (pairs, rows, per_group, per_pair, cap, extra), sizes),
        in_specs=[vmem, vmem],
        out_specs=[vmem, smem],
        out_shape=[jax.ShapeDtypeStruct((8, 128), jnp.int32), jax.ShapeDtypeStruct((1,), jnp.int32)],
        scratch_shapes=[pltpu.VMEM((8, lanes), jnp.int32)],
        name="prepare",
    )(zone.reshape(1, -1), slot.reshape(1, -1))

    def moved(wide, end, far, tag):
        dma = pltpu.SemaphoreType.DMA
        buffers = [
            *scratch_of(
                tiles, (2 * per_group,), (per_group,), (pairs - 1, wide), (pairs * per_pair + 2 * extra,), (tall,), (rows, tall),
                (far,), (far,), (far,), (2, end), (2, rows, extra), (2, rows, extra)),
            pltpu.VMEM((max(times * per_group, rows * cap, 2 * end, far), side, side), jnp.float32),
            pltpu.VMEM((strips, rows * times, cap, PART, side), jnp.float32),
            pltpu.SMEM((8, 128), jnp.int32), pltpu.SMEM(spins.shape, jnp.int32), pltpu.SMEM((far,), jnp.int32),
            dma, dma, dma((times,)), dma((1,)), dma((count,)), dma((pairs - 1,)), dma((count,)), dma((1,)), dma((count,)),
            dma((1,)), dma((1,)), dma((1,)), dma((count, 2)), dma((1,)), dma((count,)), dma((1,)), dma((count,)),
        ]
        return lambda: pl.pallas_call(
            functools.partial(
                exchange_balanced, (pairs, rows, per_group, per_pair, cap, extra, wide, end, far), chunks),
            in_specs=[pl.BlockSpec(memory_space=pl.ANY)] * 3,
            out_specs=vmem,
            out_shape=pltpu.VMEM((rows * times, 1, cap, side, side), jnp.float32),
            scratch_shapes=buffers,
            compiler_params=pltpu.CompilerParams(collective_id=tag, has_side_effects=True, vmem_limit_bytes=VMEM_BYTES),
            name=f"exchange_{tag}",
        )(table, spins, field)

    return lax.switch(choice[0], [moved(*size, tag) for tag, size in enumerate(sizes)])


def plain_exchange(field, zone, slot, spins, chunks, tiles, cap, per_pair):
    times, per_group, side, _ = field.shape
    columns = lax.axis_size("gx")
    rows = lax.axis_size("gy")
    pairs = columns // 2
    per_row = 2 * cap
    smem = pl.BlockSpec(memory_space=pltpu.SMEM)
    anywhere = pl.BlockSpec(memory_space=pl.ANY)
    i32 = jnp.int32
    narrow = levels(per_pair, (40,))[0]
    sizes = [(narrow, tall) for tall in levels(per_row, (36, 42))]
    sizes.append((per_pair, per_row))
    *turned, send_table, pick_table, tallies, choice = pl.pallas_call(
        functools.partial(prepare, (pairs, rows, per_group, per_pair, cap, chunks, sizes)),
        grid=(per_group // STEP_BLOCKS,),
        in_specs=[smem, smem, smem, pl.BlockSpec((times, STEP_BLOCKS, side, side), lambda i: (0, i, 0, 0))],
        out_specs=[
            *[pl.BlockSpec((2, STEP_BLOCKS) + tile, lambda i: (0, i, 0, 0, 0)) for tile in tiles],
            smem, smem, smem, smem,
        ],
        out_shape=[
            *[jax.ShapeDtypeStruct((2, per_group) + tile, jnp.float32) for tile in tiles],
            jax.ShapeDtypeStruct((pairs * per_pair + 1,), i32),
            jax.ShapeDtypeStruct((per_row * rows + 1,), i32),
            jax.ShapeDtypeStruct((2 * rows,), i32),
            jax.ShapeDtypeStruct((1,), i32),
        ],
        scratch_shapes=[pltpu.SMEM((columns * rows,), i32), pltpu.SMEM((pairs * pairs,), i32)],
        name="prepare",
    )(zone, slot, spins, field)
    count = len(chunks)

    def moved(wide, tall, tag):
        dma = pltpu.SemaphoreType.DMA
        buffers = [
            *scratch_of(
                tiles, (2 * per_group,), (pairs - 1, wide), (pairs * per_pair,), (rows - 1, tall), (rows, tall),
                (cap, rows), (cap, rows)),
            pltpu.SMEM((rows * tall,), i32),
            dma((count,)), dma((count,)), dma((count,)),
            dma((count, pairs - 1)), dma((count, pairs - 1)),
            dma((count, rows - 1)), dma((count, rows - 1)),
            dma((count,)), dma((count,)), dma((count,)),
        ]
        return lambda: pl.pallas_call(
            functools.partial(exchange, (pairs, rows, per_group, per_pair, wide, tall, cap, count)),
            in_specs=[smem, smem, smem] + [anywhere] * count,
            out_specs=[anywhere] * count,
            out_shape=[jax.ShapeDtypeStruct((2, cap, rows) + tile, jnp.float32) for tile in tiles],
            scratch_shapes=buffers,
            compiler_params=pltpu.CompilerParams(collective_id=tag, has_side_effects=True, vmem_limit_bytes=60 * 2**20),
            name=f"exchange_{tag}",
        )(send_table, pick_table, tallies, *turned)

    return lax.switch(choice[0], [moved(*size, tag) for tag, size in enumerate(sizes)])


def solution(mesh):
    placed = (P("gy", "gx", None, None), P(), P(), P(), P(("gx", "gy")))
    return jax.shard_map(
        on_device,
        mesh=mesh,
        in_specs=placed,
        out_specs=P(None, ("gx", "gy"), None, None, None),
        check_vma=False,
    )
```

```python
import functools

import jax
import jax.numpy as jnp
from jax import lax
from jax.experimental import pallas as pl
from jax.experimental.pallas import tpu as pltpu
from jax.sharding import PartitionSpec as P

MESH = pl.DeviceIdType.MESH
PART = 8
STEP_BLOCKS = 4
VMEM_BYTES = 52 * 2**20


def chunk_units(times, side):
    units = [(r, t) for r in range(side // (2 * PART)) for t in range(times)]
    small = 2 * (times // 2 + times % 2)
    cuts = list(range(0, small + 1, max(times // 2, 1)))
    cuts += list(range(small + times, len(units) - small + 1, times))
    cuts += list(range(len(units) - small + max(times // 2, 1), len(units) + 1, max(times // 2, 1)))
    return [units[a:b] for a, b in zip(cuts[:-1], cuts[1:])]


def time_major(times, side):
    units = [(r, t) for t in range(times) for r in range(side // (2 * PART))]
    sizes = [1, 1] + [2] * ((len(units) - 4) // 2) + [1, 1]
    cuts = [sum(sizes[:c]) for c in range(len(sizes) + 1)]
    return [units[a:b] for a, b in zip(cuts[:-1], cuts[1:])]


def mirror_lanes(block):
    side = block.shape[1]
    lane = side - 1 - lax.broadcasted_iota(jnp.int32, block.shape, 1)
    return jnp.take_along_axis(block, lane, axis=1)


def turn_blocks(first, chunks, spins, field, turned):
    times, blocks, side, _ = field.shape
    for b in range(blocks):
        code = spins[first + b]
        for kind in range(4):
            @pl.when(code == kind)
            def _(kind=kind, b=b):
                for t in range(times):
                    block = field[t, b]
                    if kind == 1:
                        block = mirror_lanes(block).T
                    elif kind == 2:
                        block = mirror_lanes(mirror_lanes(block).T).T
                    elif kind == 3:
                        block = mirror_lanes(block.T)
                    for c, chunk in enumerate(chunks):
                        for i, (r, at) in enumerate(chunk):
                            if at == t:
                                for h in range(2):
                                    top = h * (side // 2) + r * PART
                                    turned[c][h, b, i] = block[top:top + PART]


def prepare(dims, zone, slot, spins, field, *refs):
    pairs, rows, per_group, per_pair, cap, chunks, sizes = dims
    turned = refs[:len(chunks)]
    send_table, pick_table, tallies, choice, counts, fills = refs[len(chunks):]
    gx = lax.axis_index("gx")
    pair = gx // 2
    group = 2 * per_group
    local = 2 * rows
    step = pl.program_id(0)

    @pl.when(step == 0)
    def _():
        def clear(ref, size):
            def body(i, c):
                ref[i] = 0
                return c
            lax.fori_loop(0, size, body, 0, unroll=8)
        clear(send_table, pairs * per_pair + 1)
        clear(pick_table, local * cap + 1)
        clear(counts, pairs * local)
        clear(fills, pairs * pairs)

        for source in range(pairs):
            behind = lax.rem(pair - source + pairs, pairs) * per_pair

            def place(j, c, source=source, behind=behind):
                region = zone[source * group + j]
                counts[region] = counts[region] + 1
                target = region // local
                cell = source * pairs + target
                rank = fills[cell]
                fills[cell] = rank + 1
                ahead = lax.rem(target - source + pairs, pairs) * per_pair
                send_table[jnp.where(source == pair, ahead + rank, pairs * per_pair)] = j
                at = (region - target * local) * cap + slot[source * group + j]
                pick_table[jnp.where(target == pair, at, local * cap)] = behind + rank
                return c
            lax.fori_loop(0, group, place, 0, unroll=4)
        most_pair = jnp.int32(0)
        most_row = jnp.int32(0)
        for q in range(pairs):
            for r in range(pairs):
                if q != r:
                    most_pair = jnp.maximum(most_pair, fills[q * pairs + r])
            pooled = [counts[q * local + r] + counts[q * local + rows + r] for r in range(rows)]
            for value in pooled:
                most_row = jnp.maximum(most_row, value)
        for r in range(local):
            tallies[r] = counts[pair * local + r]
        chosen = jnp.int32(len(sizes) - 1)
        for at in range(len(sizes) - 2, -1, -1):
            wide, tall = sizes[at]
            fits = jnp.logical_and(most_pair <= wide, most_row <= tall)
            chosen = jnp.where(fits, at, chosen)
        choice[0] = chosen

    turn_blocks(gx * per_group + step * field.shape[1], chunks, spins, field, turned)


def origin_of(z, rows, k, relay):
    if not relay:
        return lax.rem(z - k + rows, rows)
    low = z < 2
    return [z, z + 1 - 2 * lax.rem(z, 2), jnp.where(low, 2, 1), jnp.where(low, 3, 0)][k]


def exchange(dims, send_table, pick_table, tallies, *refs):
    pairs, rows, per_group, per_pair, wide, tall, cap, chunks = dims
    turned, final, scratch = refs[:chunks], refs[chunks:2 * chunks], refs[2 * chunks:]
    kinds = 7
    groups = [scratch[i * chunks:(i + 1) * chunks] for i in range(kinds)]
    held, packed, landed, lifted, risen, given, kept = groups
    sems = list(scratch[kinds * chunks:])
    row_list = sems.pop(0)
    own_sem, swap_send, swap_recv, pair_send, pair_recv, row_send, row_recv, give_send, give_recv, keep_sem = sems
    gx = lax.axis_index("gx")
    z = lax.axis_index("gy")
    pair = gx // 2
    half = lax.rem(gx, 2)
    mate = (2 * pair + 1 - half, z)

    def across(o):
        return (2 * lax.rem(pair + o, pairs) + half, z)

    def along(o):
        return (gx, lax.rem(z + o, rows))

    barrier = pltpu.get_barrier_semaphore()
    friends = [mate] + [across(o) for o in range(1, pairs)] + [along(o) for o in range(1, rows)]
    for friend in friends:
        pl.semaphore_signal(barrier, inc=1, device_id=friend, device_id_type=MESH)
    own_copies = []
    for c in range(chunks):
        own = pltpu.make_async_copy(turned[c].at[half], held[c].at[pl.ds(half * per_group, per_group)], own_sem.at[c])
        own.start()
        own_copies.append(own)
    pl.semaphore_wait(barrier, len(friends))

    swaps = []
    for c in range(chunks):
        swap = pltpu.make_async_remote_copy(
            src_ref=turned[c].at[1 - half], dst_ref=held[c].at[pl.ds(half * per_group, per_group)],
            send_sem=swap_send.at[c], recv_sem=swap_recv.at[c], device_id=mate, device_id_type=MESH)
        swap.start()
        swaps.append(swap)

    unsent = []
    pair_copies = []
    for c in range(chunks):
        own_copies[c].wait()
        swaps[c].wait_recv()
        unsent.append(swaps[c])
        sent = []
        for o in range(1, pairs):
            def pack(k, carry, o=o, c=c):
                packed[c][o - 1, k] = held[c][send_table[o * per_pair + k]]
                return carry
            lax.fori_loop(0, wide, pack, 0, unroll=4)
            copy = pltpu.make_async_remote_copy(
                src_ref=packed[c].at[o - 1], dst_ref=landed[c].at[pl.ds(o * per_pair, wide)],
                send_sem=pair_send.at[c, o - 1], recv_sem=pair_recv.at[c, o - 1],
                device_id=across(o), device_id_type=MESH)
            copy.start()
            sent.append(copy)
        unsent.extend(sent)

        def stay(k, carry, c=c):
            landed[c][k] = held[c][send_table[k]]
            return carry
        lax.fori_loop(0, per_pair, stay, 0, unroll=4)
        pair_copies.append(sent)

    for r in range(rows):
        first = tallies[r]

        def compact(k, carry, r=r, first=first):
            at = jnp.minimum(jnp.where(k < first, r * cap + k, (rows + r) * cap + k - first), 2 * rows * cap - 1)
            row_list[r * tall + k] = pick_table[at]
            return carry
        lax.fori_loop(0, tall, compact, 0, unroll=4)

    gives = []

    def settle_all(c):
        first = tallies[z]

        def settle(s, carry, c=c):
            mine = jnp.minimum(s + half * first, tall - 1)
            other = jnp.minimum(s + (1 - half) * first, tall - 1)
            for o in range(rows):
                given[c][s, o] = risen[c][o, other]
                kept[c][s, o] = risen[c][o, mine]
            return carry
        lax.fori_loop(0, cap, settle, 0)
        give = pltpu.make_async_remote_copy(
            src_ref=given[c], dst_ref=final[c].at[half],
            send_sem=give_send.at[c], recv_sem=give_recv.at[c], device_id=mate, device_id_type=MESH)
        give.start()
        keep = pltpu.make_async_copy(kept[c], final[c].at[half], keep_sem.at[c])
        keep.start()
        gives.append((give, keep))

    row_copies = []
    for c in range(chunks):
        for copy in pair_copies[c]:
            copy.wait_recv()
        sent = []
        for o in list(range(rows - 1, 0, -1)) + [0]:
            row = lax.rem(z + o, rows)

            def lift(k, carry, o=o, c=c, row=row):
                tile = landed[c][row_list[row * tall + k]]
                if o > 0:
                    lifted[c][o - 1, k] = tile
                else:
                    risen[c][0, k] = tile
                return carry
            lax.fori_loop(0, tall, lift, 0, unroll=4)
            if o > 0:
                copy = pltpu.make_async_remote_copy(
                    src_ref=lifted[c].at[o - 1], dst_ref=risen[c].at[o],
                    send_sem=row_send.at[c, o - 1], recv_sem=row_recv.at[c, o - 1],
                    device_id=along(o), device_id_type=MESH)
                copy.start()
                sent.append(copy)
        row_copies.append(sent)
        unsent.extend(sent)
    for c in range(chunks):
        for copy in row_copies[c]:
            copy.wait_recv()
        settle_all(c)
    for copy in unsent:
        copy.wait_send()
    for give, keep in gives:
        give.wait()
        keep.wait()


def finish(rows, chunks, tally, *refs):
    final, regional = refs[:-1], refs[-1]
    z = lax.axis_index("gy")
    slot = pl.program_id(0)
    side = regional.shape[3]
    times = regional.shape[0] // rows
    place = {unit: (c, i) for c, chunk in enumerate(chunks) for i, unit in enumerate(chunk)}

    @pl.when(slot < tally[0])
    def _():
        for h in range(2):
            for r in range(side // (2 * PART)):
                span = pl.ds(h * (side // 2) + r * PART, PART)
                tiles = {}
                for t in range(times):
                    c, i = place[(r, t)]
                    for o in range(rows):
                        tiles[o, t] = final[c][h, 0, o, i]
                mean = sum(tiles.values()) * jnp.float32(1.0 / (rows * times))
                for o in range(rows):
                    start = origin_of(z, rows, o, False) * times
                    for t in range(times):
                        regional[start + t, 0, 0, span, :] = tiles[o, t] - mean

    @pl.when(slot >= tally[0])
    def _():
        regional[...] = jnp.zeros_like(regional)


def levels(most, steps):
    return sorted({-(-most * s // 48) for s in steps})


def balanced_sizes(per_pair, tall):
    steps = (
        (36, 34, 50), (36, 34, 52), (36, 36, 54), (38, 38, 56), (40, 38, 58), (40, 40, 60), (44, 44, 64), (48, 48, 70),
        (48, 48, 96))
    return [(-(-per_pair * w // 48), -(-tall * e // 48), -(-tall * f // 48)) for w, e, f in steps]

def beside(x, step):
    return jnp.concatenate([x[step:], x[:step]], axis=0)


def plan_tables(dims, sizes, pair, zone, slot, allow):
    pairs, rows, per_group, per_pair, cap, extra = dims
    group, local, tall = 2 * per_group, 2 * rows, 2 * cap
    bins = pairs * rows
    width = zone.shape[1]
    i32, f32, bf16 = jnp.int32, jnp.float32, jnp.bfloat16
    lane = lax.broadcasted_iota(i32, (1, width), 1)
    valid = zone >= 0
    source = sum((lane >= group * k).astype(i32) for k in range(1, pairs))
    home = sum((zone >= local * k).astype(i32) for k in range(1, pairs))
    inside = zone - home * local
    side = (inside >= rows).astype(i32)
    row = inside - side * rows
    bin_at = lax.broadcasted_iota(i32, (bins, width), 0)
    before = (lax.broadcasted_iota(i32, (width, width), 0) < lax.broadcasted_iota(i32, (width, width), 1)).astype(bf16)

    def marks(key):
        return jnp.where(bin_at == jnp.where(valid, key, -1), 1.0, 0.0).astype(f32)

    def tally(mark):
        return jnp.sum(mark, axis=1, keepdims=True)

    def look(mark, table):
        return jnp.sum(mark * table, axis=0, keepdims=True)

    def ranks(mark):
        return jnp.dot(mark.astype(bf16), before, preferred_element_type=f32)

    spot = lax.broadcasted_iota(i32, (bins, 128), 0)
    at_row = spot & (rows - 1)
    at_home = spot >> (rows.bit_length() - 1)
    edge = jnp.logical_or(at_row == 0, at_row == rows - 1)

    def flip(x, bit):
        step = 1 << bit
        if 2 * step == bins:
            return beside(x, step)
        return jnp.where((spot & step) == 0, beside(x, step), beside(x, bins - step))

    across_x = lambda x: flip(x, 2)
    across_y = lambda x: flip(x, 3)
    mark = marks(home * rows + row)
    home_x = home & 1
    home_y = home >> 1
    beside_x = home_y * 2 + 1 - home_x
    beside_y = (1 - home_y) * 2 + home_x
    kinds = [source == beside_x, jnp.logical_and(source != beside_x, source != beside_y), source == beside_y]
    split = [jnp.where(kind, mark, 0.0) for kind in kinds]
    split_ranks = ranks(jnp.concatenate(split, axis=0))
    counts = [tally(part) for part in split]
    order = sum(look(part, split_ranks[k * bins:(k + 1) * bins] + sum(counts[:k])) for k, part in enumerate(split))
    total = sum(counts)
    native = jnp.broadcast_to(total, (bins, 128)).astype(i32)

    def whole(x):
        x = x + across_x(x)
        return x + across_y(x)

    load = native
    half_sum = whole(native + flip(native, 0))
    goal = (jnp.maximum(half_sum, flip(half_sum, 1)) + pairs - 1) >> (pairs.bit_length() - 1)
    row_sum = (whole(native) + pairs - 1) >> (pairs.bit_length() - 1)
    end_goal = jnp.maximum(jnp.maximum(row_sum, flip(flip(row_sum, 0), 1)), (9 * goal) >> 4)
    used = [jnp.zeros_like(native), jnp.zeros_like(native)]
    for _ in range(3):
        for d, partner in enumerate((across_x, across_y)):
            for stage in range(3):
                now, want = (load, end_goal) if stage == 0 else (load + flip(load, 0), goal)
                here = jnp.logical_not(edge) if stage == 1 else edge
                move = jnp.minimum((now - partner(now) + stage % 2) >> 1, now - want)
                move = jnp.minimum(move, jnp.minimum(extra - used[d], native - used[0] - used[1]))
                move = jnp.where(here, jnp.maximum(move, 0), 0)
                used[d] = used[d] + move
                load = load + partner(move) - move
    first = look(mark, (used[0] * allow)[:, :1].astype(f32))
    second = look(mark, (used[1] * allow)[:, :1].astype(f32))
    leaves_x = order < first
    keeps = look(mark, total) - second
    leaves_y = order >= keeps
    way = leaves_y.astype(i32)
    guest = order - jnp.where(leaves_y, keeps, 0.0)
    via = jnp.where(leaves_x, beside_x, jnp.where(leaves_y, beside_y, home))

    flow = marks(source * pairs + via)
    line = marks(via * rows + row)
    both = ranks(jnp.concatenate([flow, line], axis=0))
    rank = look(flow, both[:bins])
    place = look(line, both[bins:])
    flows = jnp.broadcast_to(tally(flow), (bins, 128))
    lines = jnp.broadcast_to(tally(line), (bins, 128))
    halves = lines + flip(lines, 0)
    stays = at_home == at_row
    chosen = jnp.full((1, 128), len(sizes), i32)
    for at, (wide, end, far) in reversed(list(enumerate(sizes))):
        over = jnp.where(flows > jnp.where(stays, per_pair + 2 * extra, wide).astype(f32), 1.0, 0.0)
        over = jnp.maximum(over, jnp.where(lines > jnp.where(edge, end, tall).astype(f32), 1.0, 0.0))
        over = jnp.maximum(over, jnp.where(halves > jnp.float32(far), 1.0, 0.0))
        chosen = jnp.where(jnp.max(over, axis=0, keepdims=True) > 0.0, chosen, at)

    my_x, my_y = pair % 2, pair // 2

    def offset(other):
        other_y = other >> 1
        other_x = other - 2 * other_y
        return jnp.where(other_x == my_x, 0, 1) + jnp.where(other_y == my_y, 0, 2)

    def invert(here, key, value):
        key = jnp.where(jnp.logical_and(valid, here), key, -1)
        hit = jnp.where(lax.broadcasted_iota(i32, (128, width), 0) == key, 1.0, 0.0).astype(bf16)
        value = jnp.broadcast_to(value.astype(bf16), (16, width))
        return lax.dot_general(value, hit, (((1,), (1,)), ((), ())), preferred_element_type=f32)[:1]

    rank = rank.astype(i32)
    place = place.astype(i32)
    guest = guest.astype(i32)

    def based(hop):
        return hop * per_pair + jnp.where(hop > 0, 2 * extra, 0)

    landing = based(offset(source)) + rank
    mine = via == pair
    ours = home == pair
    return chosen, [
        invert(source == pair, based(offset(via)) + rank, (lane - group * pair).astype(f32)),
        invert(mine, row * tall + place, landing.astype(f32)),
        invert(jnp.logical_and(mine, home != pair), (way * rows + row) * extra + guest, place.astype(f32)),
        invert(ours, (side * rows + row) * cap + slot, jnp.where(mine, place, tall + way * extra + guest).astype(f32)),
        invert(mine, row, jnp.ones((1, width), f32)),
        invert(ours, side * rows + row, jnp.ones((1, width), f32)),
    ]


def prepare_balanced(dims, sizes, zone, slot, table, choice, padded):
    pair = lax.axis_index("gx") // 2
    padded[...] = jnp.full_like(padded, -1)
    padded[0:1, 0:zone.shape[1]] = zone[...]
    padded[1:2, 0:zone.shape[1]] = slot[...]

    def fill(sizes, allow):
        chosen, lines = plan_tables(dims, sizes, pair, padded[0:1], padded[1:2], allow)
        for k, line in enumerate(lines):
            table[k:k + 1] = line.astype(jnp.int32)
        return jnp.max(chosen)

    chosen = fill(sizes, 1)
    choice[0] = jnp.minimum(chosen, len(sizes) - 1)

    @pl.when(chosen == len(sizes))
    def _():
        fill(sizes[:0], 0)


def mirror_rows(block):
    side = block.shape[0]
    row = PART - 1 - lax.broadcasted_iota(jnp.int32, (PART, block.shape[1]), 0)
    parts = [block[r - PART:r] for r in range(side, 0, -PART)]
    return jnp.concatenate([jnp.take_along_axis(part, row, axis=0) for part in parts], axis=0)


def turn(block, code):
    block = jnp.where(jnp.logical_or(code == 1, code == 2), mirror_lanes(block), block)
    block = jnp.where(code >= 2, mirror_rows(block), block)
    return jnp.where(jnp.logical_or(code == 1, code == 3), block.T, block)


def exchange_balanced(dims, chunks, table_in, spins_in, field, regional, *scratch):
    pairs, rows, per_group, per_pair, cap, extra, wide, end, far = dims
    tall = 2 * cap
    count = len(chunks)
    times, _, side, _ = field.shape
    strips = side // (2 * PART)
    kinds = 12
    groups = [scratch[i * count:(i + 1) * count] for i in range(kinds)]
    held, swapped, packed, landed, lifted, risen, pooled, crossed_in, crossed_out, passed, leaving, visiting = groups
    crossed = (crossed_in, crossed_out)
    raw, given, table, spins, far_list, *sems = scratch[kinds * count:]
    table_sem, spins_sem, raw_sem, swap_send, swap_recv, pair_send, pair_recv, near_send, near_recv = sems[:9]
    give_send, give_recv, far_send, far_recv, pass_send, pass_recv, side_send, side_recv = sems[9:]
    unit_at = {unit: (c, i) for c, chunk in enumerate(chunks) for i, unit in enumerate(chunk)}
    gx = lax.axis_index("gx")
    z = lax.axis_index("gy")
    pair = gx // 2
    half = lax.rem(gx, 2)
    mate = (2 * pair + 1 - half, z)
    pair_x = lax.rem(pair, 2)
    pair_y = pair // 2
    near, far_in, far_out = (origin_of(z, rows, k, True) for k in (1, 2, 3))
    inner = jnp.logical_or(z == 1, z == 2)
    outer = jnp.logical_not(inner)

    def across(o):
        x = 1 - pair_x if o % 2 else pair_x
        y = 1 - pair_y if o // 2 else pair_y
        return (2 * (2 * y + x) + half, z)

    spins_load = pltpu.make_async_copy(spins_in, spins, spins_sem)
    spins_load.start()
    table_load = pltpu.make_async_copy(table_in, table, table_sem)
    loads = []
    for t in range(times):
        loads.append(pltpu.make_async_copy(field.at[t], raw.at[pl.ds(t * per_group, per_group)], raw_sem.at[t]))
        loads[t].start()
    table_load.start()

    barrier = pltpu.get_barrier_semaphore()
    friends = [mate] + [across(o) for o in range(1, pairs)] + [(gx, lax.rem(z + o, rows)) for o in range(1, rows)]
    for friend in friends:
        pl.semaphore_signal(barrier, inc=1, device_id=friend, device_id_type=MESH)

    def turn_time(t):
        loads[t].wait()

        def one(b, carry):
            block = turn(raw[t * per_group + b], spins[gx * per_group + b])
            for r in range(strips):
                c, i = unit_at[r, t]
                top = block[r * PART:(r + 1) * PART]
                bottom = block[side // 2 + r * PART:side // 2 + (r + 1) * PART]
                held[c][half * per_group + b, i] = jnp.where(half == 0, top, bottom)
                swapped[c][b, i] = jnp.where(half == 0, bottom, top)
            return carry
        lax.fori_loop(0, per_group, one, 0, unroll=4)

    def wait_sent(sem, blocks):
        span = raw.at[pl.ds(0, blocks)]
        pltpu.make_async_copy(span, span, sem).wait()

    spins_load.wait()
    turn_time(0)
    table_load.wait()
    pl.semaphore_wait(barrier, len(friends))

    swaps = {}

    def swap_time(t):
        for c in sorted({unit_at[r, t][0] for r in range(strips)}):
            swaps[c] = pltpu.make_async_remote_copy(
                src_ref=swapped[c], dst_ref=held[c].at[pl.ds(half * per_group, per_group)],
                send_sem=swap_send.at[0], recv_sem=swap_recv.at[c], device_id=mate, device_id_type=MESH)
            swaps[c].start()

    swap_time(0)

    def send_pairs(c):
        if c == 1:
            for t in range(1, times):
                turn_time(t)
                swap_time(t)
        swaps[c].wait_recv()
        sent = []
        for o in range(1, pairs):
            def pack(k, carry, o=o):
                packed[c][o - 1, k] = held[c][table[0, o * per_pair + 2 * extra + k]]
                return carry
            lax.fori_loop(0, wide, pack, 0, unroll=4)
            sent.append(pltpu.make_async_remote_copy(
                src_ref=packed[c].at[o - 1], dst_ref=landed[c].at[pl.ds(o * per_pair + 2 * extra, wide)],
                send_sem=pair_send.at[o - 1], recv_sem=pair_recv.at[c],
                device_id=across(o), device_id_type=MESH))

        @pl.when(half == 0)
        def _():
            for copy in sent:
                copy.start()

        @pl.when(half == 1)
        def _():
            for copy in sent[::-1]:
                copy.start()

        def stay(k, carry):
            landed[c][k] = held[c][table[0, k]]
            return carry
        lax.fori_loop(0, per_pair + 2 * extra, stay, 0, unroll=4)

        if c == 0:
            lead = table[4, far_in]

            def gather_far(k, carry):
                at = jnp.where(k < lead, far_in * tall + k, far_out * tall + k - lead)
                far_list[k] = table[1, jnp.minimum(at, rows * tall - 1)]
                return carry
            lax.fori_loop(0, far, gather_far, 0, unroll=4)

    skip = table[4, z]

    def near_copy(c, size):
        return pltpu.make_async_remote_copy(
            src_ref=lifted[c].at[pl.ds(0, size)], dst_ref=risen[c].at[1, pl.ds(0, size)],
            send_sem=near_send.at[0], recv_sem=near_recv.at[c],
            device_id=(gx, near), device_id_type=MESH)

    def far_copy(c, place):
        return pltpu.make_async_remote_copy(
            src_ref=pooled[c], dst_ref=crossed[place][c],
            send_sem=far_send.at[0], recv_sem=far_recv.at[c, place],
            device_id=(gx, far_in), device_id_type=MESH)

    def pass_copy(c, place):
        return pltpu.make_async_remote_copy(
            src_ref=passed[c].at[place], dst_ref=risen[c].at[2 + place, pl.ds(0, end)],
            send_sem=pass_send.at[0], recv_sem=pass_recv.at[c],
            device_id=(gx, near), device_id_type=MESH)

    def side_copy(c, d):
        return pltpu.make_async_remote_copy(
            src_ref=leaving[c].at[d], dst_ref=visiting[c].at[d],
            send_sem=side_send.at[0], recv_sem=side_recv.at[c],
            device_id=across(1 + d), device_id_type=MESH)

    def send_rows(c):
        pltpu.make_async_copy(packed[c], packed[c], pair_recv.at[c]).wait()

        def pool(k, carry):
            pooled[c][k] = landed[c][far_list[k]]
            return carry
        lax.fori_loop(0, far, pool, 0, unroll=4)

        def lift(k, carry):
            lifted[c][k] = landed[c][table[1, near * tall + k]]
            return carry
        lax.fori_loop(0, tall, lift, 0, unroll=4)

        def send_far():
            for place, mine in enumerate((inner, outer)):
                @pl.when(mine)
                def _(place=place):
                    far_copy(c, place).start()

        @pl.when(half == 0)
        def _():
            send_far()

        @pl.when(inner)
        def _():
            near_copy(c, end).start()

        @pl.when(outer)
        def _():
            near_copy(c, tall).start()

        @pl.when(half == 1)
        def _():
            send_far()

        def own(k, carry):
            risen[c][0, k] = landed[c][table[1, z * tall + k]]
            return carry
        lax.fori_loop(0, tall, own, 0, unroll=4)

    def hand_on(c, place):
        @pl.when(inner)
        def _():
            far_copy(c, place).wait_recv()

            def onward(k, carry):
                passed[c][place, k] = crossed[place][c][jnp.minimum(skip + k, far - 1)]
                return carry
            lax.fori_loop(0, end, onward, 0, unroll=4)
            pass_copy(c, place).start()

            def land(k, carry):
                risen[c][2 + place, k] = crossed[place][c][k]
                return carry
            lax.fori_loop(0, tall, land, 0, unroll=4)

    def hand_on_inner(c):
        hand_on(c, 0)

    def hand_on_outer(c):
        hand_on(c, 1)

    def send_sides(c):
        @pl.when(inner)
        def _():
            near_copy(c, tall).wait_recv()

        @pl.when(outer)
        def _():
            near_copy(c, end).wait_recv()
            pltpu.make_async_copy(passed[c], passed[c], pass_recv.at[c]).wait()

        for d in range(2):
            def leave(k, carry, d=d):
                at = table[2, (d * rows + z) * extra + k]
                for o in range(rows):
                    leaving[c][d, o, k] = risen[c][o, at]
                return carry
            lax.fori_loop(0, extra, leave, 0)
            side_copy(c, d).start()

    def settle(c):
        pltpu.make_async_copy(visiting[c], visiting[c], side_recv.at[c]).wait()
        for r, _ in chunks[c]:
            if max(unit_at[r, t][0] for t in range(times)) == c:
                settle_strip(r)

    def settle_strip(r):
        span = pl.ds(pl.multiple_of(half * (side // 2) + r * PART, PART), PART)

        def place(s, carry):
            for core in (1 - half, half):
                at = table[3, (core * rows + z) * cap + s]
                live = s < table[5, core * rows + z]
                guest = jnp.maximum(at - tall, 0)
                way = guest // extra
                tiles = {}
                for t in range(times):
                    c, i = unit_at[r, t]
                    for o in range(rows):
                        home = risen[c][o, jnp.minimum(at, tall - 1), i]
                        visitor = visiting[c][way, o, guest - way * extra, i]
                        tiles[o, t] = jnp.where(at < tall, home, visitor)
                mean = sum(tiles.values()) * jnp.float32(1.0 / (rows * times))
                for (o, t), tile in tiles.items():
                    value = jnp.where(live, tile - mean, 0.0)
                    if core is half:
                        regional[origin_of(z, rows, o, True) * times + t, 0, s, span, :] = value
                    else:
                        given[r, origin_of(z, rows, o, True) * times + t, s] = value
            return carry
        lax.fori_loop(0, cap, place, 0)
        give = pltpu.make_async_remote_copy(
            src_ref=given.at[r], dst_ref=regional.at[:, 0, :, span, :],
            send_sem=give_send.at[0], recv_sem=give_recv.at[0], device_id=mate, device_id_type=MESH)
        give.start()

    starts = []
    for chunk in chunks:
        begin = starts[-1][1] if starts else 0
        starts.append((begin, begin + len(chunk)))
    for _, _, c, act in timetable(starts, wide, tall, end, far, extra, (send_pairs, send_rows, hand_on_outer, hand_on_inner, send_sides, settle)):
        act(c)

    wait_sent(swap_send.at[0], per_group)
    for o in range(1, pairs):
        wait_sent(pair_send.at[o - 1], wide)
    wait_sent(far_send.at[0], far)
    wait_sent(side_send.at[0], 2 * rows * extra)

    @pl.when(inner)
    def _():
        wait_sent(near_send.at[0], end)
        wait_sent(pass_send.at[0], 2 * end)

    @pl.when(outer)
    def _():
        wait_sent(near_send.at[0], tall)

    wait_sent(give_send.at[0], rows * cap)
    wait_sent(give_recv.at[0], rows * cap)


def timetable(starts, wide, tall, end, far, extra, acts):
    hop = 60
    sent = soon = crossed = passed = 0.0
    busy = 4 * wide * starts[-1][1]
    events = []
    for c, (begin, close) in enumerate(starts):
        size = close - begin
        sent = sent + 4 * wide * size
        landed = sent + hop
        soon = max(soon, landed) + (1.9 if 6 * far >= 7 * tall else 1.95) * (tall + far) * size
        crossed = max(crossed, landed) + 4 * far * size
        passed = max(passed, crossed + hop) + 4 * end * size
        sides = passed + hop
        busy = max(busy, sides) + 8 * extra * size
        for k, at in enumerate((0.0, landed, soon + hop, crossed + hop, sides, busy + 2 * hop)):
            events.append((at, k, c, acts[k]))
    return sorted(events, key=lambda e: e[:3])


def on_device(field, zone, slot, spins, tally):
    times, per_group, side, _ = field.shape
    columns = lax.axis_size("gx")
    rows = lax.axis_size("gy")
    pairs = columns // 2
    cap = 2 * per_group // rows
    per_pair = 4 * (2 * per_group // columns)
    balanced = rows == 4 and pairs == 4 and times == 2 and columns * per_group < 256 and 2 * rows * cap <= 128 and pairs * per_pair + 2 * (cap // 3) <= 128
    if balanced:
        return balanced_exchange(field, zone, slot, spins, cap, per_pair)
    chunks = chunk_units(times, side)
    tiles = [(len(chunk), PART, side) for chunk in chunks]
    final = plain_exchange(field, zone, slot, spins, chunks, tiles, cap, per_pair)
    return pl.pallas_call(
        functools.partial(finish, rows, chunks),
        grid_spec=pltpu.PrefetchScalarGridSpec(
            num_scalar_prefetch=1,
            grid=(cap,),
            in_specs=[pl.BlockSpec(
                (2, 1, rows) + tile,
                lambda s, count: (0, jnp.maximum(jnp.minimum(s, count[0] - 1), 0), 0, 0, 0, 0)) for tile in tiles],
            out_specs=pl.BlockSpec((rows * times, 1, 1, side, side), lambda s, count: (0, 0, s, 0, 0)),
        ),
        out_shape=jax.ShapeDtypeStruct((rows * times, 1, cap, side, side), jnp.float32),
        name="finish",
    )(tally, *final)


def scratch_of(tiles, *shapes):
    return [pltpu.VMEM(lead + tile, jnp.float32) for lead in shapes for tile in tiles]


def balanced_exchange(field, zone, slot, spins, cap, per_pair):
    times, per_group, side, _ = field.shape
    columns = lax.axis_size("gx")
    rows = lax.axis_size("gy")
    pairs = columns // 2
    tall = 2 * cap
    extra = cap // 3
    chunks = time_major(times, side)
    tiles = [(len(chunk), PART, side) for chunk in chunks]
    count = len(chunks)
    strips = side // (2 * PART)
    smem = pl.BlockSpec(memory_space=pltpu.SMEM)
    vmem = pl.BlockSpec(memory_space=pltpu.VMEM)
    sizes = balanced_sizes(per_pair, tall)
    lanes = -(-columns * per_group // 128) * 128
    table, choice = pl.pallas_call(
        functools.partial(prepare_balanced, (pairs, rows, per_group, per_pair, cap, extra), sizes),
        in_specs=[vmem, vmem],
        out_specs=[vmem, smem],
        out_shape=[jax.ShapeDtypeStruct((8, 128), jnp.int32), jax.ShapeDtypeStruct((1,), jnp.int32)],
        scratch_shapes=[pltpu.VMEM((8, lanes), jnp.int32)],
        name="prepare",
    )(zone.reshape(1, -1), slot.reshape(1, -1))

    def moved(wide, end, far, tag):
        dma = pltpu.SemaphoreType.DMA
        buffers = [
            *scratch_of(
                tiles, (2 * per_group,), (per_group,), (pairs - 1, wide), (pairs * per_pair + 2 * extra,), (tall,), (rows, tall),
                (far,), (far,), (far,), (2, end), (2, rows, extra), (2, rows, extra)),
            pltpu.VMEM((max(times * per_group, rows * cap, 2 * end, far), side, side), jnp.float32),
            pltpu.VMEM((strips, rows * times, cap, PART, side), jnp.float32),
            pltpu.SMEM((8, 128), jnp.int32), pltpu.SMEM(spins.shape, jnp.int32), pltpu.SMEM((far,), jnp.int32),
            dma, dma, dma((times,)), dma((1,)), dma((count,)), dma((pairs - 1,)), dma((count,)), dma((1,)), dma((count,)),
            dma((1,)), dma((1,)), dma((1,)), dma((count, 2)), dma((1,)), dma((count,)), dma((1,)), dma((count,)),
        ]
        return lambda: pl.pallas_call(
            functools.partial(
                exchange_balanced, (pairs, rows, per_group, per_pair, cap, extra, wide, end, far), chunks),
            in_specs=[pl.BlockSpec(memory_space=pl.ANY)] * 3,
            out_specs=vmem,
            out_shape=pltpu.VMEM((rows * times, 1, cap, side, side), jnp.float32),
            scratch_shapes=buffers,
            compiler_params=pltpu.CompilerParams(collective_id=tag, has_side_effects=True, vmem_limit_bytes=VMEM_BYTES),
            name=f"exchange_{tag}",
        )(table, spins, field)

    return lax.switch(choice[0], [moved(*size, tag) for tag, size in enumerate(sizes)])


def plain_exchange(field, zone, slot, spins, chunks, tiles, cap, per_pair):
    times, per_group, side, _ = field.shape
    columns = lax.axis_size("gx")
    rows = lax.axis_size("gy")
    pairs = columns // 2
    per_row = 2 * cap
    smem = pl.BlockSpec(memory_space=pltpu.SMEM)
    anywhere = pl.BlockSpec(memory_space=pl.ANY)
    i32 = jnp.int32
    narrow = levels(per_pair, (40,))[0]
    sizes = [(narrow, tall) for tall in levels(per_row, (36, 42))]
    sizes.append((per_pair, per_row))
    *turned, send_table, pick_table, tallies, choice = pl.pallas_call(
        functools.partial(prepare, (pairs, rows, per_group, per_pair, cap, chunks, sizes)),
        grid=(per_group // STEP_BLOCKS,),
        in_specs=[smem, smem, smem, pl.BlockSpec((times, STEP_BLOCKS, side, side), lambda i: (0, i, 0, 0))],
        out_specs=[
            *[pl.BlockSpec((2, STEP_BLOCKS) + tile, lambda i: (0, i, 0, 0, 0)) for tile in tiles],
            smem, smem, smem, smem,
        ],
        out_shape=[
            *[jax.ShapeDtypeStruct((2, per_group) + tile, jnp.float32) for tile in tiles],
            jax.ShapeDtypeStruct((pairs * per_pair + 1,), i32),
            jax.ShapeDtypeStruct((per_row * rows + 1,), i32),
            jax.ShapeDtypeStruct((2 * rows,), i32),
            jax.ShapeDtypeStruct((1,), i32),
        ],
        scratch_shapes=[pltpu.SMEM((columns * rows,), i32), pltpu.SMEM((pairs * pairs,), i32)],
        name="prepare",
    )(zone, slot, spins, field)
    count = len(chunks)

    def moved(wide, tall, tag):
        dma = pltpu.SemaphoreType.DMA
        buffers = [
            *scratch_of(
                tiles, (2 * per_group,), (pairs - 1, wide), (pairs * per_pair,), (rows - 1, tall), (rows, tall),
                (cap, rows), (cap, rows)),
            pltpu.SMEM((rows * tall,), i32),
            dma((count,)), dma((count,)), dma((count,)),
            dma((count, pairs - 1)), dma((count, pairs - 1)),
            dma((count, rows - 1)), dma((count, rows - 1)),
            dma((count,)), dma((count,)), dma((count,)),
        ]
        return lambda: pl.pallas_call(
            functools.partial(exchange, (pairs, rows, per_group, per_pair, wide, tall, cap, count)),
            in_specs=[smem, smem, smem] + [anywhere] * count,
            out_specs=[anywhere] * count,
            out_shape=[jax.ShapeDtypeStruct((2, cap, rows) + tile, jnp.float32) for tile in tiles],
            scratch_shapes=buffers,
            compiler_params=pltpu.CompilerParams(collective_id=tag, has_side_effects=True, vmem_limit_bytes=60 * 2**20),
            name=f"exchange_{tag}",
        )(send_table, pick_table, tallies, *turned)

    return lax.switch(choice[0], [moved(*size, tag) for tag, size in enumerate(sizes)])


def solution(mesh):
    placed = (P("gy", "gx", None, None), P(), P(), P(), P(("gx", "gy")))
    return jax.shard_map(
        on_device,
        mesh=mesh,
        in_specs=placed,
        out_specs=P(None, ("gx", "gy"), None, None, None),
        check_vma=False,
    )
```
